32 devices in a mesh: dp: 1 (over z), tp: 4 (over y), cp: 8 (over x, core).
Axes of the slice: x: 4, y: 4, z: 1, core: 2. Of those that a mesh axis runs over, the one named last changes fastest.
The devices are a block of a 4x4x8 slice.
Arguments:
- tokens_in: bfloat16 [8192, 4096], P(('dp', 'cp', 'tp'))
- grad_out: bfloat16 [8192, 4096], P(('dp', 'cp', 'tp'))
- w_query: bfloat16 [4096, 4096], P(None, 'tp')
- w_key: bfloat16 [4096, 4096], P(None, 'tp')
- w_value: bfloat16 [4096, 4096], P(None, 'tp')
- w_out: bfloat16 [4096, 4096], P('tp')
Outputs:
- output 1: bfloat16 [8192, 4096], P(('dp', 'cp', 'tp'))
- output 2: bfloat16 [8192, 4096], P(('dp', 'cp', 'tp'))
All inputs are finite; a program needn't handle non-finite values.
Results may differ from the reference program's by a relative error of at most 0.0104356.
Values are sent between devices in bfloat16 or wider.
A program may use at most 768 MiB of HBM per device.

```python
import math
import jax
import jax.numpy as jnp
from jax import lax

D = 4096
HQ = 32
HKV = 32
HEAD = 128
CP = 8
SEQ = 8192

GROUP_SIZE = HQ // HKV
SEQ_LOC = SEQ // CP
PIECE = SEQ_LOC // 2
ROW_BLOCK = 2 ** max(3, min(7, int(math.log2(max(1, 2 ** 22 // (SEQ * HQ))))))


def setup_inputs(seed: int = 0, part: int = 0) -> dict:
    base_key = jax.random.key(seed)
    data_key, weight_key = jax.random.split(base_key)
    part_key = jax.random.fold_in(data_key, part)
    key_x, key_dy = jax.random.split(part_key)
    key_q, key_k, key_v, key_o = jax.random.split(weight_key, 4)
    query_gain = math.sqrt(0.5 * math.log(SEQ))
    tokens_in = jax.random.normal(key_x, (SEQ, D), jnp.float32).astype(jnp.bfloat16)
    grad_out = jax.random.normal(key_dy, (SEQ, D), jnp.float32).astype(jnp.bfloat16)
    w_query = (jax.random.normal(key_q, (D, HQ * HEAD), jnp.float32) * (query_gain / math.sqrt(D))).astype(jnp.bfloat16)
    w_key = (jax.random.normal(key_k, (D, HKV * HEAD), jnp.float32) / math.sqrt(D)).astype(jnp.bfloat16)
    w_value = (jax.random.normal(key_v, (D, HKV * HEAD), jnp.float32) / math.sqrt(D)).astype(jnp.bfloat16)
    w_out = (jax.random.normal(key_o, (HQ * HEAD, D), jnp.float32) / math.sqrt(HQ * HEAD)).astype(jnp.bfloat16)
    return dict(tokens_in=tokens_in, grad_out=grad_out, w_query=w_query, w_key=w_key, w_value=w_value, w_out=w_out)


def fold_positions():
    row_ids = jnp.arange(SEQ, dtype=jnp.int32)
    shard_idx = row_ids // SEQ_LOC
    within = row_ids % SEQ_LOC
    piece_id = jnp.where(within < PIECE, shard_idx, 2 * CP - 1 - shard_idx)
    return piece_id * PIECE + within % PIECE


def reference(tokens_in, grad_out, w_query, w_key, w_value, w_out):
    score_scale = HEAD ** -0.5
    positions = fold_positions()
    queries = jnp.dot(tokens_in, w_query, preferred_element_type=jnp.float32).astype(jnp.bfloat16).reshape(SEQ, HKV, GROUP_SIZE, HEAD)
    keys_all = jnp.dot(tokens_in, w_key, preferred_element_type=jnp.float32).astype(jnp.bfloat16).reshape(SEQ, HKV, HEAD)
    values_all = jnp.dot(tokens_in, w_value, preferred_element_type=jnp.float32).astype(jnp.bfloat16).reshape(SEQ, HKV, HEAD)
    d_out = jnp.dot(grad_out, w_out.T, preferred_element_type=jnp.float32).astype(jnp.bfloat16).reshape(SEQ, HKV, GROUP_SIZE, HEAD)
    keys_f32 = keys_all.astype(jnp.float32)
    values_f32 = values_all.astype(jnp.float32)
    block_count = SEQ // ROW_BLOCK

    def block_step(acc_pair, blk_in):
        dk_acc, dv_acc = acc_pair
        q_blk, do_blk, pos_blk = blk_in
        query_f32 = q_blk.astype(jnp.float32)
        dout_f32 = do_blk.astype(jnp.float32)
        scores = jnp.einsum('qhgd,khd->hgqk', query_f32, keys_f32) * score_scale
        allowed = pos_blk[:, None] >= positions[None, :]
        scores = jnp.where(allowed, scores, -jnp.inf)
        log_norm = jax.nn.logsumexp(scores, axis=-1, keepdims=True)
        prob_f32 = jnp.exp(scores - log_norm).astype(jnp.bfloat16).astype(jnp.float32)
        out_blk = jnp.einsum('hgqk,khd->qhgd', prob_f32, values_f32).astype(jnp.bfloat16)
        row_delta = jnp.sum(dout_f32 * out_blk.astype(jnp.float32), axis=-1)
        d_prob = jnp.einsum('qhgd,khd->hgqk', dout_f32, values_f32)
        dscore_f32 = (prob_f32 * (d_prob - jnp.transpose(row_delta, (1, 2, 0))[..., None])).astype(jnp.bfloat16).astype(jnp.float32)
        dq_blk = (jnp.einsum('hgqk,khd->qhgd', dscore_f32, keys_f32) * score_scale).astype(jnp.bfloat16)
        dk_acc = dk_acc + jnp.einsum('hgqk,qhgd->khd', dscore_f32, query_f32) * score_scale
        dv_acc = dv_acc + jnp.einsum('hgqk,qhgd->khd', prob_f32, dout_f32)
        return (dk_acc, dv_acc), (out_blk, dq_blk)

    blk_inputs = (queries.reshape(block_count, ROW_BLOCK, HKV, GROUP_SIZE, HEAD), d_out.reshape(block_count, ROW_BLOCK, HKV, GROUP_SIZE, HEAD), positions.reshape(block_count, ROW_BLOCK))
    zeros_kv = jnp.zeros((SEQ, HKV, HEAD), jnp.float32)
    (dk_sum, dv_sum), (out_blocks, dq_blocks) = lax.scan(block_step, (zeros_kv, zeros_kv), blk_inputs)
    attn_out = out_blocks.reshape(SEQ, HQ * HEAD)
    d_query = dq_blocks.reshape(SEQ, HQ * HEAD)
    layer_out = jnp.dot(attn_out, w_out, preferred_element_type=jnp.float32).astype(jnp.bfloat16)
    grad_in = (jnp.dot(d_query, w_query.T, preferred_element_type=jnp.float32)
               + jnp.dot(dk_sum.astype(jnp.bfloat16).reshape(SEQ, HKV * HEAD), w_key.T, preferred_element_type=jnp.float32)
               + jnp.dot(dv_sum.astype(jnp.bfloat16).reshape(SEQ, HKV * HEAD), w_value.T, preferred_element_type=jnp.float32)).astype(jnp.bfloat16)
    return layer_out, grad_in
```

```python
import functools, math
import jax
import jax.numpy as jnp
from jax import lax
from jax.experimental import pallas as pl
from jax.experimental.pallas import tpu as pltpu

HEAD_DIM = 128
F32, BF16 = jnp.float32, jnp.bfloat16
LOG2E = math.log2(math.e)


def dot_nt(a, b):
    return lax.dot_general(a, b, (((1,), (1,)), ((), ())), preferred_element_type=F32)


def dot_nn(a, b):
    return lax.dot_general(a, b, (((1,), (0,)), ((), ())), preferred_element_type=F32)


def attn_fwd_kernel(bq, sub, q_ref, k_ref, v_ref, o_ref, l_ref, vt_ref, s_ref, acc_ref):
    seq = q_ref.shape[0]
    nblk = seq // bq
    nsub = bq // sub
    c = HEAD_DIM ** -0.5 * LOG2E

    def transpose_step(b, _):
        rows = pl.ds(pl.multiple_of(b * bq, bq), bq)
        vt_ref[:, rows] = v_ref[rows, :].T
        return 0

    lax.fori_loop(0, nblk, transpose_step, 0)

    def fill(q, blk, m, masked):
        for r in range(nsub):
            rows = pl.ds(pl.multiple_of(blk * bq + r * sub, sub), sub)
            s = dot_nt(k_ref[rows, :], q)
            if masked:
                kk = lax.broadcasted_iota(jnp.int32, (sub, bq), 0) + r * sub
                qq = lax.broadcasted_iota(jnp.int32, (sub, bq), 1)
                s = jnp.where(kk <= qq, s, -jnp.inf)
            s_ref[r * sub:(r + 1) * sub, :] = s
            m = jnp.maximum(m, jnp.max(s, axis=0, keepdims=True))
        return m

    def use(blk, m, m_old, l):
        mc = m * c
        alpha = jnp.exp2(m_old * c - mc)
        part = jnp.zeros((1, bq), F32)
        out = None
        for r in range(nsub):
            cols = pl.ds(pl.multiple_of(blk * bq + r * sub, sub), sub)
            p = jnp.exp2(s_ref[r * sub:(r + 1) * sub, :] * c - mc)
            part = part + jnp.sum(p, axis=0, keepdims=True)
            d = dot_nn(vt_ref[:, cols], p.astype(BF16))
            out = d if out is None else out + d
        acc_ref[...] = acc_ref[...] * alpha + out
        return l * alpha + part

    def q_step(i, _):
        rows = pl.ds(pl.multiple_of(i * bq, bq), bq)
        q = q_ref[rows, :]
        acc_ref[...] = jnp.zeros_like(acc_ref)
        m0 = jnp.full((1, bq), -jnp.inf, F32)
        m1 = fill(q, i, m0, True)

        def body(t, carry):
            m_old, m, l = carry
            cur = jnp.where(t == 0, i, t - 1)
            mc = m * c
            alpha = jnp.exp2(m_old * c - mc)
            part = jnp.zeros((1, bq), F32)
            m_new = m
            out = None
            for r in range(nsub):
                cols = pl.ds(pl.multiple_of(cur * bq + r * sub, sub), sub)
                krows = pl.ds(pl.multiple_of(t * bq + r * sub, sub), sub)
                p = jnp.exp2(s_ref[r * sub:(r + 1) * sub, :] * c - mc)
                s = dot_nt(k_ref[krows, :], q)
                part = part + jnp.sum(p, axis=0, keepdims=True)
                d = dot_nn(vt_ref[:, cols], p.astype(BF16))
                out = d if out is None else out + d
                m_new = jnp.maximum(m_new, jnp.max(s, axis=0, keepdims=True))
                s_ref[r * sub:(r + 1) * sub, :] = s
            acc_ref[...] = acc_ref[...] * alpha + out
            return m, m_new, l * alpha + part

        m_old, m, l = lax.fori_loop(0, i, body, (m1, m1, jnp.zeros((1, bq), F32)))
        l = use(jnp.where(i == 0, i, i - 1), m, m_old, l)
        o_ref[rows, :] = (acc_ref[...] * (1.0 / l)).T.astype(BF16)
        l_ref[i] = jnp.broadcast_to(m * c + jnp.log2(l), (8, bq))
        return 0

    lax.fori_loop(0, nblk, q_step, 0)


def attn_fwd(q, k, v, bq=512, sub=256):
    seq = q.shape[0]
    full = pl.BlockSpec(memory_space=pltpu.VMEM)
    tiles = seq * seq // 2
    return pl.pallas_call(
        functools.partial(attn_fwd_kernel, bq, sub),
        out_shape=(jax.ShapeDtypeStruct((seq, HEAD_DIM), BF16), jax.ShapeDtypeStruct((seq // bq, 8, bq), F32)),
        in_specs=[full] * 3,
        out_specs=(full, full),
        scratch_shapes=[pltpu.VMEM((HEAD_DIM, seq), BF16), pltpu.VMEM((bq, bq), F32), pltpu.VMEM((HEAD_DIM, bq), F32)],
        compiler_params=pltpu.CompilerParams(vmem_limit_bytes=48 << 20),
        cost_estimate=pl.CostEstimate(flops=4 * tiles * HEAD_DIM, bytes_accessed=8 * seq * HEAD_DIM, transcendentals=tiles),
        name="attn_fwd",
    )(q, k, v)


def attn_bwd_kernel(bq, sub, q_ref, k_ref, v_ref, do_ref, o_ref, l_ref, dq_ref, dk_ref, dv_ref, kt_ref, p_ref, ds_ref, dqt_ref, dk_acc, dv_acc):
    seq = q_ref.shape[0]
    nblk = seq // bq
    nsub = bq // sub
    scale = HEAD_DIM ** -0.5
    c = scale * LOG2E

    def init_step(b, _):
        rows = pl.ds(pl.multiple_of(b * bq, bq), bq)
        kt_ref[:, rows] = k_ref[rows, :].T
        dk_acc[rows, :] = jnp.zeros((bq, HEAD_DIM), F32)
        dv_acc[rows, :] = jnp.zeros((bq, HEAD_DIM), F32)
        return 0

    lax.fori_loop(0, nblk, init_step, 0)

    def q_step(i, _):
        rows = pl.ds(pl.multiple_of(i * bq, bq), bq)
        q = q_ref[rows, :]
        do = do_ref[rows, :]
        prod = do.astype(F32) * o_ref[rows, :].astype(F32)
        delta = jnp.sum(prod.T, axis=0, keepdims=True)
        lse = l_ref[i][0:1, :]
        dqt_ref[...] = jnp.zeros_like(dqt_ref)

        def make(blk, r, masked):
            krows = pl.ds(pl.multiple_of(blk * bq + r * sub, sub), sub)
            s = dot_nt(k_ref[krows, :], q)
            dp = dot_nt(v_ref[krows, :], do)
            p = jnp.exp2(s * c - lse)
            if masked:
                kk = lax.broadcasted_iota(jnp.int32, (sub, bq), 0) + r * sub
                qq = lax.broadcasted_iota(jnp.int32, (sub, bq), 1)
                p = jnp.where(kk <= qq, p, 0.0)
            pb = p.astype(BF16)
            ds = (pb.astype(F32) * (dp - delta)).astype(BF16)
            return pb, ds

        def flush(blk, r, pb, ds):
            krows = pl.ds(pl.multiple_of(blk * bq + r * sub, sub), sub)
            dv_acc[krows, :] += dot_nn(pb, do)
            dk_acc[krows, :] += dot_nn(ds, q)
            return dot_nn(kt_ref[:, krows], ds)

        for r in range(nsub):
            sl = slice(r * sub, (r + 1) * sub)
            p_ref[sl, :], ds_ref[sl, :] = make(i, r, True)

        def body(t, _):
            cur = jnp.where(t == 0, i, t - 1)
            out = None
            for r in range(nsub):
                sl = slice(r * sub, (r + 1) * sub)
                d = flush(cur, r, p_ref[sl, :], ds_ref[sl, :])
                out = d if out is None else out + d
                p_ref[sl, :], ds_ref[sl, :] = make(t, r, False)
            dqt_ref[...] += out
            return 0

        lax.fori_loop(0, i, body, 0)
        cur = jnp.where(i == 0, i, i - 1)
        out = None
        for r in range(nsub):
            sl = slice(r * sub, (r + 1) * sub)
            d = flush(cur, r, p_ref[sl, :], ds_ref[sl, :])
            out = d if out is None else out + d
        dq_ref[rows, :] = ((dqt_ref[...] + out) * scale).T.astype(BF16)
        return 0

    lax.fori_loop(0, nblk, q_step, 0)

    def final_step(b, _):
        rows = pl.ds(pl.multiple_of(b * bq, bq), bq)
        dk_ref[rows, :] = (dk_acc[rows, :] * scale).astype(BF16)
        dv_ref[rows, :] = dv_acc[rows, :].astype(BF16)
        return 0

    lax.fori_loop(0, nblk, final_step, 0)


def attn_bwd(q, k, v, do, o, lse, bq=512, sub=256):
    seq = q.shape[0]
    full = pl.BlockSpec(memory_space=pltpu.VMEM)
    tiles = seq * seq // 2
    shape = jax.ShapeDtypeStruct((seq, HEAD_DIM), BF16)
    return pl.pallas_call(
        functools.partial(attn_bwd_kernel, bq, sub),
        out_shape=(shape, shape, shape),
        in_specs=[full] * 6,
        out_specs=(full, full, full),
        scratch_shapes=[
            pltpu.VMEM((HEAD_DIM, seq), BF16),
            pltpu.VMEM((bq, bq), BF16),
            pltpu.VMEM((bq, bq), BF16),
            pltpu.VMEM((HEAD_DIM, bq), F32),
            pltpu.VMEM((seq, HEAD_DIM), F32),
            pltpu.VMEM((seq, HEAD_DIM), F32),
        ],
        compiler_params=pltpu.CompilerParams(vmem_limit_bytes=56 << 20),
        cost_estimate=pl.CostEstimate(flops=10 * tiles * HEAD_DIM, bytes_accessed=16 * seq * HEAD_DIM, transcendentals=tiles),
        name="attn_bwd",
    )(q, k, v, do, o, lse)


from jax.sharding import PartitionSpec as P

MESH = pl.DeviceIdType.MESH


def exchange_kernel(cp_size, to_heads, *refs):
    count = (len(refs) - 4) // 2
    srcs, dsts = refs[:count], refs[count:2 * count]
    stage, local_sem, send_sem, recv_sem = refs[2 * count:]
    me = lax.axis_index('cp')
    piece = stage.shape[2]

    def by_rows(ref, owner, half):
        start = jnp.where(half == 0, owner, 2 * cp_size - 1 - owner) * piece
        return ref.at[pl.ds(pl.multiple_of(start, piece), piece), :]

    def by_head(ref, head, half):
        return ref.at[pl.ds(half * piece, piece), pl.ds(pl.multiple_of(head * HEAD_DIM, HEAD_DIM), HEAD_DIM)]

    def ends(a, peer, half):
        if to_heads:
            return by_head(srcs[a], peer, half), by_rows(dsts[a], me, half)
        return by_rows(srcs[a], peer, half), by_head(dsts[a], me, half)

    barrier = pltpu.get_barrier_semaphore()
    for d in range(1, cp_size):
        pl.semaphore_signal(barrier, inc=1, device_id={'cp': lax.rem(me + d, cp_size)}, device_id_type=MESH)
    pl.semaphore_wait(barrier, cp_size - 1)
    copies = []
    order = sorted(range(1, cp_size), key=lambda d: -min(d, cp_size - d))
    for a in range(count):
        for d in order:
            peer = lax.rem(me + d, cp_size)
            for half in range(2):
                src, dst = ends(a, peer, half)
                copy = pltpu.make_async_remote_copy(
                    src_ref=src, dst_ref=dst, send_sem=send_sem.at[a, d - 1, half], recv_sem=recv_sem.at[a, d - 1, half],
                    device_id={'cp': peer}, device_id_type=MESH)
                copy.start()
                copies.append(copy)
    pulls = []
    for a in range(count):
        for half in range(2):
            src, dst = ends(a, me, half)
            pull = pltpu.make_async_copy(src, stage.at[a, half], local_sem.at[a, half])
            pull.start()
            pulls.append((pull, a, half, dst))
    pushes = []
    for pull, a, half, dst in pulls:
        pull.wait()
        push = pltpu.make_async_copy(stage.at[a, half], dst, local_sem.at[a, half])
        push.start()
        pushes.append(push)
    for push in pushes:
        push.wait()
    for copy in copies:
        copy.wait()


def exchange(arrays, cp_size, to_heads, collective_id):
    count = len(arrays)
    rows, cols = arrays[0].shape
    piece = rows // 2 if to_heads else rows // (2 * cp_size)
    out = (rows * cp_size, cols // cp_size) if to_heads else (rows // cp_size, cols * cp_size)
    sent = count * rows * cols * 2 * (cp_size - 1) // cp_size
    anywhere = pl.BlockSpec(memory_space=pl.ANY)
    return pl.pallas_call(
        functools.partial(exchange_kernel, cp_size, to_heads),
        out_shape=tuple(jax.ShapeDtypeStruct(out, BF16) for _ in arrays),
        in_specs=[anywhere] * count,
        out_specs=(anywhere,) * count,
        scratch_shapes=[
            pltpu.VMEM((count, 2, piece, HEAD_DIM), BF16),
            pltpu.SemaphoreType.DMA((count, 2)),
            pltpu.SemaphoreType.DMA((count, cp_size - 1, 2)),
            pltpu.SemaphoreType.DMA((count, cp_size - 1, 2)),
        ],
        compiler_params=pltpu.CompilerParams(collective_id=collective_id, has_side_effects=True, vmem_limit_bytes=8 << 20),
        cost_estimate=pl.CostEstimate(flops=1000 * sent, bytes_accessed=2 * sent, transcendentals=0),
        name="exchange_to_heads" if to_heads else "exchange_to_rows",
    )(*arrays)


def project(a, w):
    return jnp.dot(a, w, preferred_element_type=F32).astype(BF16)


def solution(mesh):
    cp_size = mesh.shape['cp']
    row_spec = P(('dp', 'cp', 'tp'), None)

    def local_step(x_blk, dy_blk, w_query, w_key, w_value, w_out):
        x_loc = lax.all_gather(x_blk, 'tp', axis=0, tiled=True)
        x_loc, dy_blk = lax.optimization_barrier((x_loc, dy_blk))
        dy_loc = lax.all_gather(dy_blk, 'tp', axis=0, tiled=True)
        q, k, v = exchange([project(x_loc, w) for w in (w_query, w_key, w_value)], cp_size, True, 0)
        out, lse = attn_fwd(q, k, v)
        dy_loc, out = lax.optimization_barrier((dy_loc, out))
        d_out = dot_nt(dy_loc, w_out).astype(BF16)
        (out_rows,) = exchange([out], cp_size, False, 2)
        y_part = jnp.dot(out_rows, w_out, preferred_element_type=F32)
        d_out, y_part = lax.optimization_barrier((d_out, y_part))
        y_blk = lax.psum_scatter(y_part, 'tp', scatter_dimension=0, tiled=True).astype(BF16)
        (do,) = exchange([d_out], cp_size, True, 1)
        grads = attn_bwd(q, k, v, do, out, lse)
        dq, dk, dv = exchange(list(grads), cp_size, False, 3)
        dx_part = dot_nt(dq, w_query) + dot_nt(dk, w_key) + dot_nt(dv, w_value)
        dx_blk = lax.psum_scatter(dx_part, 'tp', scatter_dimension=0, tiled=True).astype(BF16)
        return y_blk, dx_blk

    weight = P(None, 'tp')
    return jax.shard_map(local_step, mesh=mesh, in_specs=(row_spec, row_spec, weight, weight, weight, P('tp', None)), out_specs=(row_spec, row_spec), check_vma=False)
```

```python
import functools
import math

import jax
import jax.numpy as jnp
from jax import lax
from jax.experimental import pallas as pl
from jax.experimental.pallas import tpu as pltpu
from jax.sharding import PartitionSpec as P

HEAD_DIM = 128
F32, BF16 = jnp.float32, jnp.bfloat16
LOG2E = math.log2(math.e)
MESH = pl.DeviceIdType.MESH
ANYWHERE = pl.BlockSpec(memory_space=pltpu.HBM)
DMA = pltpu.SemaphoreType.DMA


def dot_nt(a, b):
    return lax.dot_general(a, b, (((1,), (1,)), ((), ())), preferred_element_type=F32)


def dot_nn(a, b):
    return lax.dot_general(a, b, (((1,), (0,)), ((), ())), preferred_element_type=F32)


def rows_at(start, size):
    return pl.ds(pl.multiple_of(start, size), size)


def ring(axis, size):
    me = lax.axis_index(axis)
    return me, lax.rem(me + 1, size), lax.rem(me + size - 1, size)


def meet(cp_size, tp_size, use_cp, use_tp):
    barrier = pltpu.get_barrier_semaphore()
    count = 0
    if use_cp:
        me = lax.axis_index('cp')
        for d in range(1, cp_size):
            pl.semaphore_signal(barrier, inc=1, device_id={'cp': lax.rem(me + d, cp_size)}, device_id_type=MESH)
        count += cp_size - 1
    if use_tp:
        _, right, left = ring('tp', tp_size)
        for peer in (right, left):
            pl.semaphore_signal(barrier, inc=1, device_id={'tp': peer}, device_id_type=MESH)
        count += 2
    pl.semaphore_wait(barrier, count)


def params(collective_id):
    return pltpu.CompilerParams(collective_id=collective_id, has_side_effects=True, vmem_limit_bytes=63 << 20)


def far_first(cp_size):
    return sorted(range(1, cp_size), key=lambda d: -min(d, cp_size - d))


def group_rows(tp_size):
    me, right, left = ring('tp', tp_size)
    far = lax.rem(me + 2, tp_size)
    return ((me, 0), (me, 1)), ((right, 0), (left, 1)), ((right, 1), (left, 0)), ((far, 0), (far, 1))


def position(cp_size, tp_size, block, owner, half):
    piece = block * tp_size // 2
    first = owner < tp_size // 2
    cp_rank = lax.axis_index('cp')
    piece_id = jnp.where(first, cp_rank, 2 * cp_size - 1 - cp_rank)
    return piece_id * piece + jnp.where(first, owner, owner - tp_size // 2) * block + half * (block // 2)


class HeadSender:
    def __init__(self, cp_size, tp_size, res, dst, send, recv, local):
        self.cp_size, self.tp_size = cp_size, tp_size
        self.res, self.dst, self.sems = res, dst, (send, recv, local)
        self.copies = []

    def start(self, g):
        send, recv, local = self.sems
        me = lax.axis_index('cp')
        block = self.res.shape[3]
        for half, (owner, part) in enumerate(group_rows(self.tp_size)[g]):
            rows = rows_at(position(self.cp_size, self.tp_size, block, owner, part), block // 2)
            here = pl.ds(half * (block // 2), block // 2)
            for d in far_first(self.cp_size):
                peer = lax.rem(me + d, self.cp_size)
                copy = pltpu.make_async_remote_copy(
                    src_ref=self.res.at[g, peer, :, here, :], dst_ref=self.dst.at[:, rows, :],
                    send_sem=send.at[d - 1, g, half], recv_sem=recv.at[d - 1, g, half],
                    device_id={'cp': peer}, device_id_type=MESH)
                copy.start()
                self.copies.append(copy)
            copy = pltpu.make_async_copy(self.res.at[g, me, :, here, :], self.dst.at[:, rows, :], local.at[g, half])
            copy.start()
            self.copies.append(copy)

    def wait(self):
        for copy in self.copies:
            copy.wait()


def head_scratch(cp_size, arrays, block):
    return [
        pltpu.VMEM((4, cp_size, arrays, block, HEAD_DIM), BF16),
        DMA((cp_size - 1, 4, 2)),
        DMA((cp_size - 1, 4, 2)),
        DMA((4, 2)),
    ]


def project_kernel(cp_size, tp_size, x_ref, dy_ref, wq_ref, wk_ref, wv_ref, qkv_ref, dy1_ref, w_v, xg, res, send, recv, local, w_sem, x_sem, y_send, y_recv):
    block = x_ref.shape[0]
    half = block // 2
    low, high = pl.ds(0, half), pl.ds(half, half)
    _, right, left = ring('tp', tp_size)
    heads = HeadSender(cp_size, tp_size, res, qkv_ref, send, recv, local)

    def pass_on(k, src, dst, peer):
        copy = pltpu.make_async_remote_copy(
            src_ref=src, dst_ref=dst, send_sem=y_send.at[k], recv_sem=y_recv.at[k], device_id={'tp': peer}, device_id_type=MESH)
        copy.start()
        return copy

    own = pltpu.make_async_copy(x_ref, xg.at[0], x_sem)
    own.start()
    loads = [pltpu.make_async_copy(w, w_v.at[n], w_sem.at[n]) for n, w in enumerate((wq_ref, wk_ref, wv_ref))]
    meet(cp_size, tp_size, True, True)
    hops = [
        pass_on(0, x_ref.at[low, :], xg.at[1, low, :], left),
        pass_on(1, x_ref.at[high, :], xg.at[1, high, :], right),
        pass_on(2, x_ref.at[high, :], xg.at[2, low, :], left),
        pass_on(3, x_ref.at[low, :], xg.at[2, high, :], right),
    ]
    for load in loads:
        load.start()
    own.wait()

    wide = min(4, cp_size)
    cols = wide * HEAD_DIM
    steps = cp_size // wide

    def compute(g, n):
        def body(s, _):
            out = dot_nn(xg[g], w_v[n, :, rows_at(s * cols, cols)]).astype(BF16)
            for k in range(wide):
                res[g, wide * s + k, n] = out[:, k * HEAD_DIM:(k + 1) * HEAD_DIM]
            return 0

        lax.fori_loop(0, steps, body, 0)

    for n in range(3):
        loads[n].wait()
        compute(0, n)
    heads.start(0)
    hops[0].wait_recv()
    hops.append(pass_on(4, xg.at[1, low, :], xg.at[3, low, :], left))
    hops[1].wait_recv()
    hops.append(pass_on(5, xg.at[1, high, :], xg.at[3, high, :], right))
    hops.append(pass_on(6, dy_ref.at[low, :], dy1_ref.at[low, :], left))
    hops.append(pass_on(7, dy_ref.at[high, :], dy1_ref.at[high, :], right))
    for g, arrived in ((1, ()), (2, (2, 3)), (3, (4, 5))):
        for k in arrived:
            hops[k].wait_recv()
        for n in range(3):
            compute(g, n)
        heads.start(g)
    for k in range(6):
        hops[k].wait_send()
    for k in (6, 7):
        hops[k].wait()
    heads.wait()


def project(x_blk, dy_blk, weights, cp_size, tp_size):
    block, width = x_blk.shape
    cols = weights[0].shape[1]
    seq = block * tp_size * cp_size
    return pl.pallas_call(
        functools.partial(project_kernel, cp_size, tp_size),
        out_shape=(jax.ShapeDtypeStruct((3, seq, HEAD_DIM), BF16), jax.ShapeDtypeStruct((block, width), BF16)),
        in_specs=[ANYWHERE] * 5,
        out_specs=(ANYWHERE, ANYWHERE),
        scratch_shapes=[pltpu.VMEM((3, width, cols), BF16), pltpu.VMEM((4, block, width), BF16)] + head_scratch(cp_size, 3, block) + [
            DMA((3,)), DMA, DMA((8,)), DMA((8,))],
        compiler_params=params(0),
        cost_estimate=pl.CostEstimate(flops=6 * block * tp_size * width * cols, bytes_accessed=6 * width * cols, transcendentals=0),
        name="project_qkv",
    )(x_blk, dy_blk, *weights)


def send_piece(cp_size, i, src, dst_of, send, recv, local, start):
    me = lax.axis_index('cp')
    half = jnp.where(i < cp_size, 0, 1)
    owner = jnp.where(i < cp_size, i, 2 * cp_size - 1 - i)

    @pl.when(owner == me)
    def _():
        copy = pltpu.make_async_copy(src, dst_of(half, me), local.at[half])
        copy.start() if start else copy.wait()

    @pl.when(owner != me)
    def _():
        copy = pltpu.make_async_remote_copy(
            src_ref=src, dst_ref=dst_of(half, me), send_sem=send.at[i], recv_sem=recv.at[me, half],
            device_id={'cp': owner}, device_id_type=MESH)
        copy.start() if start else copy.wait_send()


def wait_pieces(cp_size, src_of, dst_of, send, recv, local):
    me = lax.axis_index('cp')

    def sent(i, _):
        send_piece(cp_size, i, src_of(i), dst_of, send, recv, local, False)
        return 0

    lax.fori_loop(0, 2 * cp_size, sent, 0)
    for d in range(1, cp_size):
        peer = lax.rem(me + d, cp_size)
        for half in range(2):
            pltpu.make_async_remote_copy(
                src_ref=src_of(0), dst_ref=dst_of(half, peer), send_sem=send.at[0], recv_sem=recv.at[peer, half],
                device_id={'cp': peer}, device_id_type=MESH).wait_recv()


def forward_kernel(cp_size, tp_size, qkv_ref, dy_ref, dy1_ref, o_ref, l_ref, rows_ref, dy23_ref,
                   qkv, o_v, l_v, vt_ref, s_ref, acc_ref, in_sem, send, recv, local, y_send, y_recv, out_sem):
    seq = qkv.shape[1]
    bq = s_ref.shape[0]
    nblk = seq // bq
    c = HEAD_DIM ** -0.5 * LOG2E
    _, right, left = ring('tp', tp_size)
    half = dy_ref.shape[0] // 2
    low, high = pl.ds(0, half), pl.ds(half, half)

    load = pltpu.make_async_copy(qkv_ref, qkv, in_sem)
    load.start()
    meet(cp_size, tp_size, True, True)
    hops = []
    for k, (src, dst, peer) in enumerate((
            (dy_ref.at[high, :], dy23_ref.at[0, low, :], left),
            (dy_ref.at[low, :], dy23_ref.at[0, high, :], right),
            (dy1_ref.at[low, :], dy23_ref.at[1, low, :], left),
            (dy1_ref.at[high, :], dy23_ref.at[1, high, :], right))):
        hop = pltpu.make_async_remote_copy(
            src_ref=src, dst_ref=dst, send_sem=y_send.at[k], recv_sem=y_recv.at[k], device_id={'tp': peer}, device_id_type=MESH)
        hop.start()
        hops.append(hop)
    load.wait()

    def transpose_step(b, _):
        rows = rows_at(b * bq, bq)
        vt_ref[:, rows] = qkv[2, rows, :].T
        return 0

    lax.fori_loop(0, nblk, transpose_step, 0)

    def src_of(i):
        return o_v.at[rows_at(i * bq, bq), :]

    def dst_of(part, head):
        return rows_ref.at[rows_at(part * bq, bq), rows_at(head * HEAD_DIM, HEAD_DIM)]

    def q_step(i, _):
        rows = rows_at(i * bq, bq)
        q = qkv[0, rows, :]
        acc_ref[...] = jnp.zeros_like(acc_ref)
        s = dot_nt(qkv[1, rows, :], q)
        kk = lax.broadcasted_iota(jnp.int32, (bq, bq), 0)
        qq = lax.broadcasted_iota(jnp.int32, (bq, bq), 1)
        s = jnp.where(kk <= qq, s, -jnp.inf)
        s_ref[...] = s
        first = jnp.max(s, axis=0, keepdims=True)

        def use(blk, m_old, m, l, following):
            mc = m * c
            alpha = jnp.exp2(m_old * c - mc)
            p = jnp.exp2(s_ref[...] * c - mc)
            m_new = m
            if following is not None:
                s = dot_nt(qkv[1, rows_at(following * bq, bq), :], q)
            part = jnp.sum(p, axis=0, keepdims=True)
            out = dot_nn(vt_ref[:, rows_at(blk * bq, bq)], p.astype(BF16))
            if following is not None:
                m_new = jnp.maximum(m, jnp.max(s, axis=0, keepdims=True))
                s_ref[...] = s
            acc_ref[...] = acc_ref[...] * alpha + out
            return m, m_new, l * alpha + part

        def body(t, carry):
            return use(jnp.where(t == 0, i, t - 1), *carry, t)

        carry = lax.fori_loop(0, i, body, (first, first, jnp.zeros((1, bq), F32)))
        m, _, l = use(jnp.where(i == 0, i, i - 1), *carry, None)
        o_v[rows, :] = (acc_ref[...] * (1.0 / l)).T.astype(BF16)
        l_v[i] = jnp.broadcast_to(m * c + jnp.log2(l), (8, bq))
        send_piece(cp_size, i, src_of(i), dst_of, send, recv, local, True)
        return 0

    lax.fori_loop(0, nblk, q_step, 0)
    out_o = pltpu.make_async_copy(o_v, o_ref, out_sem.at[0])
    out_l = pltpu.make_async_copy(l_v, l_ref, out_sem.at[1])
    out_o.start()
    out_l.start()
    wait_pieces(cp_size, src_of, dst_of, send, recv, local)
    for hop in hops:
        hop.wait()
    out_o.wait()
    out_l.wait()


def forward(qkv, dy_blk, dy1, cp_size, tp_size):
    seq = qkv.shape[1]
    bq = seq // (2 * cp_size)
    block, width = dy_blk.shape
    pairs = seq * seq // 2
    return pl.pallas_call(
        functools.partial(forward_kernel, cp_size, tp_size),
        out_shape=(
            jax.ShapeDtypeStruct((seq, HEAD_DIM), BF16),
            jax.ShapeDtypeStruct((seq // bq, 8, bq), F32),
            jax.ShapeDtypeStruct((2 * bq, cp_size * HEAD_DIM), BF16),
            jax.ShapeDtypeStruct((2, block, width), BF16),
        ),
        in_specs=[ANYWHERE] * 3,
        out_specs=(ANYWHERE,) * 4,
        scratch_shapes=[
            pltpu.VMEM((3, seq, HEAD_DIM), BF16),
            pltpu.VMEM((seq, HEAD_DIM), BF16),
            pltpu.VMEM((seq // bq, 8, bq), F32),
            pltpu.VMEM((HEAD_DIM, seq), BF16),
            pltpu.VMEM((bq, bq), F32),
            pltpu.VMEM((HEAD_DIM, bq), F32),
            DMA, DMA((2 * cp_size,)), DMA((cp_size, 2)), DMA((2,)), DMA((4,)), DMA((4,)), DMA((2,)),
        ],
        compiler_params=params(1),
        cost_estimate=pl.CostEstimate(flops=4 * pairs * HEAD_DIM, bytes_accessed=8 * seq * HEAD_DIM, transcendentals=pairs),
        name="attention_forward",
    )(qkv, dy_blk, dy1)


def middle_kernel(cp_size, tp_size, dy_ref, dy1_ref, dy23_ref, wo_ref, rows_ref, do_ref, y_ref,
                  dyg, wo, o_v, y_v, res, send, recv, local, in_sem, y_sem):
    block = dy_ref.shape[0]
    heads = HeadSender(cp_size, tp_size, res, do_ref, send, recv, local)
    loads = [
        pltpu.make_async_copy(wo_ref, wo, in_sem.at[0]),
        pltpu.make_async_copy(dy_ref, dyg.at[0], in_sem.at[1]),
        pltpu.make_async_copy(dy1_ref, dyg.at[1], in_sem.at[2]),
        pltpu.make_async_copy(dy23_ref, dyg.at[pl.ds(2, 2)], in_sem.at[3]),
        pltpu.make_async_copy(rows_ref, o_v, in_sem.at[4]),
    ]
    for load in loads:
        load.start()
    meet(cp_size, tp_size, True, False)
    per_step = min(4, cp_size)
    cols = per_step * HEAD_DIM
    loads[0].wait()
    for g in range(4):
        if g < 3:
            loads[g + 1].wait()

        def body(s, _):
            out = dot_nt(dyg[g], wo[rows_at(s * cols, cols), :]).astype(BF16)
            for k in range(per_step):
                res[g, per_step * s + k, 0] = out[:, k * HEAD_DIM:(k + 1) * HEAD_DIM]
            return 0

        lax.fori_loop(0, wo.shape[0] // cols, body, 0)
        heads.start(g)
    loads[4].wait()
    wide = y_v.shape[2]
    count = wo.shape[1] // wide

    def put(s, slot):
        return pltpu.make_async_copy(y_v.at[slot], y_ref.at[:, rows_at(s * wide, wide)], y_sem.at[slot])

    def y_step(s, _):
        slot = lax.rem(s, 2)

        @pl.when(s >= 2)
        def _():
            put(s - 2, slot).wait()

        y_v[slot] = dot_nn(o_v[...], wo[:, rows_at(s * wide, wide)])
        put(s, slot).start()
        return 0

    lax.fori_loop(0, count, y_step, 0)
    for s in range(count - 2, count):
        put(s, s % 2).wait()
    heads.wait()


def middle(dy_blk, dy1, dy23, w_out, o_rows, cp_size, tp_size):
    block, width = dy_blk.shape
    cols = w_out.shape[0]
    rows = block * tp_size
    wide = width // 8
    return pl.pallas_call(
        functools.partial(middle_kernel, cp_size, tp_size),
        out_shape=(jax.ShapeDtypeStruct((1, rows * cp_size, HEAD_DIM), BF16), jax.ShapeDtypeStruct((rows, width), F32)),
        in_specs=[ANYWHERE] * 5,
        out_specs=(ANYWHERE, ANYWHERE),
        scratch_shapes=[
            pltpu.VMEM((4, block, width), BF16),
            pltpu.VMEM((cols, width), BF16),
            pltpu.VMEM((rows, cols), BF16),
            pltpu.VMEM((2, rows, wide), F32),
        ] + head_scratch(cp_size, 1, block) + [DMA((5,)), DMA((2,))],
        compiler_params=params(2),
        cost_estimate=pl.CostEstimate(flops=4 * rows * width * cols, bytes_accessed=8 * rows * width, transcendentals=0),
        name="project_middle",
    )(dy_blk, dy1, dy23, w_out, o_rows)


def backward_kernel(cp_size, qkv_ref, do_ref, o_ref, l_ref, rows_ref,
                    qkv, do_v, o_v, l_v, kt_ref, p_ref, ds_ref, dqt_ref, dk_acc, dv_acc, grads, in_sem, send, recv, local):
    seq = qkv.shape[1]
    bq = p_ref.shape[0]
    nblk = seq // bq
    sub = bq // 2
    scale = HEAD_DIM ** -0.5
    c = scale * LOG2E
    loads = [
        pltpu.make_async_copy(qkv_ref, qkv, in_sem.at[0]),
        pltpu.make_async_copy(do_ref.at[0], do_v, in_sem.at[1]),
        pltpu.make_async_copy(o_ref, o_v, in_sem.at[2]),
        pltpu.make_async_copy(l_ref, l_v, in_sem.at[3]),
    ]
    for load in loads:
        load.start()
    meet(cp_size, 0, True, False)
    for load in loads:
        load.wait()

    def init_step(b, _):
        rows = rows_at(b * bq, bq)
        kt_ref[:, rows] = qkv[1, rows, :].T
        dk_acc[rows, :] = jnp.zeros((bq, HEAD_DIM), F32)
        dv_acc[rows, :] = jnp.zeros((bq, HEAD_DIM), F32)
        return 0

    lax.fori_loop(0, nblk, init_step, 0)

    def src_of(i):
        return grads.at[:, rows_at(i * bq, bq), :]

    def dst_of(part, head):
        return rows_ref.at[:, rows_at(part * bq, bq), rows_at(head * HEAD_DIM, HEAD_DIM)]

    def q_step(back, _):
        i = nblk - 1 - back
        rows = rows_at(i * bq, bq)
        q = qkv[0, rows, :]
        do = do_v[rows, :]
        prod = do.astype(F32) * o_v[rows, :].astype(F32)
        delta = jnp.sum(prod.T, axis=0, keepdims=True)
        lse = l_v[i][0:1, :]
        dqt_ref[...] = jnp.zeros_like(dqt_ref)

        def make(blk, r, masked):
            krows = rows_at(blk * bq + r * sub, sub)
            s = dot_nt(qkv[1, krows, :], q)
            dp = dot_nt(qkv[2, krows, :], do)
            p = jnp.exp2(s * c - lse)
            if masked:
                kk = lax.broadcasted_iota(jnp.int32, (sub, bq), 0) + r * sub
                qq = lax.broadcasted_iota(jnp.int32, (sub, bq), 1)
                p = jnp.where(kk <= qq, p, 0.0)
            pb = p.astype(BF16)
            ds = (pb.astype(F32) * (dp - delta)).astype(BF16)
            return pb, ds

        def flush(blk, r):
            krows = rows_at(blk * bq + r * sub, sub)
            sl = slice(r * sub, (r + 1) * sub)
            ds = ds_ref[sl, :]
            dv_acc[krows, :] += dot_nn(p_ref[sl, :], do)
            dk_acc[krows, :] += dot_nn(ds, q)
            return dot_nn(kt_ref[:, krows], ds)

        for r in range(2):
            sl = slice(r * sub, (r + 1) * sub)
            p_ref[sl, :], ds_ref[sl, :] = make(i, r, True)

        def body(t, _):
            cur = jnp.where(t == 0, i, t - 1)
            out = None
            for r in range(2):
                sl = slice(r * sub, (r + 1) * sub)
                d = flush(cur, r)
                out = d if out is None else out + d
                p_ref[sl, :], ds_ref[sl, :] = make(t, r, False)
            dqt_ref[...] += out
            return 0

        lax.fori_loop(0, i, body, 0)
        cur = jnp.where(i == 0, i, i - 1)
        out = flush(cur, 0) + flush(cur, 1)
        grads[0, rows, :] = ((dqt_ref[...] + out) * scale).T.astype(BF16)
        grads[1, rows, :] = (dk_acc[rows, :] * scale).astype(BF16)
        grads[2, rows, :] = dv_acc[rows, :].astype(BF16)
        send_piece(cp_size, i, src_of(i), dst_of, send, recv, local, True)
        return 0

    lax.fori_loop(0, nblk, q_step, 0)
    wait_pieces(cp_size, src_of, dst_of, send, recv, local)


def backward(qkv, do, o, lse, cp_size):
    seq = qkv.shape[1]
    bq = seq // (2 * cp_size)
    pairs = seq * seq // 2
    return pl.pallas_call(
        functools.partial(backward_kernel, cp_size),
        out_shape=jax.ShapeDtypeStruct((3, 2 * bq, cp_size * HEAD_DIM), BF16),
        in_specs=[ANYWHERE] * 4,
        out_specs=ANYWHERE,
        scratch_shapes=[
            pltpu.VMEM((3, seq, HEAD_DIM), BF16),
            pltpu.VMEM((seq, HEAD_DIM), BF16),
            pltpu.VMEM((seq, HEAD_DIM), BF16),
            pltpu.VMEM((seq // bq, 8, bq), F32),
            pltpu.VMEM((HEAD_DIM, seq), BF16),
            pltpu.VMEM((bq, bq), BF16),
            pltpu.VMEM((bq, bq), BF16),
            pltpu.VMEM((HEAD_DIM, bq), F32),
            pltpu.VMEM((seq, HEAD_DIM), F32),
            pltpu.VMEM((seq, HEAD_DIM), F32),
            pltpu.VMEM((3, seq, HEAD_DIM), BF16),
            DMA((4,)), DMA((2 * cp_size,)), DMA((cp_size, 2)), DMA((2,)),
        ],
        compiler_params=params(3),
        cost_estimate=pl.CostEstimate(flops=10 * pairs * HEAD_DIM, bytes_accessed=16 * seq * HEAD_DIM, transcendentals=pairs),
        name="attention_backward",
    )(qkv, do, o, lse)


def reduce_kernel(tp_size, chunks, rows_ref, wq_ref, wk_ref, wv_ref, out_ref,
                  g_v, w_v, part, mid, last, out_v, in_sem, w_sem, out_sem, sends, recvs):
    me, right, left = ring('tp', tp_size)
    far = lax.rem(me + 2, tp_size)
    block = part.shape[1]
    half = block // 2
    low, high = pl.ds(0, half), pl.ds(half, half)
    wide = part.shape[2] // chunks
    weights = (wq_ref, wk_ref, wv_ref)

    def w_load(n, a):
        return pltpu.make_async_copy(weights[a].at[rows_at(n * wide, wide), :], w_v.at[lax.rem(n, 2), a], w_sem.at[lax.rem(n, 2), a])

    load = pltpu.make_async_copy(rows_ref, g_v, in_sem)
    load.start()
    for a in range(3):
        w_load(0, a).start()
    meet(0, tp_size, False, True)

    def hop(kind, n):
        cols = rows_at(n * wide, wide)
        src, dst, peer = {
            'far_r': (part.at[0, low, cols], mid.at[0, :, cols], right),
            'far_l': (part.at[0, high, cols], mid.at[1, :, cols], left),
            'plain_r': (part.at[1, high, cols], last.at[0, high, cols], right),
            'plain_l': (part.at[2, low, cols], last.at[1, low, cols], left),
            'sum_r': (part.at[1, low, cols], last.at[0, low, cols], right),
            'sum_l': (part.at[2, high, cols], last.at[1, high, cols], left),
        }[kind]
        k = ('far_r', 'far_l', 'plain_r', 'plain_l', 'sum_r', 'sum_l').index(kind)
        return pltpu.make_async_remote_copy(
            src_ref=src, dst_ref=dst, send_sem=sends.at[k, n], recv_sem=recvs.at[k, n], device_id={'tp': peer}, device_id_type=MESH)

    load.wait()
    owners = (far, right, left, me)

    def compute(n, _):
        slot = lax.rem(n, 2)

        @pl.when(n + 1 < chunks)
        def _():
            for a in range(3):
                w_load(n + 1, a).start()

        for a in range(3):
            w_load(n, a).wait()
        cols = rows_at(n * wide, wide)
        for k in range(4):
            rows = rows_at(owners[k] * block, block)
            total = dot_nt(g_v[0, rows, :], w_v[slot, 0])
            total = total + dot_nt(g_v[1, rows, :], w_v[slot, 1])
            part[k, :, cols] = total + dot_nt(g_v[2, rows, :], w_v[slot, 2])
        for kind in ('far_r', 'far_l', 'plain_r', 'plain_l'):
            hop(kind, n).start()
        return 0

    lax.fori_loop(0, chunks, compute, 0)

    def forward_sums(n, _):
        cols = rows_at(n * wide, wide)
        hop('far_r', n).wait_recv()
        part[1, :half, cols] += mid[0, :, cols]
        hop('sum_r', n).start()
        hop('far_l', n).wait_recv()
        part[2, half:, cols] += mid[1, :, cols]
        hop('sum_l', n).start()
        return 0

    lax.fori_loop(0, chunks, forward_sums, 0)

    def put(n):
        cols = rows_at(n * wide, wide)
        return pltpu.make_async_copy(out_v.at[:, cols], out_ref.at[:, cols], out_sem.at[n])

    def finish(n, _):
        cols = rows_at(n * wide, wide)
        for kind in ('plain_r', 'plain_l', 'sum_r', 'sum_l'):
            hop(kind, n).wait_recv()
        out_v[:, cols] = (part[3, :, cols] + last[0, :, cols] + last[1, :, cols]).astype(BF16)
        put(n).start()
        return 0

    lax.fori_loop(0, chunks, finish, 0)

    def close(n, _):
        put(n).wait()
        for kind in ('far_r', 'far_l', 'plain_r', 'plain_l', 'sum_r', 'sum_l'):
            hop(kind, n).wait_send()
        return 0

    lax.fori_loop(0, chunks, close, 0)


def reduce_out(grad_rows, weights, tp_size):
    width, cols = weights[0].shape
    rows = grad_rows.shape[1]
    block = rows // tp_size
    chunks = 8
    wide = width // chunks
    return pl.pallas_call(
        functools.partial(reduce_kernel, tp_size, chunks),
        out_shape=jax.ShapeDtypeStruct((block, width), BF16),
        in_specs=[ANYWHERE] * 4,
        out_specs=ANYWHERE,
        scratch_shapes=[
            pltpu.VMEM((3, rows, cols), BF16),
            pltpu.VMEM((2, 3, wide, cols), BF16),
            pltpu.VMEM((4, block, width), F32),
            pltpu.VMEM((2, block // 2, width), F32),
            pltpu.VMEM((2, block, width), F32),
            pltpu.VMEM((block, width), BF16),
            DMA, DMA((2, 3)), DMA((chunks,)), DMA((6, chunks)), DMA((6, chunks)),
        ],
        compiler_params=params(4),
        cost_estimate=pl.CostEstimate(flops=6 * rows * width * cols, bytes_accessed=6 * width * cols, transcendentals=0),
        name="project_reduce",
    )(grad_rows, *weights)


def solution(mesh):
    cp_size, tp_size = mesh.shape['cp'], mesh.shape['tp']
    row_spec = P(('dp', 'cp', 'tp'), None)

    def local_step(x_blk, dy_blk, w_query, w_key, w_value, w_out):
        weights = (w_query, w_key, w_value)
        qkv, dy1 = project(x_blk, dy_blk, weights, cp_size, tp_size)
        o, lse, o_rows, dy23 = forward(qkv, dy_blk, dy1, cp_size, tp_size)
        do, y_part = middle(dy_blk, dy1, dy23, w_out, o_rows, cp_size, tp_size)
        y_blk = lax.psum_scatter(y_part, 'tp', scatter_dimension=0, tiled=True).astype(BF16)
        grad_rows = backward(qkv, do, o, lse, cp_size)
        dx_blk = reduce_out(grad_rows, weights, tp_size)
        return y_blk, dx_blk

    weight = P(None, 'tp')
    return jax.shard_map(local_step, mesh=mesh, in_specs=(row_spec, row_spec, weight, weight, weight, P('tp', None)), out_specs=(row_spec, row_spec), check_vma=False)
```

```python
import functools
import math

import jax
import jax.numpy as jnp
from jax import lax
from jax.experimental import pallas as pl
from jax.experimental.pallas import tpu as pltpu
from jax.sharding import PartitionSpec as P

HEAD_DIM = 128
F32, BF16 = jnp.float32, jnp.bfloat16
LOG2E = math.log2(math.e)
MESH = pl.DeviceIdType.MESH
ANYWHERE = pl.BlockSpec(memory_space=pltpu.HBM)
DMA = pltpu.SemaphoreType.DMA


def dot_nt(a, b):
    return lax.dot_general(a, b, (((1,), (1,)), ((), ())), preferred_element_type=F32)


def dot_nn(a, b):
    return lax.dot_general(a, b, (((1,), (0,)), ((), ())), preferred_element_type=F32)


def rows_at(start, size):
    return pl.ds(pl.multiple_of(start, size), size)


def ring(axis, size):
    me = lax.axis_index(axis)
    return me, lax.rem(me + 1, size), lax.rem(me + size - 1, size)


def meet(*peers):
    barrier = pltpu.get_barrier_semaphore()
    for peer in peers:
        pl.semaphore_signal(barrier, inc=1, device_id=peer, device_id_type=MESH)
    pl.semaphore_wait(barrier, len(peers))


def others(axis, size):
    me = lax.axis_index(axis)
    return [{axis: lax.rem(me + d, size)} for d in range(1, size)]


def beside(tp_size):
    _, right, left = ring('tp', tp_size)
    return [{'tp': right}, {'tp': left}]


def partner():
    me = lax.axis_index('cp')
    return me + 1 - 2 * lax.rem(me, 2)


def params(collective_id):
    return pltpu.CompilerParams(collective_id=collective_id, has_side_effects=True, vmem_limit_bytes=63 << 20)


def far_first(cp_size):
    return sorted(range(1, cp_size), key=lambda d: -min(d, cp_size - d))


def row_groups(tp_size, block, split_last):
    me, right, left = ring('tp', tp_size)
    far = lax.rem(me + 2, tp_size)
    half, part = block // 2, block // 4
    groups = [
        (0, half, ((me, 0), (me, half))),
        (block, half, ((right, 0), (left, half))),
        (2 * block, half, ((right, half), (left, 0))),
    ]
    if not split_last:
        return groups + [(3 * block, half, ((far, 0), (far, half)))]
    return groups + [
        (3 * block, part, ((far, 0), (far, half))),
        (3 * block + half, part, ((far, part), (far, half + part))),
    ]


def position(cp_size, tp_size, block, owner, row):
    piece = block * tp_size // 2
    first = owner < tp_size // 2
    cp_rank = lax.axis_index('cp')
    piece_id = jnp.where(first, cp_rank, 2 * cp_size - 1 - cp_rank)
    return piece_id * piece + jnp.where(first, owner, owner - tp_size // 2) * block + row


class HeadSender:
    def __init__(self, cp_size, tp_size, block, groups, res, dst, send, recv, local):
        self.cp_size, self.tp_size, self.block, self.groups = cp_size, tp_size, block, groups
        self.res, self.dst, self.sems = res, dst, (send, recv, local)

    def copies(self, g):
        send, recv, local = self.sems
        me = lax.axis_index('cp')
        start, length, parts = self.groups[g]
        for n, (owner, row) in enumerate(parts):
            rows = rows_at(position(self.cp_size, self.tp_size, self.block, owner, row), length)
            here = pl.ds(start + n * length, length)
            for d in far_first(self.cp_size):
                peer = lax.rem(me + d, self.cp_size)
                yield pltpu.make_async_remote_copy(
                    src_ref=self.res.at[peer, :, here, :], dst_ref=self.dst.at[:, rows, :],
                    send_sem=send.at[d - 1, g, n], recv_sem=recv.at[d - 1, g, n],
                    device_id={'cp': peer}, device_id_type=MESH)
            yield pltpu.make_async_copy(self.res.at[me, :, here, :], self.dst.at[:, rows, :], local.at[g, n])

    def start(self, g):
        for copy in self.copies(g):
            copy.start()

    def wait(self):
        for g in range(len(self.groups)):
            for copy in self.copies(g):
                copy.wait()


def head_scratch(cp_size, arrays, rows, groups):
    return [
        pltpu.VMEM((cp_size, arrays, rows, HEAD_DIM), BF16),
        DMA((cp_size - 1, groups, 2)),
        DMA((cp_size - 1, groups, 2)),
        DMA((groups, 2)),
    ]


def project_kernel(cp_size, tp_size, x_ref, dy_ref, wq_ref, wk_ref, wv_ref, qkv_ref, dy1_ref, w_v, xg, res, send, recv, local, w_sem, x_sem, y_send, y_recv):
    block = x_ref.shape[0]
    half, part = block // 2, block // 4
    _, right, left = ring('tp', tp_size)
    groups = row_groups(tp_size, block, True)
    heads = HeadSender(cp_size, tp_size, block, groups, res, qkv_ref, send, recv, local)

    def pass_on(k, src, dst, peer):
        copy = pltpu.make_async_remote_copy(
            src_ref=src, dst_ref=dst, send_sem=y_send.at[k], recv_sem=y_recv.at[k], device_id={'tp': peer}, device_id_type=MESH)
        copy.start()
        return copy

    def landed(start, size):
        return xg.at[pl.ds(start, size), :]

    low, high = x_ref.at[pl.ds(0, half), :], x_ref.at[pl.ds(half, half), :]
    own = pltpu.make_async_copy(x_ref, landed(0, block), x_sem)
    own.start()
    loads = [pltpu.make_async_copy(w, w_v.at[n], w_sem.at[n]) for n, w in enumerate((wq_ref, wk_ref, wv_ref))]
    meet(*others('cp', cp_size), *beside(tp_size))
    hops = [
        pass_on(0, low, landed(block, half), left),
        pass_on(1, high, landed(block + half, half), right),
        pass_on(2, high, landed(2 * block, half), left),
        pass_on(3, low, landed(2 * block + half, half), right),
    ]
    for load in loads:
        load.start()
    own.wait()

    wide = min(4, cp_size)
    cols = wide * HEAD_DIM
    steps = cp_size // wide

    def compute(g, n):
        start, length, _ = groups[g]
        rows = pl.ds(start, 2 * length)

        def body(s, _):
            out = dot_nn(xg[rows, :], w_v[n, :, rows_at(s * cols, cols)]).astype(BF16)
            for k in range(wide):
                res[wide * s + k, n, rows, :] = out[:, k * HEAD_DIM:(k + 1) * HEAD_DIM]
            return 0

        lax.fori_loop(0, steps, body, 0)

    for n in range(3):
        loads[n].wait()
        compute(0, n)
    heads.start(0)
    hops[0].wait_recv()
    hops.append(pass_on(4, landed(block, part), landed(3 * block, part), left))
    hops.append(pass_on(5, landed(block + part, part), landed(3 * block + half, part), left))
    hops[1].wait_recv()
    hops.append(pass_on(6, landed(block + half, part), landed(3 * block + part, part), right))
    hops.append(pass_on(7, landed(block + half + part, part), landed(3 * block + half + part, part), right))
    hops.append(pass_on(8, dy_ref.at[pl.ds(0, half), :], dy1_ref.at[pl.ds(0, half), :], left))
    hops.append(pass_on(9, dy_ref.at[pl.ds(half, half), :], dy1_ref.at[pl.ds(half, half), :], right))
    for g, arrived in ((1, ()), (2, (2, 3)), (3, (4, 6)), (4, (5, 7))):
        for k in arrived:
            hops[k].wait_recv()
        for n in range(3):
            compute(g, n)
        heads.start(g)
    for k in range(8):
        hops[k].wait_send()
    for k in (8, 9):
        hops[k].wait()
    heads.wait()


def project(x_blk, dy_blk, weights, cp_size, tp_size):
    block, width = x_blk.shape
    cols = weights[0].shape[1]
    seq = block * tp_size * cp_size
    return pl.pallas_call(
        functools.partial(project_kernel, cp_size, tp_size),
        out_shape=(jax.ShapeDtypeStruct((3, seq, HEAD_DIM), BF16), jax.ShapeDtypeStruct((block, width), BF16)),
        in_specs=[ANYWHERE] * 5,
        out_specs=(ANYWHERE, ANYWHERE),
        scratch_shapes=[pltpu.VMEM((3, width, cols), BF16), pltpu.VMEM((4 * block, width), BF16)]
        + head_scratch(cp_size, 3, 4 * block, 5) + [DMA((3,)), DMA, DMA((10,)), DMA((10,))],
        compiler_params=params(0),
        cost_estimate=pl.CostEstimate(flops=6 * block * tp_size * width * cols, bytes_accessed=6 * width * cols, transcendentals=0),
        name="project_qkv",
    )(x_blk, dy_blk, *weights)


def send_piece(cp_size, i, src, dst_of, send, recv, local, start):
    me = lax.axis_index('cp')
    half = jnp.where(i < cp_size, 0, 1)
    owner = jnp.where(i < cp_size, i, 2 * cp_size - 1 - i)

    @pl.when(owner == me)
    def _():
        copy = pltpu.make_async_copy(src, dst_of(half, me), local.at[half])
        copy.start() if start else copy.wait()

    @pl.when(owner != me)
    def _():
        copy = pltpu.make_async_remote_copy(
            src_ref=src, dst_ref=dst_of(half, me), send_sem=send.at[i], recv_sem=recv.at[me, half],
            device_id={'cp': owner}, device_id_type=MESH)
        copy.start() if start else copy.wait_send()


def wait_pieces(cp_size, src_of, dst_of, send, recv, local):
    me = lax.axis_index('cp')

    def sent(i, _):
        send_piece(cp_size, i, src_of(i), dst_of, send, recv, local, False)
        return 0

    lax.fori_loop(0, 2 * cp_size, sent, 0)
    for d in range(1, cp_size):
        peer = lax.rem(me + d, cp_size)
        for half in range(2):
            pltpu.make_async_remote_copy(
                src_ref=src_of(0), dst_ref=dst_of(half, peer), send_sem=send.at[0], recv_sem=recv.at[peer, half],
                device_id={'cp': peer}, device_id_type=MESH).wait_recv()


def forward_kernel(cp_size, tp_size, qkv_ref, dy_ref, dy1_ref, wo_ref, o_ref, l_ref, rows_ref, do_ref,
                   qkv, o_v, l_v, vt_ref, s_ref, acc_ref, dyg, wo, res, h_send, h_recv, h_local,
                   in_sem, send, recv, local, y_send, y_recv, out_sem):
    seq = qkv.shape[1]
    bq = s_ref.shape[0]
    nblk = seq // bq
    c = HEAD_DIM ** -0.5 * LOG2E
    _, right, left = ring('tp', tp_size)
    block = dy_ref.shape[0]
    half = block // 2
    low, high = pl.ds(0, half), pl.ds(half, half)
    groups = row_groups(tp_size, block, False)
    heads = HeadSender(cp_size, tp_size, block, groups, res, do_ref, h_send, h_recv, h_local)

    loads = [
        pltpu.make_async_copy(dy_ref, dyg.at[pl.ds(0, block), :], in_sem.at[0]),
        pltpu.make_async_copy(dy1_ref, dyg.at[pl.ds(block, block), :], in_sem.at[1]),
        pltpu.make_async_copy(wo_ref, wo, in_sem.at[2]),
        pltpu.make_async_copy(qkv_ref, qkv, in_sem.at[3]),
    ]
    for load in loads:
        load.start()
    meet(*others('cp', cp_size), *beside(tp_size))
    hops = []
    for k, (src, start, peer) in enumerate((
            (dy_ref.at[high, :], 2 * block, left),
            (dy_ref.at[low, :], 2 * block + half, right),
            (dy1_ref.at[low, :], 3 * block, left),
            (dy1_ref.at[high, :], 3 * block + half, right))):
        hop = pltpu.make_async_remote_copy(
            src_ref=src, dst_ref=dyg.at[pl.ds(start, half), :], send_sem=y_send.at[k], recv_sem=y_recv.at[k],
            device_id={'tp': peer}, device_id_type=MESH)
        hop.start()
        hops.append(hop)

    per_step = min(4, cp_size)
    cols = per_step * HEAD_DIM

    def compute(g):
        rows = pl.ds(groups[g][0], block)

        def body(s, _):
            out = dot_nt(dyg[rows, :], wo[rows_at(s * cols, cols), :]).astype(BF16)
            for k in range(per_step):
                res[per_step * s + k, 0, rows, :] = out[:, k * HEAD_DIM:(k + 1) * HEAD_DIM]
            return 0

        lax.fori_loop(0, cp_size // per_step, body, 0)
        heads.start(g)

    for load in loads[:3]:
        load.wait()
    compute(0)
    compute(1)
    loads[3].wait()

    def transpose_step(b, _):
        rows = rows_at(b * bq, bq)
        vt_ref[:, rows] = qkv[2, rows, :].T
        return 0

    lax.fori_loop(0, nblk, transpose_step, 0)

    def src_of(i):
        return o_v.at[rows_at(i * bq, bq), :]

    def dst_of(part, head):
        return rows_ref.at[rows_at(part * bq, bq), rows_at(head * HEAD_DIM, HEAD_DIM)]

    def q_step(i, _):
        @pl.when(i == nblk - 2)
        def _():
            for hop in hops:
                hop.wait()
            compute(2)
            compute(3)

        rows = rows_at(i * bq, bq)
        q = qkv[0, rows, :]
        acc_ref[...] = jnp.zeros_like(acc_ref)
        s = dot_nt(qkv[1, rows, :], q)
        kk = lax.broadcasted_iota(jnp.int32, (bq, bq), 0)
        qq = lax.broadcasted_iota(jnp.int32, (bq, bq), 1)
        s = jnp.where(kk <= qq, s, -jnp.inf)
        s_ref[...] = s
        first = jnp.max(s, axis=0, keepdims=True)

        def use(blk, m_old, m, l, following):
            mc = m * c
            alpha = jnp.exp2(m_old * c - mc)
            p = jnp.exp2(s_ref[...] * c - mc)
            m_new = m
            if following is not None:
                s = dot_nt(qkv[1, rows_at(following * bq, bq), :], q)
            part = jnp.sum(p, axis=0, keepdims=True)
            out = dot_nn(vt_ref[:, rows_at(blk * bq, bq)], p.astype(BF16))
            if following is not None:
                m_new = jnp.maximum(m, jnp.max(s, axis=0, keepdims=True))
                s_ref[...] = s
            acc_ref[...] = acc_ref[...] * alpha + out
            return m, m_new, l * alpha + part

        def body(t, carry):
            return use(jnp.where(t == 0, i, t - 1), *carry, t)

        carry = lax.fori_loop(0, i, body, (first, first, jnp.zeros((1, bq), F32)))
        m, _, l = use(jnp.where(i == 0, i, i - 1), *carry, None)
        o_v[rows, :] = (acc_ref[...] * (1.0 / l)).T.astype(BF16)
        l_v[i] = jnp.broadcast_to(m * c + jnp.log2(l), (8, bq))
        send_piece(cp_size, i, src_of(i), dst_of, send, recv, local, True)
        return 0

    lax.fori_loop(0, nblk, q_step, 0)
    out_o = pltpu.make_async_copy(o_v, o_ref, out_sem.at[0])
    out_l = pltpu.make_async_copy(l_v, l_ref, out_sem.at[1])
    out_o.start()
    out_l.start()
    wait_pieces(cp_size, src_of, dst_of, send, recv, local)
    heads.wait()
    out_o.wait()
    out_l.wait()


def forward(qkv, dy_blk, dy1, w_out, cp_size, tp_size):
    seq = qkv.shape[1]
    bq = seq // (2 * cp_size)
    block, width = dy_blk.shape
    cols = w_out.shape[0]
    pairs = seq * seq // 2
    return pl.pallas_call(
        functools.partial(forward_kernel, cp_size, tp_size),
        out_shape=(
            jax.ShapeDtypeStruct((seq, HEAD_DIM), BF16),
            jax.ShapeDtypeStruct((seq // bq, 8, bq), F32),
            jax.ShapeDtypeStruct((2 * bq, cp_size * HEAD_DIM), BF16),
            jax.ShapeDtypeStruct((1, seq, HEAD_DIM), BF16),
        ),
        in_specs=[ANYWHERE] * 4,
        out_specs=(ANYWHERE,) * 4,
        scratch_shapes=[
            pltpu.VMEM((3, seq, HEAD_DIM), BF16),
            pltpu.VMEM((seq, HEAD_DIM), BF16),
            pltpu.VMEM((seq // bq, 8, bq), F32),
            pltpu.VMEM((HEAD_DIM, seq), BF16),
            pltpu.VMEM((bq, bq), F32),
            pltpu.VMEM((HEAD_DIM, bq), F32),
            pltpu.VMEM((4 * block, width), BF16),
            pltpu.VMEM((cols, width), BF16),
        ] + head_scratch(cp_size, 1, 4 * block, 4) + [
            DMA((4,)), DMA((2 * cp_size,)), DMA((cp_size, 2)), DMA((2,)), DMA((4,)), DMA((4,)), DMA((2,)),
        ],
        compiler_params=params(1),
        cost_estimate=pl.CostEstimate(flops=4 * pairs * HEAD_DIM, bytes_accessed=8 * seq * HEAD_DIM, transcendentals=pairs),
        name="attention_forward",
    )(qkv, dy_blk, dy1, w_out)


def backward_kernel(cp_size, tp_size, qkv_ref, do_ref, o_ref, l_ref, o_rows_ref, wo_ref, rows_ref, oy_ref, wy_ref, wx_ref,
                    qkv, do_v, o_v, l_v, kt_ref, p_ref, ds_ref, dst_ref, qt_ref, dot_ref, dqt_ref, dk_acc, dv_acc, grads,
                    in_sem, send, recv, local, y_send, y_recv, x_send, x_recv):
    seq = qkv.shape[1]
    bq = p_ref.shape[0]
    nblk = seq // bq
    sub = bq // 2
    scale = HEAD_DIM ** -0.5
    c = scale * LOG2E
    loads = [
        pltpu.make_async_copy(qkv_ref, qkv, in_sem.at[0]),
        pltpu.make_async_copy(do_ref.at[0], do_v, in_sem.at[1]),
        pltpu.make_async_copy(o_ref, o_v, in_sem.at[2]),
        pltpu.make_async_copy(l_ref, l_v, in_sem.at[3]),
    ]
    for load in loads:
        load.start()
    meet(*others('cp', cp_size), *others('tp', tp_size))
    me_c, me_t = lax.axis_index('cp'), lax.axis_index('tp')
    share = wy_ref.shape[1]
    block = oy_ref.shape[1]
    y_hops = []
    for r in range(1, tp_size):
        peer = lax.rem(me_t + r, tp_size)
        y_hops.append((wo_ref.at[rows_at(me_c * share, share), :], wy_ref.at[r - 1], peer))
    for r in range(1, tp_size):
        peer = lax.rem(me_t + r, tp_size)
        y_hops.append((o_rows_ref.at[rows_at(peer * block, block), :], oy_ref.at[r - 1], peer))
    y_hops = [
        pltpu.make_async_remote_copy(
            src_ref=src, dst_ref=dst, send_sem=y_send.at[k], recv_sem=y_recv.at[k], device_id={'tp': peer}, device_id_type=MESH)
        for k, (src, dst, peer) in enumerate(y_hops)]
    x_hops = [
        pltpu.make_async_remote_copy(
            src_ref=wy_ref.at[0], dst_ref=wx_ref.at[k - 1], send_sem=x_send.at[k - 1], recv_sem=x_recv.at[k - 1],
            device_id={'cp': lax.rem(me_c + 2 * k, cp_size)}, device_id_type=MESH)
        for k in range(1, cp_size // 2)]
    for hop in y_hops:
        hop.start()
    for load in loads:
        load.wait()

    def init_step(b, _):
        rows = rows_at(b * bq, bq)
        kt_ref[:, rows] = qkv[1, rows, :].T
        dk_acc[:, rows] = jnp.zeros((HEAD_DIM, bq), F32)
        dv_acc[:, rows] = jnp.zeros((HEAD_DIM, bq), F32)
        return 0

    lax.fori_loop(0, nblk, init_step, 0)

    def src_of(i):
        return grads.at[:, rows_at(i * bq, bq), :]

    def dst_of(part, head):
        return rows_ref.at[:, rows_at(part * bq, bq), rows_at(head * HEAD_DIM, HEAD_DIM)]

    def q_step(back, _):
        i = nblk - 1 - back
        rows = rows_at(i * bq, bq)
        q = qkv[0, rows, :]
        do = do_v[rows, :]
        prod = do.astype(F32) * o_v[rows, :].astype(F32)
        delta = jnp.sum(prod.T, axis=0, keepdims=True)
        lse = l_v[i][0:1, :]
        dqt_ref[...] = jnp.zeros_like(dqt_ref)
        qt_ref[...] = q.T
        dot_ref[...] = do.T

        @pl.when(back == 3)
        def _():
            y_hops[0].wait_recv()
            for hop in x_hops:
                hop.start()

        def make(blk, r, masked):
            krows = rows_at(blk * bq + r * sub, sub)
            s = dot_nt(qkv[1, krows, :], q)
            dp = dot_nt(qkv[2, krows, :], do)
            p = jnp.exp2(s * c - lse)
            if masked:
                kk = lax.broadcasted_iota(jnp.int32, (sub, bq), 0) + r * sub
                qq = lax.broadcasted_iota(jnp.int32, (sub, bq), 1)
                p = jnp.where(kk <= qq, p, 0.0)
            pb = p.astype(BF16)
            ds = (pb.astype(F32) * (dp - delta)).astype(BF16)
            return pb.T, ds, ds.T

        def put(r, made):
            sl = slice(r * sub, (r + 1) * sub)
            p_ref[:, sl], ds_ref[sl, :], dst_ref[:, sl] = made

        def take(r):
            sl = slice(r * sub, (r + 1) * sub)
            return p_ref[:, sl], ds_ref[sl, :], dst_ref[:, sl]

        def flush(blk, r, p, ds_t, ds):
            krows = rows_at(blk * bq + r * sub, sub)
            dv_acc[:, krows] += dot_nn(dot_ref[...], p)
            dk_acc[:, krows] += dot_nn(qt_ref[...], ds)
            return dot_nn(kt_ref[:, krows], ds_t)

        for r in range(2):
            put(r, make(i, r, True))

        def body(t, _):
            cur = jnp.where(t == 0, i, t - 1)
            out = None
            for r in range(2):
                old = take(r)
                new = make(t, r, False)
                d = flush(cur, r, *old)
                out = d if out is None else out + d
                put(r, new)
            dqt_ref[...] += out
            return 0

        lax.fori_loop(0, i, body, 0)
        cur = jnp.where(i == 0, i, i - 1)
        out = flush(cur, 0, *take(0)) + flush(cur, 1, *take(1))
        grads[0, rows, :] = ((dqt_ref[...] + out) * scale).T.astype(BF16)
        grads[1, rows, :] = (dk_acc[:, rows] * scale).T.astype(BF16)
        grads[2, rows, :] = dv_acc[:, rows].T.astype(BF16)
        send_piece(cp_size, i, src_of(i), dst_of, send, recv, local, True)
        return 0

    lax.fori_loop(0, nblk, q_step, 0)
    wait_pieces(cp_size, src_of, dst_of, send, recv, local)
    for k, hop in enumerate(y_hops):
        hop.wait_send() if k == 0 else hop.wait()
    for hop in x_hops:
        hop.wait()


def backward(qkv, do, o, lse, o_rows, w_out, cp_size, tp_size):
    seq = qkv.shape[1]
    cols, width = w_out.shape
    block = o_rows.shape[0] // tp_size
    share = cols // cp_size
    bq = seq // (2 * cp_size)
    pairs = seq * seq // 2
    return pl.pallas_call(
        functools.partial(backward_kernel, cp_size, tp_size),
        out_shape=(
            jax.ShapeDtypeStruct((3, 2 * bq, cp_size * HEAD_DIM), BF16),
            jax.ShapeDtypeStruct((tp_size - 1, block, cols), BF16),
            jax.ShapeDtypeStruct((tp_size - 1, share, width), BF16),
            jax.ShapeDtypeStruct((max(1, cp_size // 2 - 1), share, width), BF16),
        ),
        in_specs=[ANYWHERE] * 6,
        out_specs=(ANYWHERE,) * 4,
        scratch_shapes=[
            pltpu.VMEM((3, seq, HEAD_DIM), BF16),
            pltpu.VMEM((seq, HEAD_DIM), BF16),
            pltpu.VMEM((seq, HEAD_DIM), BF16),
            pltpu.VMEM((seq // bq, 8, bq), F32),
            pltpu.VMEM((HEAD_DIM, seq), BF16),
            pltpu.VMEM((bq, bq), BF16),
            pltpu.VMEM((bq, bq), BF16),
            pltpu.VMEM((bq, bq), BF16),
            pltpu.VMEM((HEAD_DIM, bq), BF16),
            pltpu.VMEM((HEAD_DIM, bq), BF16),
            pltpu.VMEM((HEAD_DIM, bq), F32),
            pltpu.VMEM((HEAD_DIM, seq), F32),
            pltpu.VMEM((HEAD_DIM, seq), F32),
            pltpu.VMEM((3, seq, HEAD_DIM), BF16),
            DMA((4,)), DMA((2 * cp_size,)), DMA((cp_size, 2)), DMA((2,)), DMA((6,)), DMA((6,)), DMA((cp_size,)), DMA((cp_size,)),
        ],
        compiler_params=params(2),
        cost_estimate=pl.CostEstimate(flops=10 * pairs * HEAD_DIM, bytes_accessed=16 * seq * HEAD_DIM, transcendentals=pairs),
        name="attention_backward",
    )(qkv, do, o, lse, o_rows, w_out)


def reduce_kernel(cp_size, tp_size, chunks, rows_ref, wq_ref, wk_ref, wv_ref, o_rows_ref, oy_ref, wo_ref, wy_ref, wx_ref,
                  out_ref, y_ref, wx2_ref, sib_ref,
                  g_v, w_v, part, mid, last, out_v, stage, y_acc, o_v, in_sem, w_sem, out_sem, sends, recvs,
                  x_send, x_recv, d_send, d_recv, o_sem, s_sem):
    me, right, left = ring('tp', tp_size)
    far = lax.rem(me + 2, tp_size)
    block = part.shape[1]
    half = block // 2
    low, high = pl.ds(0, half), pl.ds(half, half)
    wide = part.shape[2] // chunks
    weights = (wq_ref, wk_ref, wv_ref)

    def w_load(n, a):
        return pltpu.make_async_copy(weights[a].at[rows_at(n * wide, wide), :], w_v.at[lax.rem(n, 2), a], w_sem.at[lax.rem(n, 2), a])

    load = pltpu.make_async_copy(rows_ref, g_v, in_sem)
    load.start()
    for a in range(3):
        w_load(0, a).start()
    me_c, mate = lax.axis_index('cp'), partner()
    steps = range(1, cp_size // 2)
    meet(*beside(tp_size), {'cp': mate}, *({'cp': lax.rem(me_c + 2 * k, cp_size)} for k in steps))

    def share_ref(s, k):
        if k == 0:
            return wy_ref.at[s]
        return wx_ref.at[k - 1] if s == 0 else wx2_ref.at[s - 1, k - 1]

    def along(s, k):
        return pltpu.make_async_remote_copy(
            src_ref=wy_ref.at[s], dst_ref=wx2_ref.at[s - 1, k - 1], send_sem=x_send.at[s - 1, k - 1], recv_sem=x_recv.at[s - 1, k - 1],
            device_id={'cp': lax.rem(me_c + 2 * k, cp_size)}, device_id_type=MESH)

    def across(s, k):
        return pltpu.make_async_remote_copy(
            src_ref=share_ref(s, k), dst_ref=sib_ref.at[s, k], send_sem=d_send.at[s, k], recv_sem=d_recv.at[s, k],
            device_id={'cp': mate}, device_id_type=MESH)

    for s in range(1, tp_size - 1):
        for k in steps:
            along(s, k).start()
    for s in range(tp_size - 1):
        across(s, 0).start()
    for k in steps:
        across(0, k).start()
    o_loads = [pltpu.make_async_copy(o_rows_ref.at[rows_at(me * (o_rows_ref.shape[0] // tp_size), o_rows_ref.shape[0] // tp_size), :], o_v.at[0], o_sem.at[0])]
    for s in range(tp_size - 1):
        o_loads.append(pltpu.make_async_copy(oy_ref.at[s], o_v.at[s + 1], o_sem.at[s + 1]))
    for copy in o_loads:
        copy.start()

    def hop(kind, n):
        cols = rows_at(n * wide, wide)
        src, dst, peer = {
            'far_r': (part.at[0, low, cols], mid.at[0, :, cols], right),
            'far_l': (part.at[0, high, cols], mid.at[1, :, cols], left),
            'plain_r': (part.at[1, high, cols], last.at[0, high, cols], right),
            'plain_l': (part.at[2, low, cols], last.at[1, low, cols], left),
            'sum_r': (part.at[1, low, cols], last.at[0, low, cols], right),
            'sum_l': (part.at[2, high, cols], last.at[1, high, cols], left),
        }[kind]
        k = ('far_r', 'far_l', 'plain_r', 'plain_l', 'sum_r', 'sum_l').index(kind)
        return pltpu.make_async_remote_copy(
            src_ref=src, dst_ref=dst, send_sem=sends.at[k, n], recv_sem=recvs.at[k, n], device_id={'tp': peer}, device_id_type=MESH)

    load.wait()
    owners = (far, right, left, me)

    def compute(n, _):
        slot = lax.rem(n, 2)

        @pl.when(n + 1 < chunks)
        def _():
            for a in range(3):
                w_load(n + 1, a).start()

        for a in range(3):
            w_load(n, a).wait()
        cols = rows_at(n * wide, wide)
        for k in range(4):
            rows = rows_at(owners[k] * block, block)
            total = dot_nt(g_v[0, rows, :], w_v[slot, 0])
            total = total + dot_nt(g_v[1, rows, :], w_v[slot, 1])
            part[k, :, cols] = total + dot_nt(g_v[2, rows, :], w_v[slot, 2])
        for kind in ('far_r', 'far_l', 'plain_r', 'plain_l'):
            hop(kind, n).start()
        return 0

    lax.fori_loop(0, chunks, compute, 0)

    def forward_sums(n, _):
        cols = rows_at(n * wide, wide)
        hop('far_r', n).wait_recv()
        part[1, :half, cols] += mid[0, :, cols]
        hop('sum_r', n).start()
        hop('far_l', n).wait_recv()
        part[2, half:, cols] += mid[1, :, cols]
        hop('sum_l', n).start()
        return 0

    lax.fori_loop(0, chunks, forward_sums, 0)

    for s in range(1, tp_size - 1):
        for k in steps:
            along(s, k).wait_recv()
            across(s, k).start()
    for copy in o_loads:
        copy.wait()
    share = wy_ref.shape[1]
    span = stage.shape[2]
    halves = y_acc.shape[1] // span

    def stage_copies(n):
        s, h = divmod(n, halves)
        cols = pl.ds(h * span, span)
        slot = n % 2
        if s == 0:
            return [pltpu.make_async_copy(wo_ref.at[:, cols], stage.at[slot], s_sem.at[slot, 0])]
        copies = []
        for k in range(cp_size // 2):
            mine, its = lax.rem(me_c + cp_size - 2 * k, cp_size), lax.rem(mate + cp_size - 2 * k, cp_size)
            copies.append(pltpu.make_async_copy(
                share_ref(s - 1, k).at[:, cols], stage.at[slot, rows_at(mine * share, share), :], s_sem.at[slot, 2 * k]))
            copies.append(pltpu.make_async_copy(
                sib_ref.at[s - 1, k, :, cols], stage.at[slot, rows_at(its * share, share), :], s_sem.at[slot, 2 * k + 1]))
        return copies

    def stage_start(n):
        s, h = divmod(n, halves)
        if s > 0 and h == 0:
            for k in range(cp_size // 2):
                across(s - 1, k).wait_recv()
        for copy in stage_copies(n):
            copy.start()

    total_steps = tp_size * halves
    stage_start(0)
    for n in range(total_steps):
        if n + 1 < total_steps:
            stage_start(n + 1)
        for copy in stage_copies(n):
            copy.wait()
        s, h = divmod(n, halves)
        tile = min(512, span)

        def y_step(j, _):
            cols = rows_at(j * tile, tile)
            out = rows_at(h * span + j * tile, tile)
            product = dot_nn(o_v[s], stage[n % 2, :, cols])
            if s == 0:
                y_acc[:, out] = product
            elif s < tp_size - 1:
                y_acc[:, out] += product
            else:
                out_v[:, out] = (y_acc[:, out] + product).astype(BF16)
            return 0

        lax.fori_loop(0, span // tile, y_step, 0)
    y_out = pltpu.make_async_copy(out_v, y_ref, in_sem)
    y_out.start()
    y_out.wait()

    def put(n):
        cols = rows_at(n * wide, wide)
        return pltpu.make_async_copy(out_v.at[:, cols], out_ref.at[:, cols], out_sem.at[n])

    def finish(n, _):
        cols = rows_at(n * wide, wide)
        for kind in ('plain_r', 'plain_l', 'sum_r', 'sum_l'):
            hop(kind, n).wait_recv()
        out_v[:, cols] = (part[3, :, cols] + last[0, :, cols] + last[1, :, cols]).astype(BF16)
        put(n).start()
        return 0

    lax.fori_loop(0, chunks, finish, 0)

    def close(n, _):
        put(n).wait()
        for kind in ('far_r', 'far_l', 'plain_r', 'plain_l', 'sum_r', 'sum_l'):
            hop(kind, n).wait_send()
        return 0

    lax.fori_loop(0, chunks, close, 0)
    for s in range(tp_size - 1):
        for k in range(cp_size // 2):
            across(s, k).wait_send()
            if s > 0 and k > 0:
                along(s, k).wait_send()


def reduce_out(grad_rows, weights, o_rows, oy, w_out, wy, wx, cp_size, tp_size):
    width, cols = weights[0].shape
    share = wy.shape[1]
    pairs = cp_size // 2
    rows = grad_rows.shape[1]
    block = rows // tp_size
    chunks = 8
    wide = width // chunks
    return pl.pallas_call(
        functools.partial(reduce_kernel, cp_size, tp_size, chunks),
        out_shape=(
            jax.ShapeDtypeStruct((block, width), BF16),
            jax.ShapeDtypeStruct((block, width), BF16),
            jax.ShapeDtypeStruct((tp_size - 2, max(1, pairs - 1), share, width), BF16),
            jax.ShapeDtypeStruct((tp_size - 1, pairs, share, width), BF16),
        ),
        in_specs=[ANYWHERE] * 9,
        out_specs=(ANYWHERE,) * 4,
        scratch_shapes=[
            pltpu.VMEM((3, rows, cols), BF16),
            pltpu.VMEM((2, 3, wide, cols), BF16),
            pltpu.VMEM((4, block, width), F32),
            pltpu.VMEM((2, block // 2, width), F32),
            pltpu.VMEM((2, block, width), F32),
            pltpu.VMEM((block, width), BF16),
            pltpu.VMEM((2, cols, width // 2), BF16),
            pltpu.VMEM((block, width), F32),
            pltpu.VMEM((tp_size, block, cols), BF16),
            DMA, DMA((2, 3)), DMA((chunks,)), DMA((6, chunks)), DMA((6, chunks)),
            DMA((tp_size - 2, pairs)), DMA((tp_size - 2, pairs)), DMA((tp_size - 1, pairs)), DMA((tp_size - 1, pairs)),
            DMA((tp_size,)), DMA((2, cp_size)),
        ],
        compiler_params=params(3),
        cost_estimate=pl.CostEstimate(flops=6 * rows * width * cols, bytes_accessed=6 * width * cols, transcendentals=0),
        name="project_reduce",
    )(grad_rows, *weights, o_rows, oy, w_out, wy, wx)


def solution(mesh):
    cp_size, tp_size = mesh.shape['cp'], mesh.shape['tp']
    row_spec = P(('dp', 'cp', 'tp'), None)

    def local_step(x_blk, dy_blk, w_query, w_key, w_value, w_out):
        weights = (w_query, w_key, w_value)
        qkv, dy1 = project(x_blk, dy_blk, weights, cp_size, tp_size)
        o, lse, o_rows, do = forward(qkv, dy_blk, dy1, w_out, cp_size, tp_size)
        grad_rows, oy, wy, wx = backward(qkv, do, o, lse, o_rows, w_out, cp_size, tp_size)
        dx_blk, y_blk, _, _ = reduce_out(grad_rows, weights, o_rows, oy, w_out, wy, wx, cp_size, tp_size)
        return y_blk, dx_blk

    weight = P(None, 'tp')
    return jax.shard_map(local_step, mesh=mesh, in_specs=(row_spec, row_spec, weight, weight, weight, P('tp', None)), out_specs=(row_spec, row_spec), check_vma=False)
```

```python
import functools
import math

import jax
import jax.numpy as jnp
from jax import lax
from jax.experimental import pallas as pl
from jax.experimental.pallas import tpu as pltpu
from jax.sharding import PartitionSpec as P

HEAD_DIM = 128
F32, BF16 = jnp.float32, jnp.bfloat16
LOG2E = math.log2(math.e)
MESH = pl.DeviceIdType.MESH
ANYWHERE = pl.BlockSpec(memory_space=pltpu.HBM)
DMA = pltpu.SemaphoreType.DMA
FAR, RIGHT, LEFT, OWN = range(4)


def dot_nt(a, b):
    return lax.dot_general(a, b, (((1,), (1,)), ((), ())), preferred_element_type=F32)


def dot_nn(a, b):
    return lax.dot_general(a, b, (((1,), (0,)), ((), ())), preferred_element_type=F32)


def rows_at(start, size):
    return pl.ds(pl.multiple_of(start, size), size)


def ring(axis, size):
    me = lax.axis_index(axis)
    return me, lax.rem(me + 1, size), lax.rem(me + size - 1, size)


def meet(*peers):
    barrier = pltpu.get_barrier_semaphore()
    for peer in peers:
        pl.semaphore_signal(barrier, inc=1, device_id=peer, device_id_type=MESH)
    pl.semaphore_wait(barrier, len(peers))


def others(axis, size):
    me = lax.axis_index(axis)
    return [{axis: lax.rem(me + d, size)} for d in range(1, size)]


def beside(tp_size):
    _, right, left = ring('tp', tp_size)
    return [{'tp': right}, {'tp': left}]


def partner():
    me = lax.axis_index('cp')
    return me + 1 - 2 * lax.rem(me, 2)


def params(collective_id):
    return pltpu.CompilerParams(collective_id=collective_id, has_side_effects=True, vmem_limit_bytes=63 << 20)


def far_first(cp_size):
    return sorted(range(1, cp_size), key=lambda d: -min(d, cp_size - d))


def row_groups(tp_size, block, split_last):
    me, right, left = ring('tp', tp_size)
    far = lax.rem(me + 2, tp_size)
    half, part = block // 2, block // 4
    groups = [
        (0, half, ((me, 0), (me, half))),
        (block, half, ((right, 0), (left, half))),
        (2 * block, half, ((right, half), (left, 0))),
    ]
    if not split_last:
        return groups + [(3 * block, half, ((far, 0), (far, half)))]
    return groups + [
        (3 * block, part, ((far, 0), (far, half))),
        (3 * block + half, part, ((far, part), (far, half + part))),
    ]


def position(cp_size, tp_size, block, owner, row):
    piece = block * tp_size // 2
    first = owner < tp_size // 2
    cp_rank = lax.axis_index('cp')
    piece_id = jnp.where(first, cp_rank, 2 * cp_size - 1 - cp_rank)
    return piece_id * piece + jnp.where(first, owner, owner - tp_size // 2) * block + row


class HeadSender:
    def __init__(self, cp_size, tp_size, block, groups, res, dst, send, recv, local):
        self.cp_size, self.tp_size, self.block, self.groups = cp_size, tp_size, block, groups
        self.res, self.dst, self.sems = res, dst, (send, recv, local)

    def copies(self, g):
        send, recv, local = self.sems
        me = lax.axis_index('cp')
        start, length, parts = self.groups[g]
        for n, (owner, row) in enumerate(parts):
            rows = rows_at(position(self.cp_size, self.tp_size, self.block, owner, row), length)
            here = pl.ds(start + n * length, length)
            for d in far_first(self.cp_size):
                peer = lax.rem(me + d, self.cp_size)
                yield pltpu.make_async_remote_copy(
                    src_ref=self.res.at[peer, :, here, :], dst_ref=self.dst.at[:, rows, :],
                    send_sem=send.at[d - 1, g, n], recv_sem=recv.at[d - 1, g, n],
                    device_id={'cp': peer}, device_id_type=MESH)
            yield pltpu.make_async_copy(self.res.at[me, :, here, :], self.dst.at[:, rows, :], local.at[g, n])

    def start(self, g):
        for copy in self.copies(g):
            copy.start()

    def wait(self):
        for g in range(len(self.groups)):
            for copy in self.copies(g):
                copy.wait()


def head_scratch(cp_size, arrays, rows, groups):
    return [
        pltpu.VMEM((cp_size, arrays, rows, HEAD_DIM), BF16),
        DMA((cp_size - 1, groups, 2)),
        DMA((cp_size - 1, groups, 2)),
        DMA((groups, 2)),
    ]


def project_kernel(cp_size, tp_size, x_ref, dy_ref, wq_ref, wk_ref, wv_ref, qkv_ref, dy1_ref, w_v, xg, res, send, recv, local, w_sem, x_sem, y_send, y_recv):
    block = x_ref.shape[0]
    half, part = block // 2, block // 4
    _, right, left = ring('tp', tp_size)
    groups = row_groups(tp_size, block, True)
    heads = HeadSender(cp_size, tp_size, block, groups, res, qkv_ref, send, recv, local)

    def pass_on(k, src, dst, peer):
        copy = pltpu.make_async_remote_copy(
            src_ref=src, dst_ref=dst, send_sem=y_send.at[k], recv_sem=y_recv.at[k], device_id={'tp': peer}, device_id_type=MESH)
        copy.start()
        return copy

    def landed(start, size):
        return xg.at[pl.ds(start, size), :]

    low, high = x_ref.at[pl.ds(0, half), :], x_ref.at[pl.ds(half, half), :]
    own = pltpu.make_async_copy(x_ref, landed(0, block), x_sem)
    own.start()
    loads = [pltpu.make_async_copy(w, w_v.at[n], w_sem.at[n]) for n, w in enumerate((wq_ref, wk_ref, wv_ref))]
    meet(*others('cp', cp_size), *beside(tp_size))
    hops = [
        pass_on(0, low, landed(block, half), left),
        pass_on(1, high, landed(block + half, half), right),
        pass_on(2, high, landed(2 * block, half), left),
        pass_on(3, low, landed(2 * block + half, half), right),
    ]
    for load in loads:
        load.start()
    own.wait()

    wide = min(4, cp_size)
    cols = wide * HEAD_DIM
    steps = cp_size // wide

    def compute(g, n):
        start, length, _ = groups[g]
        rows = pl.ds(start, 2 * length)

        def body(s, _):
            out = dot_nn(xg[rows, :], w_v[n, :, rows_at(s * cols, cols)]).astype(BF16)
            for k in range(wide):
                res[wide * s + k, n, rows, :] = out[:, k * HEAD_DIM:(k + 1) * HEAD_DIM]
            return 0

        lax.fori_loop(0, steps, body, 0)

    for n in range(3):
        loads[n].wait()
        compute(0, n)
    heads.start(0)
    hops[0].wait_recv()
    hops.append(pass_on(4, landed(block, part), landed(3 * block, part), left))
    hops.append(pass_on(5, landed(block + part, part), landed(3 * block + half, part), left))
    hops[1].wait_recv()
    hops.append(pass_on(6, landed(block + half, part), landed(3 * block + part, part), right))
    hops.append(pass_on(7, landed(block + half + part, part), landed(3 * block + half + part, part), right))
    hops.append(pass_on(8, dy_ref.at[pl.ds(0, part), :], dy1_ref.at[pl.ds(0, part), :], left))
    hops.append(pass_on(9, dy_ref.at[pl.ds(half, part), :], dy1_ref.at[pl.ds(part, part), :], right))
    for g, arrived in ((1, ()), (2, (2, 3)), (3, (4, 6)), (4, (5, 7))):
        for k in arrived:
            hops[k].wait_recv()
        for n in range(3):
            compute(g, n)
        heads.start(g)
    for k in range(8):
        hops[k].wait_send()
    for k in (8, 9):
        hops[k].wait()
    heads.wait()


def project(x_blk, dy_blk, weights, cp_size, tp_size):
    block, width = x_blk.shape
    cols = weights[0].shape[1]
    seq = block * tp_size * cp_size
    return pl.pallas_call(
        functools.partial(project_kernel, cp_size, tp_size),
        out_shape=(jax.ShapeDtypeStruct((3, seq, HEAD_DIM), BF16), jax.ShapeDtypeStruct((block // 2, width), BF16)),
        in_specs=[ANYWHERE] * 5,
        out_specs=(ANYWHERE, ANYWHERE),
        scratch_shapes=[pltpu.VMEM((3, width, cols), BF16), pltpu.VMEM((4 * block, width), BF16)]
        + head_scratch(cp_size, 3, 4 * block, 5) + [DMA((3,)), DMA, DMA((10,)), DMA((10,))],
        compiler_params=params(0),
        cost_estimate=pl.CostEstimate(flops=6 * block * tp_size * width * cols, bytes_accessed=6 * width * cols, transcendentals=0),
        name="project_qkv",
    )(x_blk, dy_blk, *weights)


def send_piece(cp_size, i, src, dst_of, send, recv, local, start):
    me = lax.axis_index('cp')
    half = jnp.where(i < cp_size, 0, 1)
    owner = jnp.where(i < cp_size, i, 2 * cp_size - 1 - i)

    @pl.when(owner == me)
    def _():
        copy = pltpu.make_async_copy(src, dst_of(half, me), local.at[half])
        copy.start() if start else copy.wait()

    @pl.when(owner != me)
    def _():
        copy = pltpu.make_async_remote_copy(
            src_ref=src, dst_ref=dst_of(half, me), send_sem=send.at[i], recv_sem=recv.at[me, half],
            device_id={'cp': owner}, device_id_type=MESH)
        copy.start() if start else copy.wait_send()


def wait_pieces(cp_size, src_of, dst_of, send, recv, local):
    me = lax.axis_index('cp')

    def sent(i, _):
        send_piece(cp_size, i, src_of(i), dst_of, send, recv, local, False)
        return 0

    lax.fori_loop(0, 2 * cp_size, sent, 0)
    for d in range(1, cp_size):
        peer = lax.rem(me + d, cp_size)
        for half in range(2):
            pltpu.make_async_remote_copy(
                src_ref=src_of(0), dst_ref=dst_of(half, peer), send_sem=send.at[0], recv_sem=recv.at[peer, half],
                device_id={'cp': peer}, device_id_type=MESH).wait_recv()


def forward_kernel(cp_size, tp_size, qkv_ref, dy_ref, dy1_ref, wo_ref, o_ref, l_ref, rows_ref, do_ref,
                   qkv, o_v, l_v, vt_ref, s_ref, acc_ref, dyg, wo, res, h_send, h_recv, h_local,
                   in_sem, send, recv, local, y_send, y_recv, out_sem):
    seq = qkv.shape[1]
    bq = s_ref.shape[0]
    nblk = seq // bq
    c = HEAD_DIM ** -0.5 * LOG2E
    _, right, left = ring('tp', tp_size)
    block = dy_ref.shape[0]
    half, part = block // 2, block // 4
    groups = row_groups(tp_size, block, False)
    heads = HeadSender(cp_size, tp_size, block, groups, res, do_ref, h_send, h_recv, h_local)

    def gathered(start, size):
        return dyg.at[pl.ds(start, size), :]

    loads = [
        pltpu.make_async_copy(dy_ref, gathered(0, block), in_sem.at[0]),
        pltpu.make_async_copy(wo_ref, wo, in_sem.at[1]),
        pltpu.make_async_copy(dy1_ref.at[pl.ds(0, part), :], gathered(block, part), in_sem.at[2]),
        pltpu.make_async_copy(dy1_ref.at[pl.ds(part, part), :], gathered(block + half, part), in_sem.at[3]),
        pltpu.make_async_copy(qkv_ref, qkv, in_sem.at[4]),
    ]
    for load in loads:
        load.start()
    meet(*others('cp', cp_size), *beside(tp_size))
    hops = [
        pltpu.make_async_remote_copy(
            src_ref=src, dst_ref=gathered(start, size), send_sem=y_send.at[k], recv_sem=y_recv.at[k],
            device_id={'tp': peer}, device_id_type=MESH)
        for k, (src, start, size, peer) in enumerate((
            (dy_ref.at[pl.ds(part, part), :], block + part, part, left),
            (dy_ref.at[pl.ds(half + part, part), :], block + half + part, part, right),
            (dy_ref.at[pl.ds(half, half), :], 2 * block, half, left),
            (dy_ref.at[pl.ds(0, half), :], 2 * block + half, half, right),
            (dy1_ref.at[pl.ds(0, part), :], 3 * block, part, left),
            (dy1_ref.at[pl.ds(part, part), :], 3 * block + half, part, right),
            (gathered(block + part, part), 3 * block + part, part, left),
            (gathered(block + half + part, part), 3 * block + half + part, part, right)))]
    for hop in hops[:6]:
        hop.start()

    per_step = min(4, cp_size)
    cols = per_step * HEAD_DIM

    def compute(g):
        rows = pl.ds(groups[g][0], block)

        def body(s, _):
            out = dot_nt(dyg[rows, :], wo[rows_at(s * cols, cols), :]).astype(BF16)
            for k in range(per_step):
                res[per_step * s + k, 0, rows, :] = out[:, k * HEAD_DIM:(k + 1) * HEAD_DIM]
            return 0

        lax.fori_loop(0, cp_size // per_step, body, 0)
        heads.start(g)

    for load in loads[:2]:
        load.wait()
    compute(0)
    for load in loads[2:]:
        load.wait()

    def transpose_step(b, _):
        rows = rows_at(b * bq, bq)
        vt_ref[:, rows] = qkv[2, rows, :].T
        return 0

    lax.fori_loop(0, nblk, transpose_step, 0)

    def src_of(i):
        return o_v.at[rows_at(i * bq, bq), :]

    def dst_of(part, head):
        return rows_ref.at[rows_at(part * bq, bq), rows_at(head * HEAD_DIM, HEAD_DIM)]

    def q_step(i, _):
        @pl.when(i == nblk // 2)
        def _():
            for arrived, hop in zip(hops, hops[6:]):
                arrived.wait_recv()
                hop.start()
            compute(1)

        @pl.when(i == nblk - 1)
        def _():
            for k, hop in enumerate(hops):
                hop.wait_send() if k < 2 else hop.wait()
            compute(2)
            compute(3)

        rows = rows_at(i * bq, bq)
        q = qkv[0, rows, :]
        acc_ref[...] = jnp.zeros_like(acc_ref)
        s = dot_nt(qkv[1, rows, :], q)
        kk = lax.broadcasted_iota(jnp.int32, (bq, bq), 0)
        qq = lax.broadcasted_iota(jnp.int32, (bq, bq), 1)
        s = jnp.where(kk <= qq, s, -jnp.inf)
        s_ref[...] = s
        first = jnp.max(s, axis=0, keepdims=True)

        def use(blk, m_old, m, l, following):
            mc = m * c
            alpha = jnp.exp2(m_old * c - mc)
            p = jnp.exp2(s_ref[...] * c - mc)
            m_new = m
            if following is not None:
                s = dot_nt(qkv[1, rows_at(following * bq, bq), :], q)
            part = jnp.sum(p, axis=0, keepdims=True)
            out = dot_nn(vt_ref[:, rows_at(blk * bq, bq)], p.astype(BF16))
            if following is not None:
                m_new = jnp.maximum(m, jnp.max(s, axis=0, keepdims=True))
                s_ref[...] = s
            acc_ref[...] = acc_ref[...] * alpha + out
            return m, m_new, l * alpha + part

        def body(t, carry):
            return use(jnp.where(t == 0, i, t - 1), *carry, t)

        carry = lax.fori_loop(0, i, body, (first, first, jnp.zeros((1, bq), F32)))
        m, _, l = use(jnp.where(i == 0, i, i - 1), *carry, None)
        o_v[rows, :] = (acc_ref[...] * (1.0 / l)).T.astype(BF16)
        l_v[i] = jnp.broadcast_to(m * c + jnp.log2(l), (8, bq))
        send_piece(cp_size, i, src_of(i), dst_of, send, recv, local, True)
        return 0

    lax.fori_loop(0, nblk, q_step, 0)
    out_o = pltpu.make_async_copy(o_v, o_ref, out_sem.at[0])
    out_l = pltpu.make_async_copy(l_v, l_ref, out_sem.at[1])
    out_o.start()
    out_l.start()
    wait_pieces(cp_size, src_of, dst_of, send, recv, local)
    heads.wait()
    out_o.wait()
    out_l.wait()


def forward(qkv, dy_blk, dy1, w_out, cp_size, tp_size):
    seq = qkv.shape[1]
    bq = seq // (2 * cp_size)
    block, width = dy_blk.shape
    cols = w_out.shape[0]
    pairs = seq * seq // 2
    return pl.pallas_call(
        functools.partial(forward_kernel, cp_size, tp_size),
        out_shape=(
            jax.ShapeDtypeStruct((seq, HEAD_DIM), BF16),
            jax.ShapeDtypeStruct((seq // bq, 8, bq), F32),
            jax.ShapeDtypeStruct((2 * bq, cp_size * HEAD_DIM), BF16),
            jax.ShapeDtypeStruct((1, seq, HEAD_DIM), BF16),
        ),
        in_specs=[ANYWHERE] * 4,
        out_specs=(ANYWHERE,) * 4,
        scratch_shapes=[
            pltpu.VMEM((3, seq, HEAD_DIM), BF16),
            pltpu.VMEM((seq, HEAD_DIM), BF16),
            pltpu.VMEM((seq // bq, 8, bq), F32),
            pltpu.VMEM((HEAD_DIM, seq), BF16),
            pltpu.VMEM((bq, bq), F32),
            pltpu.VMEM((HEAD_DIM, bq), F32),
            pltpu.VMEM((4 * block, width), BF16),
            pltpu.VMEM((cols, width), BF16),
        ] + head_scratch(cp_size, 1, 4 * block, 4) + [
            DMA((5,)), DMA((2 * cp_size,)), DMA((cp_size, 2)), DMA((2,)), DMA((8,)), DMA((8,)), DMA((2,)),
        ],
        compiler_params=params(1),
        cost_estimate=pl.CostEstimate(flops=4 * pairs * HEAD_DIM, bytes_accessed=8 * seq * HEAD_DIM, transcendentals=pairs),
        name="attention_forward",
    )(qkv, dy_blk, dy1, w_out)


def backward_kernel(cp_size, tp_size, qkv_ref, do_ref, o_ref, l_ref, o_rows_ref, wo_ref, rows_ref, oy_ref, wy_ref,
                    qkv, do_v, o_v, l_v, delta_v, kt_ref, qt_ref, dot_ref, p_ref, ds_ref, dst_ref, dq_acc, dk_acc, dv_acc, grads,
                    in_sem, send, recv, local, y_send, y_recv):
    seq = qkv.shape[1]
    bq = p_ref.shape[0]
    nblk, half_blk = 2 * cp_size, cp_size
    sub = bq // 2
    scale = HEAD_DIM ** -0.5
    c = scale * LOG2E
    loads = [
        pltpu.make_async_copy(qkv_ref, qkv, in_sem.at[0]),
        pltpu.make_async_copy(do_ref.at[0], do_v, in_sem.at[1]),
        pltpu.make_async_copy(o_ref, o_v, in_sem.at[2]),
        pltpu.make_async_copy(l_ref, l_v, in_sem.at[3]),
    ]
    for load in loads:
        load.start()
    meet(*others('cp', cp_size), *others('tp', tp_size))
    me_c, me_t = lax.axis_index('cp'), lax.axis_index('tp')
    share, block = wy_ref.shape[1], oy_ref.shape[1]
    y_hops = []
    for r in range(1, tp_size):
        peer = lax.rem(me_t + r, tp_size)
        y_hops.append((wo_ref.at[rows_at(me_c * share, share), :], wy_ref.at[r - 1], peer))
        y_hops.append((o_rows_ref.at[rows_at(peer * block, block), :], oy_ref.at[r - 1], peer))
    y_hops = [
        pltpu.make_async_remote_copy(
            src_ref=src, dst_ref=dst, send_sem=y_send.at[k], recv_sem=y_recv.at[k], device_id={'tp': peer}, device_id_type=MESH)
        for k, (src, dst, peer) in enumerate(y_hops)]
    for hop in y_hops:
        hop.start()
    for load in loads:
        load.wait()

    def piece(i):
        return rows_at(i * bq, bq)

    def init_step(b, _):
        rows = piece(b)
        kt_ref[:, rows] = qkv[1, rows, :].T
        qt_ref[:, rows] = qkv[0, rows, :].T
        dot_ref[:, rows] = do_v[rows, :].T
        prod = do_v[rows, :].astype(F32) * o_v[rows, :].astype(F32)
        delta_v[b] = jnp.broadcast_to(jnp.sum(prod.T, axis=0, keepdims=True), (8, bq))
        for acc in (dq_acc, dk_acc, dv_acc):
            acc[:, rows] = jnp.zeros((HEAD_DIM, bq), F32)
        return 0

    lax.fori_loop(0, nblk, init_step, 0)

    def half_pair(r, q, k, prev, masked):
        sl = slice(r * sub, (r + 1) * sub)
        krows = rows_at(k * bq + r * sub, sub)
        if prev is not None:
            prev_q, prev_k = piece(prev[0]), rows_at(prev[1] * bq + r * sub, sub)
            old_p, old_ds_t, old_ds = p_ref[:, sl], ds_ref[sl, :], dst_ref[:, sl]
        s = dot_nt(qkv[1, krows, :], qkv[0, piece(q), :])
        if prev is not None:
            dv_acc[:, prev_k] += dot_nn(dot_ref[:, prev_q], old_p)
        p = jnp.exp2(s * c - l_v[q][0:1, :])
        if masked:
            kk = lax.broadcasted_iota(jnp.int32, (sub, bq), 0) + r * sub
            p = jnp.where(kk <= lax.broadcasted_iota(jnp.int32, (sub, bq), 1), p, 0.0)
        p = p.astype(BF16)
        dp = dot_nt(qkv[2, krows, :], do_v[piece(q), :])
        if prev is not None:
            dk_acc[:, prev_k] += dot_nn(qt_ref[:, prev_q], old_ds)
        ds = (p.astype(F32) * (dp - delta_v[q][0:1, :])).astype(BF16)
        out = dot_nn(kt_ref[:, prev_k], old_ds_t) if prev is not None else None
        p_ref[:, sl], ds_ref[sl, :], dst_ref[:, sl] = p.T, ds, ds.T
        return out

    def pair(q, k, prev, masked=False):
        out = half_pair(0, q, k, prev, masked)
        out = out + half_pair(1, q, k, prev, masked)
        dq_acc[:, piece(prev[0])] += out
        return q, k

    def send_q(i, start):
        send_piece(cp_size, i, grads.at[pl.ds(0, 1), piece(i), :], lambda part, head: rows_ref.at[pl.ds(0, 1), piece(part), rows_at(head * HEAD_DIM, HEAD_DIM)],
                   send.at[0], recv.at[0], local.at[0], start)

    def send_kv(i, start):
        send_piece(cp_size, i, grads.at[pl.ds(1, 2), piece(i), :], lambda part, head: rows_ref.at[pl.ds(1, 2), piece(part), rows_at(head * HEAD_DIM, HEAD_DIM)],
                   send.at[1], recv.at[1], local.at[1], start)

    def finish_q(i):
        grads[0, piece(i), :] = (dq_acc[:, piece(i)] * scale).T.astype(BF16)
        send_q(i, True)

    def finish_kv(i):
        grads[1, piece(i), :] = (dk_acc[:, piece(i)] * scale).T.astype(BF16)
        grads[2, piece(i), :] = dv_acc[:, piece(i)].T.astype(BF16)
        send_kv(i, True)

    for r in range(2):
        half_pair(r, 0, 0, None, True)
    prev = lax.fori_loop(1, nblk, lambda i, prev: pair(i, i, prev, True), (0, 0))

    def late_column(k, prev):
        prev = pair(k + 1, k, prev)
        finish_kv(jnp.where(k == half_blk, nblk - 1, k - 1))
        return lax.fori_loop(k + 2, nblk, lambda q, prev: pair(q, k, prev), prev)

    prev = lax.fori_loop(half_blk, nblk - 1, late_column, prev)

    def row(q, prev):
        prev = pair(q, 0, prev)

        @pl.when(q == 1)
        def _():
            finish_kv(nblk - 2)

        finish_q(q - 1)
        return lax.fori_loop(1, jnp.minimum(q, half_blk), lambda k, prev: pair(q, k, prev), prev)

    rows_done = half_blk + 2
    prev = lax.fori_loop(1, rows_done, row, prev)

    def column(n, prev):
        def key(n):
            return jnp.where(n < half_blk // 2, 2 * n, 2 * (n - half_blk // 2) + 1)

        prev = pair(rows_done, key(n), prev)

        @pl.when(n == 0)
        def _():
            finish_q(rows_done - 1)

        @pl.when(n > 0)
        def _():
            finish_kv(key(n - 1))

        return lax.fori_loop(rows_done + 1, nblk, lambda q, prev: pair(q, key(n), prev), prev)

    if rows_done < nblk:
        prev = lax.fori_loop(0, half_blk, column, prev)
    last_q, last_k = piece(prev[0]), piece(prev[1])
    dv_acc[:, last_k] += dot_nn(dot_ref[:, last_q], p_ref[...])
    dk_acc[:, last_k] += dot_nn(qt_ref[:, last_q], dst_ref[...])
    dq_acc[:, last_q] += dot_nn(kt_ref[:, last_k], ds_ref[...])
    if rows_done < nblk:
        finish_kv(half_blk - 1)
        lax.fori_loop(rows_done, nblk, lambda q, _: (finish_q(q), 0)[1], 0)
    else:
        lax.fori_loop(0, half_blk, lambda k, _: (finish_kv(k), 0)[1], 0)
        finish_q(rows_done - 1)

    def sent(i, _):
        send_q(i, False)
        send_kv(i, False)
        return 0

    lax.fori_loop(0, nblk, sent, 0)
    for d in range(1, cp_size):
        peer = lax.rem(me_c + d, cp_size)
        for half in range(2):
            for kind, parts in enumerate((pl.ds(0, 1), pl.ds(1, 2))):
                pltpu.make_async_remote_copy(
                    src_ref=grads.at[parts, piece(0), :], dst_ref=rows_ref.at[parts, piece(half), rows_at(peer * HEAD_DIM, HEAD_DIM)],
                    send_sem=send.at[kind, 0], recv_sem=recv.at[kind, peer, half],
                    device_id={'cp': peer}, device_id_type=MESH).wait_recv()
    for hop in y_hops:
        hop.wait()


def backward(qkv, do, o, lse, o_rows, w_out, cp_size, tp_size):
    seq = qkv.shape[1]
    cols, width = w_out.shape
    block = o_rows.shape[0] // tp_size
    share = cols // cp_size
    bq = seq // (2 * cp_size)
    pairs = seq * seq // 2
    turned = pltpu.VMEM((HEAD_DIM, seq), BF16)
    total = pltpu.VMEM((HEAD_DIM, seq), F32)
    square = pltpu.VMEM((bq, bq), BF16)
    return pl.pallas_call(
        functools.partial(backward_kernel, cp_size, tp_size),
        out_shape=(
            jax.ShapeDtypeStruct((3, 2 * bq, cp_size * HEAD_DIM), BF16),
            jax.ShapeDtypeStruct((tp_size - 1, block, cols), BF16),
            jax.ShapeDtypeStruct((tp_size - 1, share, width), BF16),
        ),
        in_specs=[ANYWHERE] * 6,
        out_specs=(ANYWHERE,) * 3,
        scratch_shapes=[
            pltpu.VMEM((3, seq, HEAD_DIM), BF16),
            pltpu.VMEM((seq, HEAD_DIM), BF16),
            pltpu.VMEM((seq, HEAD_DIM), BF16),
            pltpu.VMEM((seq // bq, 8, bq), F32),
            pltpu.VMEM((seq // bq, 8, bq), F32),
            turned, turned, turned, square, square, square, total, total, total,
            pltpu.VMEM((3, seq, HEAD_DIM), BF16),
            DMA((4,)), DMA((2, 2 * cp_size)), DMA((2, cp_size, 2)), DMA((2, 2)), DMA((6,)), DMA((6,)),
        ],
        compiler_params=params(2),
        cost_estimate=pl.CostEstimate(flops=10 * pairs * HEAD_DIM, bytes_accessed=16 * seq * HEAD_DIM, transcendentals=pairs),
        name="attention_backward",
    )(qkv, do, o, lse, o_rows, w_out)


def reduce_kernel(cp_size, tp_size, chunks, rows_ref, wq_ref, wk_ref, wv_ref, o_rows_ref, oy_ref, wo_ref, wy_ref,
                  out_ref, y_ref, wx_ref, sib_ref,
                  g_v, w_v, part, mid, last, out_v, stage, y_acc, o_v, in_sem, w_sem, out_sem, sends, recvs,
                  x_send, x_recv, d_send, d_recv, o_sem, s_sem):
    me, right, left = ring('tp', tp_size)
    far = lax.rem(me + 2, tp_size)
    block = part.shape[1]
    half = block // 2
    low, high = pl.ds(0, half), pl.ds(half, half)
    wide = part.shape[2] // chunks
    weights = (wq_ref, wk_ref, wv_ref)

    def w_load(n, a):
        return pltpu.make_async_copy(weights[a].at[rows_at(n * wide, wide), :], w_v.at[lax.rem(n, 2), a], w_sem.at[lax.rem(n, 2), a])

    load = pltpu.make_async_copy(rows_ref, g_v, in_sem)
    load.start()
    for a in range(3):
        w_load(0, a).start()
    me_c, mate = lax.axis_index('cp'), partner()
    chips = cp_size // 2
    ahead, behind = lax.rem(me_c + 2, cp_size), lax.rem(me_c + cp_size - 2, cp_size)
    nearest = (1, chips - 1) if chips > 2 else (1,)
    meet(*beside(tp_size), {'cp': mate}, *({'cp': peer} for peer in (ahead, behind)[:len(nearest)]))
    share = wy_ref.shape[1]

    def share_ref(s, k):
        return wy_ref.at[s] if k == 0 else wx_ref.at[s, k - 1]

    def x_copy(s, n, src, dst, peer):
        return pltpu.make_async_remote_copy(
            src_ref=src, dst_ref=dst, send_sem=x_send.at[s, n], recv_sem=x_recv.at[s, n], device_id={'cp': peer}, device_id_type=MESH)

    def along(s, n):
        return x_copy(s, n, wy_ref.at[s], wx_ref.at[s, nearest[n] - 1], (ahead, behind)[n])

    def relay(s, n):
        rows = pl.ds(n * (share // 2), share // 2)
        return x_copy(s, 2 + n, wx_ref.at[s, nearest[n] - 1, rows, :], wx_ref.at[s, 1, rows, :], (ahead, behind)[n])

    def across(s, k):
        return pltpu.make_async_remote_copy(
            src_ref=share_ref(s, k), dst_ref=sib_ref.at[s, k], send_sem=d_send.at[s, k], recv_sem=d_recv.at[s, k],
            device_id={'cp': mate}, device_id_type=MESH)

    slots = range(tp_size - 1)
    for s in slots:
        for n in range(len(nearest)):
            along(s, n).start()
        across(s, 0).start()
    o_loads = [pltpu.make_async_copy(o_rows_ref.at[rows_at(me * (o_rows_ref.shape[0] // tp_size), o_rows_ref.shape[0] // tp_size), :], o_v.at[0], o_sem.at[0])]
    for s in range(tp_size - 1):
        o_loads.append(pltpu.make_async_copy(oy_ref.at[s], o_v.at[s + 1], o_sem.at[s + 1]))
    for copy in o_loads:
        copy.start()

    kinds = ('far_r', 'far_l', 'plain_r', 'plain_l', 'sum_r', 'sum_l')

    def hop(kind, n):
        cols = rows_at(n * wide, wide)
        src, dst, peer = {
            'far_r': (part.at[FAR, low, cols], mid.at[0, :, cols], right),
            'far_l': (part.at[FAR, high, cols], mid.at[1, :, cols], left),
            'plain_r': (part.at[RIGHT, high, cols], last.at[0, high, cols], right),
            'plain_l': (part.at[LEFT, low, cols], last.at[1, low, cols], left),
            'sum_r': (part.at[RIGHT, low, cols], last.at[0, low, cols], right),
            'sum_l': (part.at[LEFT, high, cols], last.at[1, high, cols], left),
        }[kind]
        k = kinds.index(kind)
        return pltpu.make_async_remote_copy(
            src_ref=src, dst_ref=dst, send_sem=sends.at[k, n], recv_sem=recvs.at[k, n], device_id={'tp': peer}, device_id_type=MESH)

    load.wait()

    def compute(n, _):
        slot = lax.rem(n, 2)

        @pl.when(n + 1 < chunks)
        def _():
            for a in range(3):
                w_load(n + 1, a).start()

        for a in range(3):
            w_load(n, a).wait()
        cols = rows_at(n * wide, wide)
        ready = {FAR: ('far_r', 'far_l'), RIGHT: ('plain_r',), LEFT: ('plain_l',), OWN: ()}
        for k, owner in enumerate((far, right, left, me)):
            rows = rows_at(owner * block, block)
            total = dot_nt(g_v[0, rows, :], w_v[slot, 0])
            total = total + dot_nt(g_v[1, rows, :], w_v[slot, 1])
            part[k, :, cols] = total + dot_nt(g_v[2, rows, :], w_v[slot, 2])
            for kind in ready[k]:
                hop(kind, n).start()
        return 0

    lax.fori_loop(0, chunks, compute, 0)
    for s in slots:
        for n, k in enumerate(nearest):
            along(s, n).wait_recv()
            if chips > 2:
                relay(s, n).start()
            across(s, k).start()

    def forward_sums(n, _):
        cols = rows_at(n * wide, wide)
        hop('far_r', n).wait_recv()
        part[RIGHT, :half, cols] += mid[0, :, cols]
        hop('sum_r', n).start()
        hop('far_l', n).wait_recv()
        part[LEFT, half:, cols] += mid[1, :, cols]
        hop('sum_l', n).start()
        return 0

    lax.fori_loop(0, chunks, forward_sums, 0)

    if chips > 2:
        for s in slots:
            for n in range(2):
                relay(s, n).wait_recv()
            across(s, 2).start()
    for copy in o_loads:
        copy.wait()
    span = stage.shape[2]
    halves = y_acc.shape[1] // span

    def stage_copies(n):
        s, h = divmod(n, halves)
        cols = pl.ds(h * span, span)
        slot = n % 2
        if s == 0:
            return [pltpu.make_async_copy(wo_ref.at[:, cols], stage.at[slot], s_sem.at[slot, 0])]
        copies = []
        for k in range(cp_size // 2):
            mine, its = lax.rem(me_c + cp_size - 2 * k, cp_size), lax.rem(mate + cp_size - 2 * k, cp_size)
            copies.append(pltpu.make_async_copy(
                share_ref(s - 1, k).at[:, cols], stage.at[slot, rows_at(mine * share, share), :], s_sem.at[slot, 2 * k]))
            copies.append(pltpu.make_async_copy(
                sib_ref.at[s - 1, k, :, cols], stage.at[slot, rows_at(its * share, share), :], s_sem.at[slot, 2 * k + 1]))
        return copies

    def stage_start(n):
        s, h = divmod(n, halves)
        if s > 0 and h == 0:
            for k in range(cp_size // 2):
                across(s - 1, k).wait_recv()
        for copy in stage_copies(n):
            copy.start()

    total_steps = tp_size * halves
    stage_start(0)
    for n in range(total_steps):
        if n + 1 < total_steps:
            stage_start(n + 1)
        for copy in stage_copies(n):
            copy.wait()
        s, h = divmod(n, halves)
        tile = min(512, span)

        def y_step(j, _):
            cols = rows_at(j * tile, tile)
            out = rows_at(h * span + j * tile, tile)
            product = dot_nn(o_v[s], stage[n % 2, :, cols])
            if s == 0:
                y_acc[:, out] = product
            elif s < tp_size - 1:
                y_acc[:, out] += product
            else:
                out_v[:, out] = (y_acc[:, out] + product).astype(BF16)
            return 0

        lax.fori_loop(0, span // tile, y_step, 0)
    y_out = pltpu.make_async_copy(out_v, y_ref, in_sem)
    y_out.start()
    y_out.wait()

    def put(n):
        cols = rows_at(n * wide, wide)
        return pltpu.make_async_copy(out_v.at[:, cols], out_ref.at[:, cols], out_sem.at[n])

    def finish(n, _):
        cols = rows_at(n * wide, wide)
        for kind in ('plain_r', 'plain_l', 'sum_r', 'sum_l'):
            hop(kind, n).wait_recv()
        out_v[:, cols] = (part[OWN, :, cols] + last[0, :, cols] + last[1, :, cols]).astype(BF16)
        put(n).start()
        return 0

    lax.fori_loop(0, chunks, finish, 0)

    def close(n, _):
        put(n).wait()
        for kind in kinds:
            hop(kind, n).wait_send()
        return 0

    lax.fori_loop(0, chunks, close, 0)
    for s in slots:
        for k in range(chips):
            across(s, k).wait_send()
        for n in range(len(nearest)):
            along(s, n).wait_send()
            if chips > 2:
                relay(s, n).wait_send()


def reduce_out(grad_rows, weights, o_rows, oy, w_out, wy, cp_size, tp_size):
    width, cols = weights[0].shape
    share = wy.shape[1]
    pairs = cp_size // 2
    rows = grad_rows.shape[1]
    block = rows // tp_size
    chunks = 8
    wide = width // chunks
    return pl.pallas_call(
        functools.partial(reduce_kernel, cp_size, tp_size, chunks),
        out_shape=(
            jax.ShapeDtypeStruct((block, width), BF16),
            jax.ShapeDtypeStruct((block, width), BF16),
            jax.ShapeDtypeStruct((tp_size - 1, pairs - 1, share, width), BF16),
            jax.ShapeDtypeStruct((tp_size - 1, pairs, share, width), BF16),
        ),
        in_specs=[ANYWHERE] * 8,
        out_specs=(ANYWHERE,) * 4,
        scratch_shapes=[
            pltpu.VMEM((3, rows, cols), BF16),
            pltpu.VMEM((2, 3, wide, cols), BF16),
            pltpu.VMEM((4, block, width), F32),
            pltpu.VMEM((2, block // 2, width), F32),
            pltpu.VMEM((2, block, width), F32),
            pltpu.VMEM((block, width), BF16),
            pltpu.VMEM((2, cols, width // 4), BF16),
            pltpu.VMEM((block, width), F32),
            pltpu.VMEM((tp_size, block, cols), BF16),
            DMA, DMA((2, 3)), DMA((chunks,)), DMA((6, chunks)), DMA((6, chunks)),
            DMA((tp_size - 1, 4)), DMA((tp_size - 1, 4)), DMA((tp_size - 1, pairs)), DMA((tp_size - 1, pairs)),
            DMA((tp_size,)), DMA((2, cp_size)),
        ],
        compiler_params=params(3),
        cost_estimate=pl.CostEstimate(flops=6 * rows * width * cols, bytes_accessed=6 * width * cols, transcendentals=0),
        name="project_reduce",
    )(grad_rows, *weights, o_rows, oy, w_out, wy)


def solution(mesh):
    cp_size, tp_size = mesh.shape['cp'], mesh.shape['tp']
    row_spec = P(('dp', 'cp', 'tp'), None)

    def local_step(x_blk, dy_blk, w_query, w_key, w_value, w_out):
        weights = (w_query, w_key, w_value)
        qkv, dy1 = project(x_blk, dy_blk, weights, cp_size, tp_size)
        o, lse, o_rows, do = forward(qkv, dy_blk, dy1, w_out, cp_size, tp_size)
        grad_rows, oy, wy = backward(qkv, do, o, lse, o_rows, w_out, cp_size, tp_size)
        dx_blk, y_blk, _, _ = reduce_out(grad_rows, weights, o_rows, oy, w_out, wy, cp_size, tp_size)
        return y_blk, dx_blk

    weight = P(None, 'tp')
    return jax.shard_map(local_step, mesh=mesh, in_specs=(row_spec, row_spec, weight, weight, weight, P('tp', None)), out_specs=(row_spec, row_spec), check_vma=False)
```

```python
import functools
import math

import jax
import jax.numpy as jnp
from jax import lax
from jax.experimental import pallas as pl
from jax.experimental.pallas import tpu as pltpu
from jax.sharding import PartitionSpec as P

HEAD_DIM = 128
F32, BF16 = jnp.float32, jnp.bfloat16
LOG2E = math.log2(math.e)
MESH = pl.DeviceIdType.MESH
ANYWHERE = pl.BlockSpec(memory_space=pltpu.HBM)
DMA = pltpu.SemaphoreType.DMA
FAR, RIGHT, LEFT, OWN = range(4)


def dot_nt(a, b):
    return lax.dot_general(a, b, (((1,), (1,)), ((), ())), preferred_element_type=F32)


def dot_nn(a, b):
    return lax.dot_general(a, b, (((1,), (0,)), ((), ())), preferred_element_type=F32)


def rows_at(start, size):
    return pl.ds(pl.multiple_of(start, size), size)


def ring(axis, size):
    me = lax.axis_index(axis)
    return me, lax.rem(me + 1, size), lax.rem(me + size - 1, size)


def meet(*peers):
    barrier = pltpu.get_barrier_semaphore()
    for peer in peers:
        pl.semaphore_signal(barrier, inc=1, device_id=peer, device_id_type=MESH)
    pl.semaphore_wait(barrier, len(peers))


def others(axis, size):
    me = lax.axis_index(axis)
    return [{axis: lax.rem(me + d, size)} for d in range(1, size)]


def beside(tp_size):
    _, right, left = ring('tp', tp_size)
    return [{'tp': right}, {'tp': left}]


def partner():
    me = lax.axis_index('cp')
    return me + 1 - 2 * lax.rem(me, 2)


def params(collective_id):
    return pltpu.CompilerParams(collective_id=collective_id, has_side_effects=True, vmem_limit_bytes=63 << 20)


def far_first(cp_size):
    return sorted(range(1, cp_size), key=lambda d: -min(d, cp_size - d))


def position(cp_size, tp_size, block, owner, row):
    piece = block * tp_size // 2
    first = owner < tp_size // 2
    cp_rank = lax.axis_index('cp')
    piece_id = jnp.where(first, cp_rank, 2 * cp_size - 1 - cp_rank)
    return piece_id * piece + jnp.where(first, owner, owner - tp_size // 2) * block + row


class Gather:
    STEPS = 6

    def __init__(self, tp_size, src, buf, send, recv):
        self.src, self.buf, self.sems = src, buf, (send, recv)
        self.me, self.right, self.left = ring('tp', tp_size)
        self.far = lax.rem(self.me + 2, tp_size)
        self.block = src.shape[0]
        self.part = self.block // 4

    def start_row(self, j):
        return self.block + (j - 1) * (2 * self.part)

    def rows(self, j, side):
        return self.buf.at[rows_at(self.start_row(j) + side * self.part, self.part), :]

    def first_row(self, j, side):
        return lax.rem(j + (1 if side else 3), 4) * self.part

    def parts(self, j):
        near = j <= 4
        return (
            (jnp.where(near, self.right, self.far), self.first_row(j, 0)),
            (jnp.where(near, self.left, self.far), self.first_row(j, 1)),
        )

    def hop(self, j, side, relayed, dst=None):
        src = self.rows(j - 4, side) if relayed else self.src.at[rows_at(self.first_row(j, side), self.part), :]
        return pltpu.make_async_remote_copy(
            src_ref=src, dst_ref=self.rows(j, side) if dst is None else dst,
            send_sem=self.sems[0].at[j - 1, side], recv_sem=self.sems[1].at[j - 1, side],
            device_id={'tp': self.right if side else self.left}, device_id_type=MESH)

    def start(self, j, relayed):
        for side in range(2):
            self.hop(j, side, relayed).start()

    def arrive(self, j):
        for side in range(2):
            self.hop(j, side, False).wait_recv()

    def leave(self, j):
        for side in range(2):
            self.hop(j, side, False).wait_send()


class HeadSender:
    def __init__(self, cp_size, tp_size, gather, res, dst, send, recv, local):
        self.cp_size, self.tp_size, self.gather = cp_size, tp_size, gather
        self.res, self.dst, self.sems = res, dst, (send, recv, local)

    def copies(self, j):
        send, recv, local = self.sems
        me = lax.axis_index('cp')
        own = isinstance(j, int)
        block = self.gather.block
        if own:
            start, length, parts = 0, block // 2, ((self.gather.me, 0), (self.gather.me, block // 2))
        else:
            start, length, parts = self.gather.start_row(j), self.gather.part, self.gather.parts(j)
        for n, (owner, row) in enumerate(parts):
            rows = rows_at(position(self.cp_size, self.tp_size, block, owner, row), length)
            here = rows_at(start + n * length, length)
            for d in far_first(self.cp_size):
                peer = lax.rem(me + d, self.cp_size)
                yield pltpu.make_async_remote_copy(
                    src_ref=self.res.at[peer, :, here, :], dst_ref=self.dst.at[:, rows, :],
                    send_sem=send.at[d - 1, j, n], recv_sem=recv.at[d - 1, j, n],
                    device_id={'cp': peer}, device_id_type=MESH)
            yield pltpu.make_async_copy(self.res.at[me, :, here, :], self.dst.at[:, rows, :], local.at[j, n])

    def start(self, j):
        for copy in self.copies(j):
            copy.start()

    def wait(self):
        for copy in self.copies(0):
            copy.wait()

        def step(j, _):
            for copy in self.copies(j):
                copy.wait()
            return 0

        lax.fori_loop(1, Gather.STEPS + 1, step, 0)


def head_scratch(cp_size, arrays, rows):
    each = (cp_size - 1, Gather.STEPS + 1, 2)
    return [pltpu.VMEM((cp_size, arrays, rows, HEAD_DIM), BF16), DMA(each), DMA(each), DMA(each[1:])]


def project_kernel(cp_size, tp_size, x_ref, dy_ref, wq_ref, wk_ref, wv_ref, qkv_ref, dy1_ref,
                   w_v, xg, res, send, recv, local, w_sem, x_sem, y_send, y_recv, dy_send, dy_recv):
    block = x_ref.shape[0]
    gather = Gather(tp_size, x_ref, xg, y_send, y_recv)
    early = Gather(tp_size, dy_ref, None, dy_send, dy_recv)
    heads = HeadSender(cp_size, tp_size, gather, res, qkv_ref, send, recv, local)
    part = gather.part

    def early_hop(side):
        return early.hop(1, side, False, dy1_ref.at[pl.ds(side * part, part), :])

    own = pltpu.make_async_copy(x_ref, xg.at[pl.ds(0, block), :], x_sem)
    own.start()
    loads = [pltpu.make_async_copy(w, w_v.at[n], w_sem.at[n]) for n, w in enumerate((wq_ref, wk_ref, wv_ref))]
    meet(*others('cp', cp_size), *beside(tp_size))
    for j in range(1, 5):
        gather.start(j, False)
    for load in loads:
        load.start()
    own.wait()

    wide = min(4, cp_size)
    cols = wide * HEAD_DIM
    steps = cp_size // wide

    def compute(rows, n):
        def body(s, _):
            out = dot_nn(xg[rows, :], w_v[n, :, rows_at(s * cols, cols)]).astype(BF16)
            for k in range(wide):
                res[wide * s + k, n, rows, :] = out[:, k * HEAD_DIM:(k + 1) * HEAD_DIM]
            return 0

        lax.fori_loop(0, steps, body, 0)

    for n, load in enumerate(loads):
        load.wait()
        compute(pl.ds(0, block), n)
    heads.start(0)

    def step(j, _):
        gather.arrive(j)

        @pl.when(j <= 2)
        def _():
            gather.start(j + 4, True)

        @pl.when(j == 2)
        def _():
            for side in range(2):
                early_hop(side).start()

        rows = rows_at(gather.start_row(j), 2 * part)
        lax.fori_loop(0, len(loads), lambda n, _: (compute(rows, n), 0)[1], 0)
        heads.start(j)
        return 0

    lax.fori_loop(1, Gather.STEPS + 1, step, 0)
    lax.fori_loop(1, Gather.STEPS + 1, lambda j, _: (gather.leave(j), 0)[1], 0)
    for side in range(2):
        early_hop(side).wait()
    heads.wait()


def project(x_blk, dy_blk, weights, cp_size, tp_size):
    block, width = x_blk.shape
    cols = weights[0].shape[1]
    rows = block * tp_size
    each = DMA((Gather.STEPS, 2))
    return pl.pallas_call(
        functools.partial(project_kernel, cp_size, tp_size),
        out_shape=(jax.ShapeDtypeStruct((len(weights), rows * cp_size, HEAD_DIM), BF16), jax.ShapeDtypeStruct((block // 2, width), BF16)),
        in_specs=[ANYWHERE] * 5,
        out_specs=(ANYWHERE, ANYWHERE),
        scratch_shapes=[pltpu.VMEM((len(weights), width, cols), BF16), pltpu.VMEM((rows, width), BF16)]
        + head_scratch(cp_size, len(weights), rows) + [DMA((len(weights),)), DMA, each, each, each, each],
        compiler_params=params(0),
        cost_estimate=pl.CostEstimate(flops=6 * rows * width * cols, bytes_accessed=6 * width * cols, transcendentals=0),
        name="project_qkv",
    )(x_blk, dy_blk, *weights)


def send_piece(cp_size, i, src, dst_of, send, recv, local, start):
    me = lax.axis_index('cp')
    half = jnp.where(i < cp_size, 0, 1)
    owner = jnp.where(i < cp_size, i, 2 * cp_size - 1 - i)

    @pl.when(owner == me)
    def _():
        copy = pltpu.make_async_copy(src, dst_of(half, me), local.at[half])
        copy.start() if start else copy.wait()

    @pl.when(owner != me)
    def _():
        copy = pltpu.make_async_remote_copy(
            src_ref=src, dst_ref=dst_of(half, me), send_sem=send.at[i], recv_sem=recv.at[me, half],
            device_id={'cp': owner}, device_id_type=MESH)
        copy.start() if start else copy.wait_send()


def forward_kernel(cp_size, tp_size, qkv_ref, dy_ref, dy1_ref, wo_ref, o_ref, ot_ref, l_ref, do_ref,
                   qkv, o_v, ot_v, l_v, vt_ref, s_ref, acc_ref, dyg, wo, res, h_send, h_recv, h_local, in_sem, y_send, y_recv, out_sem):
    seq = qkv.shape[1]
    bq = s_ref.shape[0]
    nblk = seq // bq
    c = HEAD_DIM ** -0.5 * LOG2E
    gather = Gather(tp_size, dy_ref, dyg, y_send, y_recv)
    heads = HeadSender(cp_size, tp_size, gather, res, do_ref, h_send, h_recv, h_local)
    block, part = gather.block, gather.part

    loads = [
        pltpu.make_async_copy(src, dst, in_sem.at[n])
        for n, (src, dst) in enumerate(((dy_ref, dyg.at[pl.ds(0, block), :]), (wo_ref, wo), (dy1_ref, dyg.at[pl.ds(block, 2 * part), :]), (qkv_ref, qkv)))]
    for load in loads:
        load.start()
    meet(*others('cp', cp_size), *beside(tp_size))
    for j in range(2, 5):
        gather.start(j, False)

    per_step = min(4, cp_size)
    cols = per_step * HEAD_DIM

    def compute(n):
        rows = rows_at(n * block, block)

        def body(s, _):
            out = dot_nt(dyg[rows, :], wo[rows_at(s * cols, cols), :]).astype(BF16)
            for k in range(per_step):
                res[per_step * s + k, 0, rows, :] = out[:, k * HEAD_DIM:(k + 1) * HEAD_DIM]
            return 0

        lax.fori_loop(0, cp_size // per_step, body, 0)

    def compute_steps(n, _):
        compute(n)
        lax.fori_loop(2 * n - 1, 2 * n + 1, lambda j, _: (heads.start(j), 0)[1], 0)
        return 0

    for load in loads[:2]:
        load.wait()
    compute(0)
    heads.start(0)
    for load in loads[2:]:
        load.wait()
    gather.start(5, True)

    def transpose_step(b, _):
        rows = rows_at(b * bq, bq)
        vt_ref[:, rows] = qkv[2, rows, :].T
        return 0

    lax.fori_loop(0, nblk, transpose_step, 0)

    def q_step(i, _):
        @pl.when(i == nblk // 2)
        def _():
            gather.arrive(2)
            gather.start(6, True)

        @pl.when(i == nblk - 1)
        def _():
            lax.fori_loop(3, Gather.STEPS + 1, lambda j, _: (gather.arrive(j), 0)[1], 0)
            lax.fori_loop(1, tp_size, compute_steps, 0)

        rows = rows_at(i * bq, bq)
        q = qkv[0, rows, :]
        acc_ref[...] = jnp.zeros_like(acc_ref)
        s = dot_nt(qkv[1, rows, :], q)
        kk = lax.broadcasted_iota(jnp.int32, (bq, bq), 0)
        qq = lax.broadcasted_iota(jnp.int32, (bq, bq), 1)
        s = jnp.where(kk <= qq, s, -jnp.inf)
        s_ref[...] = s
        first = jnp.max(s, axis=0, keepdims=True)

        def use(blk, m_old, m, l, following):
            mc = m * c
            alpha = jnp.exp2(m_old * c - mc)
            p = jnp.exp2(s_ref[...] * c - mc)
            m_new = m
            if following is not None:
                s = dot_nt(qkv[1, rows_at(following * bq, bq), :], q)
            part = jnp.sum(p, axis=0, keepdims=True)
            out = dot_nn(vt_ref[:, rows_at(blk * bq, bq)], p.astype(BF16))
            if following is not None:
                m_new = jnp.maximum(m, jnp.max(s, axis=0, keepdims=True))
                s_ref[...] = s
            acc_ref[...] = acc_ref[...] * alpha + out
            return m, m_new, l * alpha + part

        def body(t, carry):
            return use(jnp.where(t == 0, i, t - 1), *carry, t)

        carry = lax.fori_loop(0, i, body, (first, first, jnp.zeros((1, bq), F32)))
        m, _, l = use(jnp.where(i == 0, i, i - 1), *carry, None)
        out = (acc_ref[...] * (1.0 / l)).astype(BF16)
        ot_v[:, rows] = out
        o_v[rows, :] = out.T
        l_v[i] = jnp.broadcast_to(m * c + jnp.log2(l), (8, bq))
        return 0

    lax.fori_loop(0, nblk, q_step, 0)
    stores = [pltpu.make_async_copy(src, dst, out_sem.at[n]) for n, (src, dst) in enumerate(((o_v, o_ref), (ot_v, ot_ref), (l_v, l_ref)))]
    for store in stores:
        store.start()
    heads.wait()
    lax.fori_loop(2, Gather.STEPS + 1, lambda j, _: (gather.leave(j), 0)[1], 0)
    for store in stores:
        store.wait()


def forward(qkv, dy_blk, dy1, w_out, cp_size, tp_size):
    seq = qkv.shape[1]
    bq = seq // (2 * cp_size)
    block, width = dy_blk.shape
    cols = w_out.shape[0]
    pairs = seq * seq // 2
    rows, turned = (seq, HEAD_DIM), (HEAD_DIM, seq)
    logs = (seq // bq, 8, bq)
    each = DMA((Gather.STEPS, 2))
    return pl.pallas_call(
        functools.partial(forward_kernel, cp_size, tp_size),
        out_shape=(
            jax.ShapeDtypeStruct(rows, BF16),
            jax.ShapeDtypeStruct(turned, BF16),
            jax.ShapeDtypeStruct(logs, F32),
            jax.ShapeDtypeStruct((1, seq, HEAD_DIM), BF16),
        ),
        in_specs=[ANYWHERE] * 4,
        out_specs=(ANYWHERE,) * 4,
        scratch_shapes=[
            pltpu.VMEM(qkv.shape, BF16),
            pltpu.VMEM(rows, BF16),
            pltpu.VMEM(turned, BF16),
            pltpu.VMEM(logs, F32),
            pltpu.VMEM(turned, BF16),
            pltpu.VMEM((bq, bq), F32),
            pltpu.VMEM((HEAD_DIM, bq), F32),
            pltpu.VMEM((tp_size * block, width), BF16),
            pltpu.VMEM((cols, width), BF16),
        ] + head_scratch(cp_size, 1, tp_size * block) + [DMA((4,)), each, each, DMA((3,))],
        compiler_params=params(1),
        cost_estimate=pl.CostEstimate(flops=4 * pairs * HEAD_DIM, bytes_accessed=8 * seq * HEAD_DIM, transcendentals=pairs),
        name="attention_forward",
    )(qkv, dy_blk, dy1, w_out)


def backward_kernel(cp_size, tp_size, qkv_ref, do_ref, o_ref, ot_ref, l_ref, wo_ref, rows_ref, o_rows_ref, oy_ref, wy_ref,
                    qkv, do_v, ot_v, l_v, delta_v, kt_ref, qt_ref, dot_ref, p_ref, ds_ref, dst_ref, dq_acc, dk_acc, dv_acc, grads,
                    in_sem, send, recv, local, y_send, y_recv):
    seq = qkv.shape[1]
    bq = p_ref.shape[0]
    nblk, half_blk = 2 * cp_size, cp_size
    sub = bq // 2
    scale = HEAD_DIM ** -0.5
    c = scale * LOG2E
    loads = [
        pltpu.make_async_copy(qkv_ref, qkv, in_sem.at[0]),
        pltpu.make_async_copy(do_ref.at[0], do_v, in_sem.at[1]),
        pltpu.make_async_copy(ot_ref, ot_v, in_sem.at[2]),
        pltpu.make_async_copy(l_ref, l_v, in_sem.at[3]),
    ]
    for load in loads:
        load.start()
    meet(*others('cp', cp_size), *others('tp', tp_size))
    me_c, me_t = lax.axis_index('cp'), lax.axis_index('tp')
    share, block = wy_ref.shape[1], oy_ref.shape[1]

    def over_tp(kind, r):
        peer = lax.rem(me_t + r, tp_size)
        src, dst = ((wo_ref.at[rows_at(me_c * share, share), :], wy_ref), (o_rows_ref.at[rows_at(peer * block, block), :], oy_ref))[kind]
        return pltpu.make_async_remote_copy(
            src_ref=src, dst_ref=dst.at[r - 1], send_sem=y_send.at[kind, r - 1], recv_sem=y_recv.at[kind, r - 1],
            device_id={'tp': peer}, device_id_type=MESH)

    for r in range(1, tp_size):
        over_tp(0, r).start()
    for load in loads:
        load.wait()

    def piece(i):
        return rows_at(i * bq, bq)

    def init_step(b, _):
        rows = piece(b)
        kt_ref[:, rows] = qkv[1, rows, :].T
        qt_ref[:, rows] = qkv[0, rows, :].T
        dot_ref[:, rows] = do_v[rows, :].T
        prod = dot_ref[:, rows].astype(F32) * ot_v[:, rows].astype(F32)
        delta_v[b] = jnp.broadcast_to(jnp.sum(prod, axis=0, keepdims=True), (8, bq))
        for acc in (dq_acc, dk_acc, dv_acc):
            acc[:, rows] = jnp.zeros((HEAD_DIM, bq), F32)
        return 0

    lax.fori_loop(0, nblk, init_step, 0)

    def half_pair(r, q, k, prev, masked):
        sl = slice(r * sub, (r + 1) * sub)
        krows = rows_at(k * bq + r * sub, sub)
        if prev is not None:
            prev_q, prev_k = piece(prev[0]), rows_at(prev[1] * bq + r * sub, sub)
            old_p, old_ds_t, old_ds = p_ref[:, sl], ds_ref[sl, :], dst_ref[:, sl]
        s = dot_nt(qkv[1, krows, :], qkv[0, piece(q), :])
        if prev is not None:
            dv_acc[:, prev_k] += dot_nn(dot_ref[:, prev_q], old_p)
        p = jnp.exp2(s * c - l_v[q][0:1, :])
        if masked:
            kk = lax.broadcasted_iota(jnp.int32, (sub, bq), 0) + r * sub
            p = jnp.where(kk <= lax.broadcasted_iota(jnp.int32, (sub, bq), 1), p, 0.0)
        p = p.astype(BF16)
        dp = dot_nt(qkv[2, krows, :], do_v[piece(q), :])
        if prev is not None:
            dk_acc[:, prev_k] += dot_nn(qt_ref[:, prev_q], old_ds)
        ds = (p.astype(F32) * (dp - delta_v[q][0:1, :])).astype(BF16)
        out = dot_nn(kt_ref[:, prev_k], old_ds_t) if prev is not None else None
        p_ref[:, sl], ds_ref[sl, :], dst_ref[:, sl] = p.T, ds, ds.T
        return out

    def pair(q, k, prev, masked=False):
        out = half_pair(0, q, k, prev, masked)
        out = out + half_pair(1, q, k, prev, masked)
        dq_acc[:, piece(prev[0])] += out
        return q, k

    def source(kind, i):
        return (grads.at[pl.ds(0, 1), piece(i), :], grads.at[pl.ds(1, 2), piece(i), :], o_ref.at[piece(i), :])[kind]

    def target(kind, part, head):
        cols = rows_at(head * HEAD_DIM, HEAD_DIM)
        return (rows_ref.at[pl.ds(0, 1), piece(part), cols], rows_ref.at[pl.ds(1, 2), piece(part), cols], o_rows_ref.at[piece(part), cols])[kind]

    def send_kind(kind, i, start):
        send_piece(cp_size, i, source(kind, i), functools.partial(target, kind), send.at[kind], recv.at[kind], local.at[kind], start)

    def settle(kind):
        def sent(i, _):
            send_kind(kind, i, False)
            return 0

        lax.fori_loop(0, nblk, sent, 0)
        for d in range(1, cp_size):
            peer = lax.rem(me_c + d, cp_size)
            for half in range(2):
                pltpu.make_async_remote_copy(
                    src_ref=source(kind, 0), dst_ref=target(kind, half, peer), send_sem=send.at[kind, 0], recv_sem=recv.at[kind, peer, half],
                    device_id={'cp': peer}, device_id_type=MESH).wait_recv()

    lax.fori_loop(0, nblk, lambda i, _: (send_kind(2, i, True), 0)[1], 0)

    def finish_q(i):
        grads[0, piece(i), :] = (dq_acc[:, piece(i)] * scale).T.astype(BF16)
        send_kind(0, i, True)

    def finish_kv(i):
        grads[1, piece(i), :] = (dk_acc[:, piece(i)] * scale).T.astype(BF16)
        grads[2, piece(i), :] = dv_acc[:, piece(i)].T.astype(BF16)
        send_kind(1, i, True)

    for r in range(2):
        half_pair(r, 0, 0, None, True)
    prev = lax.fori_loop(1, nblk, lambda i, prev: pair(i, i, prev, True), (0, 0))

    def late_column(k, prev):
        prev = pair(k + 1, k, prev)
        finish_kv(jnp.where(k == half_blk, nblk - 1, k - 1))
        return lax.fori_loop(k + 2, nblk, lambda q, prev: pair(q, k, prev), prev)

    prev = lax.fori_loop(half_blk, nblk - 1, late_column, prev)

    def row(q, prev):
        prev = pair(q, 0, prev)

        @pl.when(q == 1)
        def _():
            finish_kv(nblk - 2)
            settle(2)
            for r in range(1, tp_size):
                over_tp(1, r).start()

        finish_q(q - 1)
        return lax.fori_loop(1, jnp.minimum(q, half_blk), lambda k, prev: pair(q, k, prev), prev)

    rows_done = half_blk + 2
    prev = lax.fori_loop(1, rows_done, row, prev)

    def column(n, prev):
        def key(n):
            return jnp.where(n < half_blk // 2, 2 * n, 2 * (n - half_blk // 2) + 1)

        prev = pair(rows_done, key(n), prev)

        @pl.when(n == 0)
        def _():
            finish_q(rows_done - 1)

        @pl.when(n > 0)
        def _():
            finish_kv(key(n - 1))

        return lax.fori_loop(rows_done + 1, nblk, lambda q, prev: pair(q, key(n), prev), prev)

    if rows_done < nblk:
        prev = lax.fori_loop(0, half_blk, column, prev)
    last_q, last_k = piece(prev[0]), piece(prev[1])
    dv_acc[:, last_k] += dot_nn(dot_ref[:, last_q], p_ref[...])
    dk_acc[:, last_k] += dot_nn(qt_ref[:, last_q], dst_ref[...])
    dq_acc[:, last_q] += dot_nn(kt_ref[:, last_k], ds_ref[...])
    if rows_done < nblk:
        finish_kv(half_blk - 1)
        lax.fori_loop(rows_done, nblk, lambda q, _: (finish_q(q), 0)[1], 0)
    else:
        lax.fori_loop(0, half_blk, lambda k, _: (finish_kv(k), 0)[1], 0)
        finish_q(rows_done - 1)

    settle(0)
    settle(1)
    for r in range(1, tp_size):
        over_tp(0, r).wait()
        over_tp(1, r).wait()


def backward(qkv, do, o, ot, lse, w_out, cp_size, tp_size):
    seq = qkv.shape[1]
    cols, width = w_out.shape
    block = seq // (cp_size * tp_size)
    share = cols // cp_size
    bq = seq // (2 * cp_size)
    pairs = seq * seq // 2
    turned = pltpu.VMEM((HEAD_DIM, seq), BF16)
    total = pltpu.VMEM((HEAD_DIM, seq), F32)
    square = pltpu.VMEM((bq, bq), BF16)
    return pl.pallas_call(
        functools.partial(backward_kernel, cp_size, tp_size),
        out_shape=(
            jax.ShapeDtypeStruct((3, 2 * bq, cols), BF16),
            jax.ShapeDtypeStruct((2 * bq, cols), BF16),
            jax.ShapeDtypeStruct((tp_size - 1, block, cols), BF16),
            jax.ShapeDtypeStruct((tp_size - 1, share, width), BF16),
        ),
        in_specs=[ANYWHERE] * 6,
        out_specs=(ANYWHERE,) * 4,
        scratch_shapes=[
            pltpu.VMEM(qkv.shape, BF16),
            pltpu.VMEM((seq, HEAD_DIM), BF16),
            turned,
            pltpu.VMEM(lse.shape, F32),
            pltpu.VMEM(lse.shape, F32),
            turned, turned, turned, square, square, square, total, total, total,
            pltpu.VMEM(qkv.shape, BF16),
            DMA((4,)), DMA((3, 2 * cp_size)), DMA((3, cp_size, 2)), DMA((3, 2)), DMA((2, tp_size)), DMA((2, tp_size)),
        ],
        compiler_params=params(2),
        cost_estimate=pl.CostEstimate(flops=10 * pairs * HEAD_DIM, bytes_accessed=16 * seq * HEAD_DIM, transcendentals=pairs),
        name="attention_backward",
    )(qkv, do, o, ot, lse, w_out)


def reduce_kernel(cp_size, tp_size, chunks, rows_ref, wq_ref, wk_ref, wv_ref, o_rows_ref, oy_ref, wo_ref, wy_ref,
                  out_ref, y_ref, wx_ref, sib_ref,
                  g_v, w_v, part, mid, last, out_v, stage, y_acc, o_v, in_sem, w_sem, out_sem, sends, recvs,
                  x_send, x_recv, d_send, d_recv, o_sem, s_sem):
    me, right, left = ring('tp', tp_size)
    far = lax.rem(me + 2, tp_size)
    block = part.shape[1]
    half = block // 2
    low, high = pl.ds(0, half), pl.ds(half, half)
    wide = part.shape[2] // chunks
    weights = (wq_ref, wk_ref, wv_ref)

    def w_load(n, a):
        return pltpu.make_async_copy(weights[a].at[rows_at(n * wide, wide), :], w_v.at[lax.rem(n, 2), a], w_sem.at[lax.rem(n, 2), a])

    load = pltpu.make_async_copy(rows_ref, g_v, in_sem)
    load.start()
    for a in range(3):
        w_load(0, a).start()
    me_c, mate = lax.axis_index('cp'), partner()
    chips = cp_size // 2
    ahead, behind = lax.rem(me_c + 2, cp_size), lax.rem(me_c + cp_size - 2, cp_size)
    nearest = (1, chips - 1) if chips > 2 else (1,)
    meet(*beside(tp_size), {'cp': mate}, *({'cp': peer} for peer in (ahead, behind)[:len(nearest)]))
    share = wy_ref.shape[1]

    def share_ref(s, k):
        return wy_ref.at[s] if k == 0 else wx_ref.at[s, k - 1]

    def x_copy(s, n, src, dst, peer):
        return pltpu.make_async_remote_copy(
            src_ref=src, dst_ref=dst, send_sem=x_send.at[s, n], recv_sem=x_recv.at[s, n], device_id={'cp': peer}, device_id_type=MESH)

    def along(s, n):
        return x_copy(s, n, wy_ref.at[s], wx_ref.at[s, nearest[n] - 1], (ahead, behind)[n])

    def relay(s, n):
        rows = pl.ds(n * (share // 2), share // 2)
        return x_copy(s, 2 + n, wx_ref.at[s, nearest[n] - 1, rows, :], wx_ref.at[s, 1, rows, :], (ahead, behind)[n])

    def across(s, k):
        return pltpu.make_async_remote_copy(
            src_ref=share_ref(s, k), dst_ref=sib_ref.at[s, k], send_sem=d_send.at[s, k], recv_sem=d_recv.at[s, k],
            device_id={'cp': mate}, device_id_type=MESH)

    slots = range(tp_size - 1)
    for s in slots:
        for n in range(len(nearest)):
            along(s, n).start()
        across(s, 0).start()
    o_loads = [pltpu.make_async_copy(o_rows_ref.at[rows_at(me * (o_rows_ref.shape[0] // tp_size), o_rows_ref.shape[0] // tp_size), :], o_v.at[0], o_sem.at[0])]
    for s in range(tp_size - 1):
        o_loads.append(pltpu.make_async_copy(oy_ref.at[s], o_v.at[s + 1], o_sem.at[s + 1]))
    for copy in o_loads:
        copy.start()

    kinds = ('far_r', 'far_l', 'plain_r', 'plain_l', 'sum_r', 'sum_l')

    def hop(kind, n):
        cols = rows_at(n * wide, wide)
        src, dst, peer = {
            'far_r': (part.at[FAR, low, cols], mid.at[0, :, cols], right),
            'far_l': (part.at[FAR, high, cols], mid.at[1, :, cols], left),
            'plain_r': (part.at[RIGHT, high, cols], last.at[0, high, cols], right),
            'plain_l': (part.at[LEFT, low, cols], last.at[1, low, cols], left),
            'sum_r': (part.at[RIGHT, low, cols], last.at[0, low, cols], right),
            'sum_l': (part.at[LEFT, high, cols], last.at[1, high, cols], left),
        }[kind]
        k = kinds.index(kind)
        return pltpu.make_async_remote_copy(
            src_ref=src, dst_ref=dst, send_sem=sends.at[k, n], recv_sem=recvs.at[k, n], device_id={'tp': peer}, device_id_type=MESH)

    load.wait()

    def compute(n, _):
        slot = lax.rem(n, 2)

        @pl.when(n + 1 < chunks)
        def _():
            for a in range(3):
                w_load(n + 1, a).start()

        for a in range(3):
            w_load(n, a).wait()
        cols = rows_at(n * wide, wide)
        ready = {FAR: ('far_r', 'far_l'), RIGHT: ('plain_r',), LEFT: ('plain_l',), OWN: ()}
        for k, owner in enumerate((far, right, left, me)):
            rows = rows_at(owner * block, block)
            total = dot_nt(g_v[0, rows, :], w_v[slot, 0])
            total = total + dot_nt(g_v[1, rows, :], w_v[slot, 1])
            part[k, :, cols] = total + dot_nt(g_v[2, rows, :], w_v[slot, 2])
            for kind in ready[k]:
                hop(kind, n).start()
        return 0

    lax.fori_loop(0, chunks, compute, 0)
    for s in slots:
        for n, k in enumerate(nearest):
            along(s, n).wait_recv()
            if chips > 2:
                relay(s, n).start()
            across(s, k).start()

    def forward_sums(n, _):
        cols = rows_at(n * wide, wide)
        hop('far_r', n).wait_recv()
        part[RIGHT, :half, cols] += mid[0, :, cols]
        hop('sum_r', n).start()
        hop('far_l', n).wait_recv()
        part[LEFT, half:, cols] += mid[1, :, cols]
        hop('sum_l', n).start()
        return 0

    lax.fori_loop(0, chunks, forward_sums, 0)

    if chips > 2:
        for s in slots:
            for n in range(2):
                relay(s, n).wait_recv()
            across(s, 2).start()
    for copy in o_loads:
        copy.wait()
    span = stage.shape[2]
    halves = y_acc.shape[1] // span

    def stage_copies(n):
        s, h = divmod(n, halves)
        cols = pl.ds(h * span, span)
        slot = n % 2
        if s == 0:
            return [pltpu.make_async_copy(wo_ref.at[:, cols], stage.at[slot], s_sem.at[slot, 0])]
        copies = []
        for k in range(cp_size // 2):
            mine, its = lax.rem(me_c + cp_size - 2 * k, cp_size), lax.rem(mate + cp_size - 2 * k, cp_size)
            copies.append(pltpu.make_async_copy(
                share_ref(s - 1, k).at[:, cols], stage.at[slot, rows_at(mine * share, share), :], s_sem.at[slot, 2 * k]))
            copies.append(pltpu.make_async_copy(
                sib_ref.at[s - 1, k, :, cols], stage.at[slot, rows_at(its * share, share), :], s_sem.at[slot, 2 * k + 1]))
        return copies

    def stage_start(n):
        s, h = divmod(n, halves)
        if s > 0 and h == 0:
            for k in range(cp_size // 2):
                across(s - 1, k).wait_recv()
        for copy in stage_copies(n):
            copy.start()

    total_steps = tp_size * halves
    stage_start(0)
    for n in range(total_steps):
        if n + 1 < total_steps:
            stage_start(n + 1)
        for copy in stage_copies(n):
            copy.wait()
        s, h = divmod(n, halves)
        tile = min(512, span)

        def y_step(j, _):
            cols = rows_at(j * tile, tile)
            out = rows_at(h * span + j * tile, tile)
            product = dot_nn(o_v[s], stage[n % 2, :, cols])
            if s == 0:
                y_acc[:, out] = product
            elif s < tp_size - 1:
                y_acc[:, out] += product
            else:
                out_v[:, out] = (y_acc[:, out] + product).astype(BF16)
            return 0

        lax.fori_loop(0, span // tile, y_step, 0)
    y_out = pltpu.make_async_copy(out_v, y_ref, in_sem)
    y_out.start()
    y_out.wait()

    def put(n):
        cols = rows_at(n * wide, wide)
        return pltpu.make_async_copy(out_v.at[:, cols], out_ref.at[:, cols], out_sem.at[n])

    def finish(n, _):
        cols = rows_at(n * wide, wide)
        for kind in ('plain_r', 'plain_l', 'sum_r', 'sum_l'):
            hop(kind, n).wait_recv()
        out_v[:, cols] = (part[OWN, :, cols] + last[0, :, cols] + last[1, :, cols]).astype(BF16)
        put(n).start()
        return 0

    lax.fori_loop(0, chunks, finish, 0)

    def close(n, _):
        put(n).wait()
        for kind in kinds:
            hop(kind, n).wait_send()
        return 0

    lax.fori_loop(0, chunks, close, 0)
    for s in slots:
        for k in range(chips):
            across(s, k).wait_send()
        for n in range(len(nearest)):
            along(s, n).wait_send()
            if chips > 2:
                relay(s, n).wait_send()


def reduce_out(grad_rows, weights, o_rows, oy, w_out, wy, cp_size, tp_size):
    width, cols = weights[0].shape
    share = wy.shape[1]
    pairs = cp_size // 2
    rows = grad_rows.shape[1]
    block = rows // tp_size
    chunks = 8
    wide = width // chunks
    return pl.pallas_call(
        functools.partial(reduce_kernel, cp_size, tp_size, chunks),
        out_shape=(
            jax.ShapeDtypeStruct((block, width), BF16),
            jax.ShapeDtypeStruct((block, width), BF16),
            jax.ShapeDtypeStruct((tp_size - 1, pairs - 1, share, width), BF16),
            jax.ShapeDtypeStruct((tp_size - 1, pairs, share, width), BF16),
        ),
        in_specs=[ANYWHERE] * 8,
        out_specs=(ANYWHERE,) * 4,
        scratch_shapes=[
            pltpu.VMEM((3, rows, cols), BF16),
            pltpu.VMEM((2, 3, wide, cols), BF16),
            pltpu.VMEM((4, block, width), F32),
            pltpu.VMEM((2, block // 2, width), F32),
            pltpu.VMEM((2, block, width), F32),
            pltpu.VMEM((block, width), BF16),
            pltpu.VMEM((2, cols, width // 4), BF16),
            pltpu.VMEM((block, width), F32),
            pltpu.VMEM((tp_size, block, cols), BF16),
            DMA, DMA((2, 3)), DMA((chunks,)), DMA((6, chunks)), DMA((6, chunks)),
            DMA((tp_size - 1, 4)), DMA((tp_size - 1, 4)), DMA((tp_size - 1, pairs)), DMA((tp_size - 1, pairs)),
            DMA((tp_size,)), DMA((2, cp_size)),
        ],
        compiler_params=params(3),
        cost_estimate=pl.CostEstimate(flops=6 * rows * width * cols, bytes_accessed=6 * width * cols, transcendentals=0),
        name="project_reduce",
    )(grad_rows, *weights, o_rows, oy, w_out, wy)


def solution(mesh):
    cp_size, tp_size = mesh.shape['cp'], mesh.shape['tp']
    row_spec = P(('dp', 'cp', 'tp'), None)

    def local_step(x_blk, dy_blk, w_query, w_key, w_value, w_out):
        weights = (w_query, w_key, w_value)
        qkv, dy1 = project(x_blk, dy_blk, weights, cp_size, tp_size)
        o, ot, lse, do = forward(qkv, dy_blk, dy1, w_out, cp_size, tp_size)
        grad_rows, o_rows, oy, wy = backward(qkv, do, o, ot, lse, w_out, cp_size, tp_size)
        dx_blk, y_blk, _, _ = reduce_out(grad_rows, weights, o_rows, oy, w_out, wy, cp_size, tp_size)
        return y_blk, dx_blk

    weight = P(None, 'tp')
    return jax.shard_map(local_step, mesh=mesh, in_specs=(row_spec, row_spec, weight, weight, weight, P('tp', None)), out_specs=(row_spec, row_spec), check_vma=False)
```

```python
import functools
import math

import jax
import jax.numpy as jnp
from jax import lax
from jax.experimental import pallas as pl
from jax.experimental.pallas import tpu as pltpu
from jax.sharding import PartitionSpec as P

HEAD_DIM = 128
F32, BF16 = jnp.float32, jnp.bfloat16
LOG2E = math.log2(math.e)
MESH = pl.DeviceIdType.MESH
ANYWHERE = pl.BlockSpec(memory_space=pltpu.HBM)
DMA = pltpu.SemaphoreType.DMA
FAR, RIGHT, LEFT, OWN = range(4)


def dot_nt(a, b):
    return lax.dot_general(a, b, (((1,), (1,)), ((), ())), preferred_element_type=F32)


def dot_nn(a, b):
    return lax.dot_general(a, b, (((1,), (0,)), ((), ())), preferred_element_type=F32)


def rows_at(start, size):
    return pl.ds(pl.multiple_of(start, size), size)


def ring(axis, size):
    me = lax.axis_index(axis)
    return me, lax.rem(me + 1, size), lax.rem(me + size - 1, size)


def meet(*peers):
    barrier = pltpu.get_barrier_semaphore()
    for peer in peers:
        pl.semaphore_signal(barrier, inc=1, device_id=peer, device_id_type=MESH)
    pl.semaphore_wait(barrier, len(peers))


def others(axis, size):
    me = lax.axis_index(axis)
    return [{axis: lax.rem(me + d, size)} for d in range(1, size)]


def beside(tp_size):
    _, right, left = ring('tp', tp_size)
    return [{'tp': right}, {'tp': left}]


def partner():
    me = lax.axis_index('cp')
    return me + 1 - 2 * lax.rem(me, 2)


def params(collective_id):
    return pltpu.CompilerParams(collective_id=collective_id, has_side_effects=True, vmem_limit_bytes=63 << 20)


def far_first(cp_size):
    return sorted(range(1, cp_size), key=lambda d: -min(d, cp_size - d))


def position(cp_size, tp_size, block, owner, row):
    piece = block * tp_size // 2
    first = owner < tp_size // 2
    cp_rank = lax.axis_index('cp')
    piece_id = jnp.where(first, cp_rank, 2 * cp_size - 1 - cp_rank)
    return piece_id * piece + jnp.where(first, owner, owner - tp_size // 2) * block + row


class Gather:
    STEPS = 6

    def __init__(self, tp_size, src, buf, send, recv):
        self.src, self.buf, self.sems = src, buf, (send, recv)
        self.me, self.right, self.left = ring('tp', tp_size)
        self.far = lax.rem(self.me + 2, tp_size)
        self.block = src.shape[0]
        self.part = self.block // 4

    def start_row(self, j):
        return self.block + (j - 1) * (2 * self.part)

    def rows(self, j, side):
        return self.buf.at[rows_at(self.start_row(j) + side * self.part, self.part), :]

    def first_row(self, j, side):
        return lax.rem(j + (1 if side else 3), 4) * self.part

    def parts(self, j):
        near = j <= 4
        return (
            (jnp.where(near, self.right, self.far), self.first_row(j, 0)),
            (jnp.where(near, self.left, self.far), self.first_row(j, 1)),
        )

    def hop(self, j, side, relayed):
        src = self.rows(j - 4, side) if relayed else self.src.at[rows_at(self.first_row(j, side), self.part), :]
        return pltpu.make_async_remote_copy(
            src_ref=src, dst_ref=self.rows(j, side),
            send_sem=self.sems[0].at[j - 1, side], recv_sem=self.sems[1].at[j - 1, side],
            device_id={'tp': self.right if side else self.left}, device_id_type=MESH)

    def start(self, j, relayed):
        for side in range(2):
            self.hop(j, side, relayed).start()

    def arrive(self, j):
        for side in range(2):
            self.hop(j, side, False).wait_recv()

    def leave(self, j):
        for side in range(2):
            self.hop(j, side, False).wait_send()


class HeadSender:
    def __init__(self, cp_size, tp_size, gather, res, dst, send, recv, local):
        self.cp_size, self.tp_size, self.gather = cp_size, tp_size, gather
        self.res, self.dst, self.sems = res, dst, (send, recv, local)

    def copies(self, j):
        send, recv, local = self.sems
        me = lax.axis_index('cp')
        own = isinstance(j, int)
        block = self.gather.block
        if own:
            start, length, parts = 0, block // 2, ((self.gather.me, 0), (self.gather.me, block // 2))
        else:
            start, length, parts = self.gather.start_row(j), self.gather.part, self.gather.parts(j)
        for n, (owner, row) in enumerate(parts):
            rows = rows_at(position(self.cp_size, self.tp_size, block, owner, row), length)
            here = rows_at(start + n * length, length)
            for d in far_first(self.cp_size):
                peer = lax.rem(me + d, self.cp_size)
                yield pltpu.make_async_remote_copy(
                    src_ref=self.res.at[peer, :, here, :], dst_ref=self.dst.at[:, rows, :],
                    send_sem=send.at[d - 1, j, n], recv_sem=recv.at[d - 1, j, n],
                    device_id={'cp': peer}, device_id_type=MESH)
            yield pltpu.make_async_copy(self.res.at[me, :, here, :], self.dst.at[:, rows, :], local.at[j, n])

    def start(self, j):
        for copy in self.copies(j):
            copy.start()

    def wait(self):
        for copy in self.copies(0):
            copy.wait()

        def step(j, _):
            for copy in self.copies(j):
                copy.wait()
            return 0

        lax.fori_loop(1, Gather.STEPS + 1, step, 0)


def head_sems(cp_size):
    each = (cp_size - 1, Gather.STEPS + 1, 2)
    return DMA(each), DMA(each), DMA(each[1:])


def project_phase(cp_size, tp_size, x_ref, weights, qkv, xg, dy_gather, send, recv, local, w_sem, x_sem, y_send, y_recv, w_v, res):
    block = x_ref.shape[0]
    gather = Gather(tp_size, x_ref, xg, y_send, y_recv)
    heads = HeadSender(cp_size, tp_size, gather, res, qkv, send, recv, local)
    own = pltpu.make_async_copy(x_ref, xg.at[pl.ds(0, block), :], x_sem)
    own.start()
    loads = [pltpu.make_async_copy(w, w_v.at[n], w_sem.at[n]) for n, w in enumerate(weights)]
    for j in range(1, 5):
        gather.start(j, False)
    for load in loads:
        load.start()
    own.wait()

    wide = min(4, cp_size)
    cols = wide * HEAD_DIM
    steps = cp_size // wide

    def compute(rows, n):
        def body(s, _):
            out = dot_nn(xg[rows, :], w_v[n, :, rows_at(s * cols, cols)]).astype(BF16)
            for k in range(wide):
                res[wide * s + k, n, rows, :] = out[:, k * HEAD_DIM:(k + 1) * HEAD_DIM]
            return 0

        lax.fori_loop(0, steps, body, 0)

    for n, load in enumerate(loads):
        load.wait()
        compute(pl.ds(0, block), n)
    heads.start(0)

    def step(j, _):
        gather.arrive(j)

        @pl.when(j <= 2)
        def _():
            gather.start(j + 4, True)

        @pl.when(j == 2)
        def _():
            for n in range(1, 5):
                dy_gather.start(n, False)

        rows = rows_at(gather.start_row(j), 2 * gather.part)
        lax.fori_loop(0, len(loads), lambda n, _: (compute(rows, n), 0)[1], 0)
        heads.start(j)
        return 0

    lax.fori_loop(1, Gather.STEPS + 1, step, 0)
    lax.fori_loop(1, Gather.STEPS + 1, lambda j, _: (gather.leave(j), 0)[1], 0)
    heads.wait()


def send_piece(cp_size, i, src, dst_of, send, recv, local, start):
    me = lax.axis_index('cp')
    half = jnp.where(i < cp_size, 0, 1)
    owner = jnp.where(i < cp_size, i, 2 * cp_size - 1 - i)

    @pl.when(owner == me)
    def _():
        copy = pltpu.make_async_copy(src, dst_of(half, me), local.at[half])
        copy.start() if start else copy.wait()

    @pl.when(owner != me)
    def _():
        copy = pltpu.make_async_remote_copy(
            src_ref=src, dst_ref=dst_of(half, me), send_sem=send.at[i], recv_sem=recv.at[me, half],
            device_id={'cp': owner}, device_id_type=MESH)
        copy.start() if start else copy.wait_send()


def forward_phase(cp_size, tp_size, gather, wo_ref, qkv, do_v, h_send, h_recv, h_local, in_sem, o_v, ot_v, l_v,
                  vt_ref, qt_ref, s_ref, acc_ref, wo, res):
    seq = qkv.shape[1]
    bq = s_ref.shape[0]
    nblk = seq // bq
    c = HEAD_DIM ** -0.5 * LOG2E
    heads = HeadSender(cp_size, tp_size, gather, res, do_v, h_send, h_recv, h_local)
    block = gather.block
    loads = [
        pltpu.make_async_copy(wo_ref, wo, in_sem.at[0]),
        pltpu.make_async_copy(gather.src, gather.buf.at[pl.ds(0, block), :], in_sem.at[1]),
    ]
    for load in loads:
        load.start()

    per_step = min(4, cp_size)
    cols = per_step * HEAD_DIM

    def compute(n):
        rows = rows_at(n * block, block)

        def body(s, _):
            out = dot_nt(gather.buf[rows, :], wo[rows_at(s * cols, cols), :]).astype(BF16)
            for k in range(per_step):
                res[per_step * s + k, 0, rows, :] = out[:, k * HEAD_DIM:(k + 1) * HEAD_DIM]
            return 0

        lax.fori_loop(0, cp_size // per_step, body, 0)

    def compute_steps(n):
        compute(n)
        lax.fori_loop(2 * n - 1, 2 * n + 1, lambda j, _: (heads.start(j), 0)[1], 0)

    def transpose_step(b, _):
        rows = rows_at(b * bq, bq)
        vt_ref[:, rows] = qkv[2, rows, :].T
        return 0

    lax.fori_loop(0, nblk, transpose_step, 0)

    def q_step(i, _):
        for n, at in enumerate((nblk // 4, nblk // 2, nblk - nblk // 4, nblk - 2)):
            @pl.when(i == at)
            def _():
                if n == 0:
                    for load in loads:
                        load.wait()
                    for j in range(1, 3):
                        gather.arrive(j)
                        gather.start(j + 4, True)
                    compute(0)
                    heads.start(0)
                else:
                    for j in range(max(3, 2 * n - 1), 2 * n + 1):
                        gather.arrive(j)
                    compute_steps(n)

        rows = rows_at(i * bq, bq)
        qt_ref[...] = qkv[0, rows, :].T
        acc_ref[...] = jnp.zeros_like(acc_ref)
        s = dot_nn(qkv[1, rows, :], qt_ref[...]) * c
        kk = lax.broadcasted_iota(jnp.int32, (bq, bq), 0)
        qq = lax.broadcasted_iota(jnp.int32, (bq, bq), 1)
        s = jnp.where(kk <= qq, s, -jnp.inf)
        s_ref[...] = s
        first = jnp.max(s, axis=0, keepdims=True)

        def use(blk, m_old, m, l, following):
            alpha = jnp.exp2(m_old - m)
            p = jnp.exp2(s_ref[...] - m)
            m_new = m
            if following is not None:
                s = dot_nn(qkv[1, rows_at(following * bq, bq), :], qt_ref[...]) * c
            part = jnp.sum(p, axis=0, keepdims=True)
            out = dot_nn(vt_ref[:, rows_at(blk * bq, bq)], p.astype(BF16))
            if following is not None:
                m_new = jnp.maximum(m, jnp.max(s, axis=0, keepdims=True))
                s_ref[...] = s
            acc_ref[...] = acc_ref[...] * alpha + out
            return m, m_new, l * alpha + part

        def body(t, carry):
            return use(jnp.where(t == 0, i, t - 1), *carry, t)

        carry = lax.fori_loop(0, i, body, (first, first, jnp.zeros((1, bq), F32)))
        m, _, l = use(jnp.where(i == 0, i, i - 1), *carry, None)
        out = (acc_ref[...] * (1.0 / l)).astype(BF16)
        ot_v[:, rows] = out
        o_v[rows, :] = out.T
        l_v[i] = jnp.broadcast_to(m + jnp.log2(l), (8, bq))
        return 0

    lax.fori_loop(0, nblk, q_step, 0)
    heads.wait()
    lax.fori_loop(1, Gather.STEPS + 1, lambda j, _: (gather.leave(j), 0)[1], 0)


def backward_phase(cp_size, tp_size, wo_ref, rows_ref, o_rows_ref, oy_ref, wy_ref, qkv, do_v, o_v, ot_v, l_v,
                   send, recv, local, y_send, y_recv,
                   delta_v, kt_ref, qt_ref, dot_ref, p_ref, ds_ref, dst_ref, dq_acc, dk_acc, dv_acc, grads):
    seq = qkv.shape[1]
    bq = p_ref.shape[0]
    nblk, half_blk = 2 * cp_size, cp_size
    sub = bq // 2
    scale = HEAD_DIM ** -0.5
    c = scale * LOG2E
    me_c, me_t = lax.axis_index('cp'), lax.axis_index('tp')
    share, block = wy_ref.shape[1], oy_ref.shape[1]

    def over_tp(kind, r):
        peer = lax.rem(me_t + r, tp_size)
        src, dst = ((wo_ref.at[rows_at(me_c * share, share), :], wy_ref), (o_rows_ref.at[rows_at(peer * block, block), :], oy_ref))[kind]
        return pltpu.make_async_remote_copy(
            src_ref=src, dst_ref=dst.at[r - 1], send_sem=y_send.at[kind, r - 1], recv_sem=y_recv.at[kind, r - 1],
            device_id={'tp': peer}, device_id_type=MESH)

    for r in range(1, tp_size):
        over_tp(0, r).start()

    def piece(i):
        return rows_at(i * bq, bq)

    def init_step(b, _):
        rows = piece(b)
        kt_ref[:, rows] = qkv[1, rows, :].T
        qt_ref[:, rows] = qkv[0, rows, :].T
        dot_ref[:, rows] = do_v[0, rows, :].T
        prod = dot_ref[:, rows].astype(F32) * ot_v[:, rows].astype(F32)
        delta_v[b] = jnp.broadcast_to(jnp.sum(prod, axis=0, keepdims=True), (8, bq))
        for acc in (dq_acc, dk_acc, dv_acc):
            acc[:, rows] = jnp.zeros((HEAD_DIM, bq), F32)
        return 0

    lax.fori_loop(0, nblk, init_step, 0)

    def half_pair(r, q, k, prev, masked):
        sl = slice(r * sub, (r + 1) * sub)
        krows = rows_at(k * bq + r * sub, sub)
        if prev is not None:
            prev_q, prev_k = piece(prev[0]), rows_at(prev[1] * bq + r * sub, sub)
            old_p, old_ds_t, old_ds = p_ref[:, sl], ds_ref[sl, :], dst_ref[:, sl]
        s = dot_nn(qkv[1, krows, :], qt_ref[:, piece(q)])
        if prev is not None:
            dv_acc[:, prev_k] += dot_nn(dot_ref[:, prev_q], old_p)
        p = jnp.exp2(s * c - l_v[q][0:1, :])
        if masked:
            kk = lax.broadcasted_iota(jnp.int32, (sub, bq), 0) + r * sub
            p = jnp.where(kk <= lax.broadcasted_iota(jnp.int32, (sub, bq), 1), p, 0.0)
        p = p.astype(BF16)
        dp = dot_nn(qkv[2, krows, :], dot_ref[:, piece(q)])
        if prev is not None:
            dk_acc[:, prev_k] += dot_nn(qt_ref[:, prev_q], old_ds)
        ds = (p.astype(F32) * (dp - delta_v[q][0:1, :])).astype(BF16)
        out = dot_nn(kt_ref[:, prev_k], old_ds_t) if prev is not None else None
        p_ref[:, sl], ds_ref[sl, :], dst_ref[:, sl] = p.T, ds, ds.T
        return out

    def pair(q, k, prev, masked=False):
        out = half_pair(0, q, k, prev, masked)
        out = out + half_pair(1, q, k, prev, masked)
        dq_acc[:, piece(prev[0])] += out
        return q, k

    def source(kind, i):
        return (grads.at[pl.ds(0, 1), piece(i), :], grads.at[pl.ds(1, 2), piece(i), :], o_v.at[piece(i), :])[kind]

    def target(kind, part, head):
        cols = rows_at(head * HEAD_DIM, HEAD_DIM)
        return (rows_ref.at[pl.ds(0, 1), piece(part), cols], rows_ref.at[pl.ds(1, 2), piece(part), cols], o_rows_ref.at[piece(part), cols])[kind]

    def send_kind(kind, i, start):
        send_piece(cp_size, i, source(kind, i), functools.partial(target, kind), send.at[kind], recv.at[kind], local.at[kind], start)

    def settle(kind):
        def sent(i, _):
            send_kind(kind, i, False)
            return 0

        lax.fori_loop(0, nblk, sent, 0)
        for d in range(1, cp_size):
            peer = lax.rem(me_c + d, cp_size)
            for half in range(2):
                pltpu.make_async_remote_copy(
                    src_ref=source(kind, 0), dst_ref=target(kind, half, peer), send_sem=send.at[kind, 0], recv_sem=recv.at[kind, peer, half],
                    device_id={'cp': peer}, device_id_type=MESH).wait_recv()

    lax.fori_loop(0, nblk, lambda i, _: (send_kind(2, i, True), 0)[1], 0)

    def finish_q(i):
        grads[0, piece(i), :] = (dq_acc[:, piece(i)] * scale).T.astype(BF16)
        send_kind(0, i, True)

    def finish_kv(i):
        grads[1, piece(i), :] = (dk_acc[:, piece(i)] * scale).T.astype(BF16)
        grads[2, piece(i), :] = dv_acc[:, piece(i)].T.astype(BF16)
        send_kind(1, i, True)

    for r in range(2):
        half_pair(r, 0, 0, None, True)
    prev = lax.fori_loop(1, nblk, lambda i, prev: pair(i, i, prev, True), (0, 0))

    def late_column(k, prev):
        prev = pair(k + 1, k, prev)
        finish_kv(jnp.where(k == half_blk, nblk - 1, k - 1))
        return lax.fori_loop(k + 2, nblk, lambda q, prev: pair(q, k, prev), prev)

    prev = lax.fori_loop(half_blk, nblk - 1, late_column, prev)

    def row(q, prev):
        prev = pair(q, 0, prev)

        @pl.when(q == 1)
        def _():
            finish_kv(nblk - 2)
            settle(2)
            for r in range(1, tp_size):
                over_tp(1, r).start()

        finish_q(q - 1)
        return lax.fori_loop(1, jnp.minimum(q, half_blk), lambda k, prev: pair(q, k, prev), prev)

    rows_done = half_blk + 2
    prev = lax.fori_loop(1, rows_done, row, prev)

    def column(n, prev):
        def key(n):
            return jnp.where(n < half_blk // 2, 2 * n, 2 * (n - half_blk // 2) + 1)

        prev = pair(rows_done, key(n), prev)

        @pl.when(n == 0)
        def _():
            finish_q(rows_done - 1)

        @pl.when(n > 0)
        def _():
            finish_kv(key(n - 1))

        return lax.fori_loop(rows_done + 1, nblk, lambda q, prev: pair(q, key(n), prev), prev)

    if rows_done < nblk:
        prev = lax.fori_loop(0, half_blk, column, prev)
    last_q, last_k = piece(prev[0]), piece(prev[1])
    dv_acc[:, last_k] += dot_nn(dot_ref[:, last_q], p_ref[...])
    dk_acc[:, last_k] += dot_nn(qt_ref[:, last_q], dst_ref[...])
    dq_acc[:, last_q] += dot_nn(kt_ref[:, last_k], ds_ref[...])
    if rows_done < nblk:
        finish_kv(half_blk - 1)
        lax.fori_loop(rows_done, nblk, lambda q, _: (finish_q(q), 0)[1], 0)
    else:
        lax.fori_loop(0, half_blk, lambda k, _: (finish_kv(k), 0)[1], 0)
        finish_q(rows_done - 1)

    settle(0)
    settle(1)
    for r in range(1, tp_size):
        over_tp(0, r).wait()
        over_tp(1, r).wait()


def layer_kernel(cp_size, tp_size, x_ref, dy_ref, wq_ref, wk_ref, wv_ref, wo_ref, rows_ref, o_rows_ref, oy_ref, wy_ref,
                 qkv, do_v, xg, dyg, w_sem, in_sem, p_send, p_recv, p_local, h_send, h_recv, h_local,
                 x_send, x_recv, g_send, g_recv, send, recv, local, y_send, y_recv):
    seq = qkv.shape[1]
    bq = seq // (2 * cp_size)
    meet(*others('cp', cp_size), *others('tp', tp_size))
    gather = Gather(tp_size, dy_ref, dyg, g_send, g_recv)
    pl.run_scoped(
        functools.partial(
            project_phase, cp_size, tp_size, x_ref, (wq_ref, wk_ref, wv_ref), qkv, xg, gather,
            p_send, p_recv, p_local, w_sem, in_sem.at[0], x_send, x_recv),
        pltpu.VMEM((3, *wq_ref.shape), BF16), pltpu.VMEM((cp_size, 3, xg.shape[0], HEAD_DIM), BF16))
    turned, total, square = pltpu.VMEM((HEAD_DIM, seq), BF16), pltpu.VMEM((HEAD_DIM, seq), F32), pltpu.VMEM((bq, bq), BF16)
    logs = pltpu.VMEM((2 * cp_size, 8, bq), F32)

    def attend(o_v, ot_v, l_v):
        pl.run_scoped(
            functools.partial(forward_phase, cp_size, tp_size, gather, wo_ref, qkv, do_v, h_send, h_recv, h_local, in_sem, o_v, ot_v, l_v),
            turned, pltpu.VMEM((HEAD_DIM, bq), BF16), pltpu.VMEM((bq, bq), F32), pltpu.VMEM((HEAD_DIM, bq), F32),
            pltpu.VMEM(wo_ref.shape, BF16), pltpu.VMEM((cp_size, 1, dyg.shape[0], HEAD_DIM), BF16))
        pl.run_scoped(
            functools.partial(
                backward_phase, cp_size, tp_size, wo_ref, rows_ref, o_rows_ref, oy_ref, wy_ref, qkv, do_v, o_v, ot_v, l_v,
                send, recv, local, y_send, y_recv),
            logs, turned, turned, turned, square, square, square, total, total, total, pltpu.VMEM(qkv.shape, BF16))

    pl.run_scoped(attend, pltpu.VMEM((seq, HEAD_DIM), BF16), turned, logs)


def layer(x_blk, dy_blk, weights, w_out, cp_size, tp_size):
    block, width = x_blk.shape
    cols = w_out.shape[0]
    rows = block * tp_size
    seq = rows * cp_size
    pairs = seq * seq // 2
    each = DMA((Gather.STEPS, 2))
    gathered = pltpu.VMEM((rows, width), BF16)
    return pl.pallas_call(
        functools.partial(layer_kernel, cp_size, tp_size),
        out_shape=(
            jax.ShapeDtypeStruct((3, rows, cols), BF16),
            jax.ShapeDtypeStruct((rows, cols), BF16),
            jax.ShapeDtypeStruct((tp_size - 1, block, cols), BF16),
            jax.ShapeDtypeStruct((tp_size - 1, cols // cp_size, width), BF16),
        ),
        in_specs=[ANYWHERE] * 6,
        out_specs=(ANYWHERE,) * 4,
        scratch_shapes=[
            pltpu.VMEM((3, seq, HEAD_DIM), BF16),
            pltpu.VMEM((1, seq, HEAD_DIM), BF16),
            gathered, gathered, DMA((3,)), DMA((2,)), *head_sems(cp_size), *head_sems(cp_size), each, each, each, each,
            DMA((3, 2 * cp_size)), DMA((3, cp_size, 2)), DMA((3, 2)), DMA((2, tp_size)), DMA((2, tp_size)),
        ],
        compiler_params=params(0),
        cost_estimate=pl.CostEstimate(flops=14 * pairs * HEAD_DIM + 8 * rows * width * cols, bytes_accessed=8 * width * cols, transcendentals=2 * pairs),
        name="project_attend",
    )(x_blk, dy_blk, *weights, w_out)


def reduce_kernel(cp_size, tp_size, chunks, rows_ref, wq_ref, wk_ref, wv_ref, o_rows_ref, oy_ref, wo_ref, wy_ref,
                  out_ref, y_ref, wx_ref, sib_ref,
                  g_v, w_v, part, mid, last, out_v, stage, y_acc, o_v, in_sem, w_sem, out_sem, sends, recvs,
                  x_send, x_recv, d_send, d_recv, o_sem, s_sem):
    me, right, left = ring('tp', tp_size)
    far = lax.rem(me + 2, tp_size)
    block = part.shape[1]
    half = block // 2
    low, high = pl.ds(0, half), pl.ds(half, half)
    wide = part.shape[2] // chunks
    weights = (wq_ref, wk_ref, wv_ref)

    def w_load(n, a):
        return pltpu.make_async_copy(weights[a].at[rows_at(n * wide, wide), :], w_v.at[lax.rem(n, 2), a], w_sem.at[lax.rem(n, 2), a])

    owners = (far, right, left, me)
    blocks = [rows_at(owner * block, block) for owner in owners]
    loads = [pltpu.make_async_copy(rows_ref.at[:, rows, :], g_v.at[:, rows, :], in_sem.at[k]) for k, rows in enumerate(blocks)]
    loads[FAR].start()
    for a in range(3):
        w_load(0, a).start()
    for load in loads[RIGHT:]:
        load.start()
    me_c, mate = lax.axis_index('cp'), partner()
    chips = cp_size // 2
    ahead, behind = lax.rem(me_c + 2, cp_size), lax.rem(me_c + cp_size - 2, cp_size)
    nearest = (1, chips - 1) if chips > 2 else (1,)
    meet(*beside(tp_size), {'cp': mate}, *({'cp': peer} for peer in (ahead, behind)[:len(nearest)]))
    share = wy_ref.shape[1]

    def share_ref(s, k):
        return wy_ref.at[s] if k == 0 else wx_ref.at[s, k - 1]

    def x_copy(s, n, src, dst, peer):
        return pltpu.make_async_remote_copy(
            src_ref=src, dst_ref=dst, send_sem=x_send.at[s, n], recv_sem=x_recv.at[s, n], device_id={'cp': peer}, device_id_type=MESH)

    def along(s, n):
        return x_copy(s, n, wy_ref.at[s], wx_ref.at[s, nearest[n] - 1], (ahead, behind)[n])

    def relay(s, n):
        rows = pl.ds(n * (share // 2), share // 2)
        return x_copy(s, 2 + n, wx_ref.at[s, nearest[n] - 1, rows, :], wx_ref.at[s, 1, rows, :], (ahead, behind)[n])

    def across(s, k):
        return pltpu.make_async_remote_copy(
            src_ref=share_ref(s, k), dst_ref=sib_ref.at[s, k], send_sem=d_send.at[s, k], recv_sem=d_recv.at[s, k],
            device_id={'cp': mate}, device_id_type=MESH)

    slots = range(tp_size - 1)
    for s in slots:
        for n in range(len(nearest)):
            along(s, n).start()
        across(s, 0).start()
    o_loads = [pltpu.make_async_copy(o_rows_ref.at[rows_at(me * (o_rows_ref.shape[0] // tp_size), o_rows_ref.shape[0] // tp_size), :], o_v.at[0], o_sem.at[0])]
    for s in range(tp_size - 1):
        o_loads.append(pltpu.make_async_copy(oy_ref.at[s], o_v.at[s + 1], o_sem.at[s + 1]))
    for copy in o_loads:
        copy.start()

    kinds = ('far_r', 'far_l', 'plain_r', 'plain_l', 'sum_r', 'sum_l')

    def hop(kind, n):
        cols = rows_at(n * wide, wide)
        src, dst, peer = {
            'far_r': (part.at[FAR, low, cols], mid.at[0, :, cols], right),
            'far_l': (part.at[FAR, high, cols], mid.at[1, :, cols], left),
            'plain_r': (part.at[RIGHT, high, cols], last.at[0, high, cols], right),
            'plain_l': (part.at[LEFT, low, cols], last.at[1, low, cols], left),
            'sum_r': (part.at[RIGHT, low, cols], last.at[0, low, cols], right),
            'sum_l': (part.at[LEFT, high, cols], last.at[1, high, cols], left),
        }[kind]
        k = kinds.index(kind)
        return pltpu.make_async_remote_copy(
            src_ref=src, dst_ref=dst, send_sem=sends.at[k, n], recv_sem=recvs.at[k, n], device_id={'tp': peer}, device_id_type=MESH)

    def compute(n, _):
        slot = lax.rem(n, 2)

        @pl.when(n + 1 < chunks)
        def _():
            for a in range(3):
                w_load(n + 1, a).start()

        for a in range(3):
            w_load(n, a).wait()
        cols = rows_at(n * wide, wide)
        ready = {FAR: ('far_r', 'far_l'), RIGHT: ('plain_r',), LEFT: ('plain_l',), OWN: ()}
        for k, rows in enumerate(blocks):
            @pl.when(n == 0)
            def _():
                loads[k].wait()

            total = dot_nt(g_v[0, rows, :], w_v[slot, 0])
            total = total + dot_nt(g_v[1, rows, :], w_v[slot, 1])
            part[k, :, cols] = total + dot_nt(g_v[2, rows, :], w_v[slot, 2])
            for kind in ready[k]:
                hop(kind, n).start()
        return 0

    lax.fori_loop(0, chunks, compute, 0)
    for s in slots:
        for n, k in enumerate(nearest):
            along(s, n).wait_recv()
            if chips > 2:
                relay(s, n).start()
            across(s, k).start()

    def forward_sums(n, _):
        cols = rows_at(n * wide, wide)
        hop('far_r', n).wait_recv()
        part[RIGHT, :half, cols] += mid[0, :, cols]
        hop('sum_r', n).start()
        hop('far_l', n).wait_recv()
        part[LEFT, half:, cols] += mid[1, :, cols]
        hop('sum_l', n).start()
        return 0

    lax.fori_loop(0, chunks, forward_sums, 0)

    if chips > 2:
        for s in slots:
            for n in range(2):
                relay(s, n).wait_recv()
            across(s, 2).start()
    for copy in o_loads:
        copy.wait()
    span = stage.shape[2]
    halves = y_acc.shape[1] // span

    def stage_copies(n):
        s, h = divmod(n, halves)
        cols = pl.ds(h * span, span)
        slot = n % 2
        if s == 0:
            return [pltpu.make_async_copy(wo_ref.at[:, cols], stage.at[slot], s_sem.at[slot, 0])]
        copies = []
        for k in range(cp_size // 2):
            mine, its = lax.rem(me_c + cp_size - 2 * k, cp_size), lax.rem(mate + cp_size - 2 * k, cp_size)
            copies.append(pltpu.make_async_copy(
                share_ref(s - 1, k).at[:, cols], stage.at[slot, rows_at(mine * share, share), :], s_sem.at[slot, 2 * k]))
            copies.append(pltpu.make_async_copy(
                sib_ref.at[s - 1, k, :, cols], stage.at[slot, rows_at(its * share, share), :], s_sem.at[slot, 2 * k + 1]))
        return copies

    def stage_start(n):
        s, h = divmod(n, halves)
        if s > 0 and h == 0:
            for k in range(cp_size // 2):
                across(s - 1, k).wait_recv()
        for copy in stage_copies(n):
            copy.start()

    total_steps = tp_size * halves
    stage_start(0)
    for n in range(total_steps):
        if n + 1 < total_steps:
            stage_start(n + 1)
        for copy in stage_copies(n):
            copy.wait()
        s, h = divmod(n, halves)
        tile = min(512, span)

        def y_step(j, _):
            cols = rows_at(j * tile, tile)
            out = rows_at(h * span + j * tile, tile)
            product = dot_nn(o_v[s], stage[n % 2, :, cols])
            if s == 0:
                y_acc[:, out] = product
            elif s < tp_size - 1:
                y_acc[:, out] += product
            else:
                out_v[:, out] = (y_acc[:, out] + product).astype(BF16)
            return 0

        lax.fori_loop(0, span // tile, y_step, 0)
    y_out = pltpu.make_async_copy(out_v, y_ref, in_sem.at[OWN])
    y_out.start()
    y_out.wait()

    def put(n):
        cols = rows_at(n * wide, wide)
        return pltpu.make_async_copy(out_v.at[:, cols], out_ref.at[:, cols], out_sem.at[n])

    def finish(n, _):
        cols = rows_at(n * wide, wide)
        for kind in ('plain_r', 'plain_l', 'sum_r', 'sum_l'):
            hop(kind, n).wait_recv()
        out_v[:, cols] = (part[OWN, :, cols] + last[0, :, cols] + last[1, :, cols]).astype(BF16)
        put(n).start()
        return 0

    lax.fori_loop(0, chunks, finish, 0)

    def close(n, _):
        put(n).wait()
        for kind in kinds:
            hop(kind, n).wait_send()
        return 0

    lax.fori_loop(0, chunks, close, 0)
    for s in slots:
        for k in range(chips):
            across(s, k).wait_send()
        for n in range(len(nearest)):
            along(s, n).wait_send()
            if chips > 2:
                relay(s, n).wait_send()


def reduce_out(grad_rows, weights, o_rows, oy, w_out, wy, cp_size, tp_size):
    width, cols = weights[0].shape
    share = wy.shape[1]
    pairs = cp_size // 2
    rows = grad_rows.shape[1]
    block = rows // tp_size
    chunks = 8
    wide = width // chunks
    return pl.pallas_call(
        functools.partial(reduce_kernel, cp_size, tp_size, chunks),
        out_shape=(
            jax.ShapeDtypeStruct((block, width), BF16),
            jax.ShapeDtypeStruct((block, width), BF16),
            jax.ShapeDtypeStruct((tp_size - 1, pairs - 1, share, width), BF16),
            jax.ShapeDtypeStruct((tp_size - 1, pairs, share, width), BF16),
        ),
        in_specs=[ANYWHERE] * 8,
        out_specs=(ANYWHERE,) * 4,
        scratch_shapes=[
            pltpu.VMEM((3, rows, cols), BF16),
            pltpu.VMEM((2, 3, wide, cols), BF16),
            pltpu.VMEM((4, block, width), F32),
            pltpu.VMEM((2, block // 2, width), F32),
            pltpu.VMEM((2, block, width), F32),
            pltpu.VMEM((block, width), BF16),
            pltpu.VMEM((2, cols, width // 4), BF16),
            pltpu.VMEM((block, width), F32),
            pltpu.VMEM((tp_size, block, cols), BF16),
            DMA((4,)), DMA((2, 3)), DMA((chunks,)), DMA((6, chunks)), DMA((6, chunks)),
            DMA((tp_size - 1, 4)), DMA((tp_size - 1, 4)), DMA((tp_size - 1, pairs)), DMA((tp_size - 1, pairs)),
            DMA((tp_size,)), DMA((2, cp_size)),
        ],
        compiler_params=params(1),
        cost_estimate=pl.CostEstimate(flops=6 * rows * width * cols, bytes_accessed=6 * width * cols, transcendentals=0),
        name="project_reduce",
    )(grad_rows, *weights, o_rows, oy, w_out, wy)


def solution(mesh):
    cp_size, tp_size = mesh.shape['cp'], mesh.shape['tp']
    row_spec = P(('dp', 'cp', 'tp'), None)

    def local_step(x_blk, dy_blk, w_query, w_key, w_value, w_out):
        weights = (w_query, w_key, w_value)
        grad_rows, o_rows, oy, wy = layer(x_blk, dy_blk, weights, w_out, cp_size, tp_size)
        dx_blk, y_blk, _, _ = reduce_out(grad_rows, weights, o_rows, oy, w_out, wy, cp_size, tp_size)
        return y_blk, dx_blk

    weight = P(None, 'tp')
    return jax.shard_map(local_step, mesh=mesh, in_specs=(row_spec, row_spec, weight, weight, weight, P('tp', None)), out_specs=(row_spec, row_spec), check_vma=False)
```

```python
import functools
import math

import jax
import jax.numpy as jnp
from jax import lax
from jax.experimental import pallas as pl
from jax.experimental.pallas import tpu as pltpu
from jax.sharding import PartitionSpec as P

HEAD_DIM = 128
F32, BF16 = jnp.float32, jnp.bfloat16
LOG2E = math.log2(math.e)
MESH = pl.DeviceIdType.MESH
ANYWHERE = pl.BlockSpec(memory_space=pltpu.HBM)
DMA = pltpu.SemaphoreType.DMA
FAR, RIGHT, LEFT, OWN = range(4)


def dot_nt(a, b):
    return lax.dot_general(a, b, (((1,), (1,)), ((), ())), preferred_element_type=F32)


def dot_nn(a, b):
    return lax.dot_general(a, b, (((1,), (0,)), ((), ())), preferred_element_type=F32)


def rows_at(start, size):
    return pl.ds(pl.multiple_of(start, size), size)


def ring(axis, size):
    me = lax.axis_index(axis)
    return me, lax.rem(me + 1, size), lax.rem(me + size - 1, size)


def meet(*peers):
    barrier = pltpu.get_barrier_semaphore()
    for peer in peers:
        pl.semaphore_signal(barrier, inc=1, device_id=peer, device_id_type=MESH)
    pl.semaphore_wait(barrier, len(peers))


def others(axis, size):
    me = lax.axis_index(axis)
    return [{axis: lax.rem(me + d, size)} for d in range(1, size)]


def beside(tp_size):
    _, right, left = ring('tp', tp_size)
    return [{'tp': right}, {'tp': left}]


def partner():
    me = lax.axis_index('cp')
    return me + 1 - 2 * lax.rem(me, 2)


def params(collective_id):
    return pltpu.CompilerParams(collective_id=collective_id, has_side_effects=True, vmem_limit_bytes=63 << 20)


def far_first(cp_size):
    return sorted(range(1, cp_size), key=lambda d: -min(d, cp_size - d))


def in_pairs(low, high, body, carry):
    count = lax.div(high - low, 2)
    carry = lax.fori_loop(0, count, lambda n, carry: body(low + 2 * n + 1, body(low + 2 * n, carry)), carry)
    return lax.fori_loop(low + 2 * count, high, body, carry)


def position(cp_size, tp_size, block, owner, row):
    piece = block * tp_size // 2
    first = owner < tp_size // 2
    cp_rank = lax.axis_index('cp')
    piece_id = jnp.where(first, cp_rank, 2 * cp_size - 1 - cp_rank)
    return piece_id * piece + jnp.where(first, owner, owner - tp_size // 2) * block + row


class Gather:
    STEPS = 6

    def __init__(self, tp_size, src, buf, send, recv):
        self.src, self.buf, self.sems = src, buf, (send, recv)
        self.me, self.right, self.left = ring('tp', tp_size)
        self.far = lax.rem(self.me + 2, tp_size)
        self.block = src.shape[0]
        self.part = self.block // 4

    def start_row(self, j):
        return self.block + (j - 1) * (2 * self.part)

    def rows(self, j, side):
        return self.buf.at[rows_at(self.start_row(j) + side * self.part, self.part), :]

    def first_row(self, j, side):
        return lax.rem(j + (1 if side else 3), 4) * self.part

    def parts(self, j):
        near = j <= 4
        return (
            (jnp.where(near, self.right, self.far), self.first_row(j, 0)),
            (jnp.where(near, self.left, self.far), self.first_row(j, 1)),
        )

    def hop(self, j, side, relayed):
        src = self.rows(j - 4, side) if relayed else self.src.at[rows_at(self.first_row(j, side), self.part), :]
        return pltpu.make_async_remote_copy(
            src_ref=src, dst_ref=self.rows(j, side),
            send_sem=self.sems[0].at[j - 1, side], recv_sem=self.sems[1].at[j - 1, side],
            device_id={'tp': self.right if side else self.left}, device_id_type=MESH)

    def start(self, j, relayed):
        for side in range(2):
            self.hop(j, side, relayed).start()

    def arrive(self, j):
        for side in range(2):
            self.hop(j, side, False).wait_recv()

    def leave(self, j):
        for side in range(2):
            self.hop(j, side, False).wait_send()


class HeadSender:
    def __init__(self, cp_size, tp_size, gather, res, dst, send, recv, local):
        self.cp_size, self.tp_size, self.gather = cp_size, tp_size, gather
        self.res, self.dst, self.sems = res, dst, (send, recv, local)

    def copies(self, j):
        send, recv, local = self.sems
        me = lax.axis_index('cp')
        own = isinstance(j, int)
        block = self.gather.block
        if own:
            start, length, parts = 0, block // 2, ((self.gather.me, 0), (self.gather.me, block // 2))
        else:
            start, length, parts = self.gather.start_row(j), self.gather.part, self.gather.parts(j)
        for n, (owner, row) in enumerate(parts):
            rows = rows_at(position(self.cp_size, self.tp_size, block, owner, row), length)
            here = rows_at(start + n * length, length)
            for d in far_first(self.cp_size):
                peer = lax.rem(me + d, self.cp_size)
                yield pltpu.make_async_remote_copy(
                    src_ref=self.res.at[peer, :, here, :], dst_ref=self.dst.at[:, rows, :],
                    send_sem=send.at[d - 1, j, n], recv_sem=recv.at[d - 1, j, n],
                    device_id={'cp': peer}, device_id_type=MESH)
            yield pltpu.make_async_copy(self.res.at[me, :, here, :], self.dst.at[:, rows, :], local.at[j, n])

    def start(self, j):
        for copy in self.copies(j):
            copy.start()

    def wait(self):
        for copy in self.copies(0):
            copy.wait()

        def step(j, _):
            for copy in self.copies(j):
                copy.wait()
            return 0

        lax.fori_loop(1, Gather.STEPS + 1, step, 0)


def head_sems(cp_size):
    each = (cp_size - 1, Gather.STEPS + 1, 2)
    return DMA(each), DMA(each), DMA(each[1:])


def project_phase(cp_size, tp_size, x_ref, weights, qkv, xg, dy_gather, send, recv, local, w_sem, x_sem, y_send, y_recv, w_v, res):
    block = x_ref.shape[0]
    gather = Gather(tp_size, x_ref, xg, y_send, y_recv)
    heads = HeadSender(cp_size, tp_size, gather, res, qkv, send, recv, local)
    own = pltpu.make_async_copy(x_ref, xg.at[pl.ds(0, block), :], x_sem)
    own.start()
    loads = [pltpu.make_async_copy(w, w_v.at[n], w_sem.at[n]) for n, w in enumerate(weights)]
    for j in range(1, 5):
        gather.start(j, False)
    for load in loads:
        load.start()
    own.wait()

    wide = min(4, cp_size)
    cols = wide * HEAD_DIM
    steps = cp_size // wide

    def compute(rows, n):
        def body(s, _):
            out = dot_nn(xg[rows, :], w_v[n, :, rows_at(s * cols, cols)]).astype(BF16)
            for k in range(wide):
                res[wide * s + k, n, rows, :] = out[:, k * HEAD_DIM:(k + 1) * HEAD_DIM]
            return 0

        lax.fori_loop(0, steps, body, 0)

    for n, load in enumerate(loads):
        load.wait()
        compute(pl.ds(0, block), n)
    heads.start(0)

    def step(j, _):
        gather.arrive(j)

        @pl.when(j <= 2)
        def _():
            gather.start(j + 4, True)

        @pl.when(j == 2)
        def _():
            for n in range(1, 5):
                dy_gather.start(n, False)

        rows = rows_at(gather.start_row(j), 2 * gather.part)
        lax.fori_loop(0, len(loads), lambda n, _: (compute(rows, n), 0)[1], 0)
        heads.start(j)
        return 0

    lax.fori_loop(1, Gather.STEPS + 1, step, 0)
    lax.fori_loop(1, Gather.STEPS + 1, lambda j, _: (gather.leave(j), 0)[1], 0)
    heads.wait()


def send_piece(cp_size, i, src, dst_of, send, recv, local, start):
    me = lax.axis_index('cp')
    half = jnp.where(i < cp_size, 0, 1)
    owner = jnp.where(i < cp_size, i, 2 * cp_size - 1 - i)

    @pl.when(owner == me)
    def _():
        copy = pltpu.make_async_copy(src, dst_of(half, me), local.at[half])
        copy.start() if start else copy.wait()

    @pl.when(owner != me)
    def _():
        copy = pltpu.make_async_remote_copy(
            src_ref=src, dst_ref=dst_of(half, me), send_sem=send.at[i], recv_sem=recv.at[me, half],
            device_id={'cp': owner}, device_id_type=MESH)
        copy.start() if start else copy.wait_send()


def forward_phase(cp_size, tp_size, gather, wo_ref, qkv, do_v, h_send, h_recv, h_local, in_sem, o_v, ot_v, l_v,
                  vt_ref, qt_ref, s_ref, acc_ref, wo, res):
    seq = qkv.shape[1]
    bq = s_ref.shape[0]
    nblk = seq // bq
    c = HEAD_DIM ** -0.5 * LOG2E
    heads = HeadSender(cp_size, tp_size, gather, res, do_v, h_send, h_recv, h_local)
    block = gather.block
    loads = [
        pltpu.make_async_copy(wo_ref, wo, in_sem.at[0]),
        pltpu.make_async_copy(gather.src, gather.buf.at[pl.ds(0, block), :], in_sem.at[1]),
    ]
    for load in loads:
        load.start()

    per_step = min(4, cp_size)
    cols = per_step * HEAD_DIM

    def compute(n):
        rows = rows_at(n * block, block)

        def body(s, _):
            out = dot_nt(gather.buf[rows, :], wo[rows_at(s * cols, cols), :]).astype(BF16)
            for k in range(per_step):
                res[per_step * s + k, 0, rows, :] = out[:, k * HEAD_DIM:(k + 1) * HEAD_DIM]
            return 0

        lax.fori_loop(0, cp_size // per_step, body, 0)

    def compute_steps(n):
        compute(n)
        lax.fori_loop(2 * n - 1, 2 * n + 1, lambda j, _: (heads.start(j), 0)[1], 0)

    def transpose_step(b, _):
        rows = rows_at(b * bq, bq)
        vt_ref[:, rows] = qkv[2, rows, :].T
        return 0

    lax.fori_loop(0, nblk, transpose_step, 0)

    def q_step(i, _):
        for n, at in enumerate((nblk // 4, nblk // 2, nblk - nblk // 4, nblk - 2)):
            @pl.when(i == at)
            def _():
                if n == 0:
                    for load in loads:
                        load.wait()
                    for j in range(1, 3):
                        gather.arrive(j)
                        gather.start(j + 4, True)
                    compute(0)
                    heads.start(0)
                else:
                    for j in range(max(3, 2 * n - 1), 2 * n + 1):
                        gather.arrive(j)
                    compute_steps(n)

        rows = rows_at(i * bq, bq)
        qt_ref[...] = qkv[0, rows, :].T
        acc_ref[...] = jnp.zeros_like(acc_ref)
        s = dot_nn(qkv[1, rows, :], qt_ref[...]) * c
        kk = lax.broadcasted_iota(jnp.int32, (bq, bq), 0)
        qq = lax.broadcasted_iota(jnp.int32, (bq, bq), 1)
        s = jnp.where(kk <= qq, s, -jnp.inf)
        s_ref[...] = s
        first = jnp.max(s, axis=0, keepdims=True)

        def use(blk, m_old, m, l, following):
            alpha = jnp.exp2(m_old - m)
            p = jnp.exp2(s_ref[...] - m)
            m_new = m
            if following is not None:
                s = dot_nn(qkv[1, rows_at(following * bq, bq), :], qt_ref[...]) * c
            part = jnp.sum(p, axis=0, keepdims=True)
            out = dot_nn(vt_ref[:, rows_at(blk * bq, bq)], p.astype(BF16))
            if following is not None:
                m_new = jnp.maximum(m, jnp.max(s, axis=0, keepdims=True))
                s_ref[...] = s
            acc_ref[...] = acc_ref[...] * alpha + out
            return m, m_new, l * alpha + part

        def body(t, carry):
            return use(jnp.where(t == 0, i, t - 1), *carry, t)

        carry = in_pairs(0, i, body, (first, first, jnp.zeros((1, bq), F32)))
        m, _, l = use(jnp.where(i == 0, i, i - 1), *carry, None)
        out = (acc_ref[...] * (1.0 / l)).astype(BF16)
        ot_v[:, rows] = out
        o_v[rows, :] = out.T
        l_v[i] = jnp.broadcast_to(m + jnp.log2(l), (8, bq))
        return 0

    lax.fori_loop(0, nblk, q_step, 0)
    heads.wait()
    lax.fori_loop(1, Gather.STEPS + 1, lambda j, _: (gather.leave(j), 0)[1], 0)


def backward_phase(cp_size, tp_size, wo_ref, rows_ref, o_rows_ref, oy_ref, wy_ref, qkv, do_v, o_v, ot_v, l_v,
                   send, recv, local, y_send, y_recv,
                   delta_v, kt_ref, qt_ref, dot_ref, p_ref, ds_ref, dst_ref, dq_acc, dk_acc, dv_acc, grads):
    seq = qkv.shape[1]
    bq = p_ref.shape[0]
    nblk, half_blk = 2 * cp_size, cp_size
    sub = bq // 2
    scale = HEAD_DIM ** -0.5
    c = scale * LOG2E
    me_c, me_t = lax.axis_index('cp'), lax.axis_index('tp')
    share, block = wy_ref.shape[1], oy_ref.shape[1]

    def over_tp(kind, r):
        peer = lax.rem(me_t + r, tp_size)
        src, dst = ((wo_ref.at[rows_at(me_c * share, share), :], wy_ref), (o_rows_ref.at[rows_at(peer * block, block), :], oy_ref))[kind]
        return pltpu.make_async_remote_copy(
            src_ref=src, dst_ref=dst.at[r - 1], send_sem=y_send.at[kind, r - 1], recv_sem=y_recv.at[kind, r - 1],
            device_id={'tp': peer}, device_id_type=MESH)

    for r in range(1, tp_size):
        over_tp(0, r).start()

    def piece(i):
        return rows_at(i * bq, bq)

    def init_step(b, _):
        rows = piece(b)
        kt_ref[:, rows] = qkv[1, rows, :].T
        qt_ref[:, rows] = qkv[0, rows, :].T
        dot_ref[:, rows] = do_v[0, rows, :].T
        prod = dot_ref[:, rows].astype(F32) * ot_v[:, rows].astype(F32)
        delta_v[b] = jnp.broadcast_to(jnp.sum(prod, axis=0, keepdims=True), (8, bq))
        for acc in (dq_acc, dk_acc, dv_acc):
            acc[:, rows] = jnp.zeros((HEAD_DIM, bq), F32)
        return 0

    lax.fori_loop(0, nblk, init_step, 0)

    def half_pair(r, q, k, prev, masked):
        sl = slice(r * sub, (r + 1) * sub)
        krows = rows_at(k * bq + r * sub, sub)
        if prev is not None:
            prev_q, prev_k = piece(prev[0]), rows_at(prev[1] * bq + r * sub, sub)
            old_p, old_ds_t, old_ds = p_ref[:, sl], ds_ref[sl, :], dst_ref[:, sl]
        s = dot_nn(qkv[1, krows, :], qt_ref[:, piece(q)])
        if prev is not None:
            dv_acc[:, prev_k] += dot_nn(dot_ref[:, prev_q], old_p)
        p = jnp.exp2(s * c - l_v[q][0:1, :])
        if masked:
            kk = lax.broadcasted_iota(jnp.int32, (sub, bq), 0) + r * sub
            p = jnp.where(kk <= lax.broadcasted_iota(jnp.int32, (sub, bq), 1), p, 0.0)
        p = p.astype(BF16)
        dp = dot_nn(qkv[2, krows, :], dot_ref[:, piece(q)])
        if prev is not None:
            dk_acc[:, prev_k] += dot_nn(qt_ref[:, prev_q], old_ds)
        ds = (p.astype(F32) * (dp - delta_v[q][0:1, :])).astype(BF16)
        out = dot_nn(kt_ref[:, prev_k], old_ds_t) if prev is not None else None
        p_ref[:, sl], ds_ref[sl, :], dst_ref[:, sl] = p.T, ds, ds.T
        return out

    def pair(q, k, prev, masked=False):
        out = half_pair(0, q, k, prev, masked)
        out = out + half_pair(1, q, k, prev, masked)
        dq_acc[:, piece(prev[0])] += out
        return q, k

    def source(kind, i):
        return (grads.at[pl.ds(0, 1), piece(i), :], grads.at[pl.ds(1, 2), piece(i), :], o_v.at[piece(i), :])[kind]

    def target(kind, part, head):
        cols = rows_at(head * HEAD_DIM, HEAD_DIM)
        return (rows_ref.at[pl.ds(0, 1), piece(part), cols], rows_ref.at[pl.ds(1, 2), piece(part), cols], o_rows_ref.at[piece(part), cols])[kind]

    def send_kind(kind, i, start):
        send_piece(cp_size, i, source(kind, i), functools.partial(target, kind), send.at[kind], recv.at[kind], local.at[kind], start)

    def settle(kind):
        def sent(i, _):
            send_kind(kind, i, False)
            return 0

        lax.fori_loop(0, nblk, sent, 0)
        for d in range(1, cp_size):
            peer = lax.rem(me_c + d, cp_size)
            for half in range(2):
                pltpu.make_async_remote_copy(
                    src_ref=source(kind, 0), dst_ref=target(kind, half, peer), send_sem=send.at[kind, 0], recv_sem=recv.at[kind, peer, half],
                    device_id={'cp': peer}, device_id_type=MESH).wait_recv()

    lax.fori_loop(0, nblk, lambda i, _: (send_kind(2, i, True), 0)[1], 0)

    def finish_q(i):
        grads[0, piece(i), :] = (dq_acc[:, piece(i)] * scale).T.astype(BF16)
        send_kind(0, i, True)

    def finish_kv(i):
        grads[1, piece(i), :] = (dk_acc[:, piece(i)] * scale).T.astype(BF16)
        grads[2, piece(i), :] = dv_acc[:, piece(i)].T.astype(BF16)
        send_kind(1, i, True)

    for r in range(2):
        half_pair(r, 0, 0, None, True)
    prev = lax.fori_loop(1, nblk, lambda i, prev: pair(i, i, prev, True), (0, 0), unroll=3)

    def late_column(k, prev):
        prev = pair(k + 1, k, prev)
        finish_kv(jnp.where(k == half_blk, nblk - 1, k - 1))
        return in_pairs(k + 2, nblk, lambda q, prev: pair(q, k, prev), prev)

    prev = lax.fori_loop(half_blk, nblk - 1, late_column, prev)

    def row(q, prev):
        prev = pair(q, 0, prev)

        @pl.when(q == 1)
        def _():
            finish_kv(nblk - 2)
            settle(2)
            for r in range(1, tp_size):
                over_tp(1, r).start()

        finish_q(q - 1)
        return in_pairs(1, jnp.minimum(q, half_blk), lambda k, prev: pair(q, k, prev), prev)

    rows_done = half_blk + 2
    prev = lax.fori_loop(1, rows_done, row, prev)

    def column(n, prev):
        def key(n):
            return jnp.where(n < half_blk // 2, 2 * n, 2 * (n - half_blk // 2) + 1)

        prev = pair(rows_done, key(n), prev)

        @pl.when(n == 0)
        def _():
            finish_q(rows_done - 1)

        @pl.when(n > 0)
        def _():
            finish_kv(key(n - 1))

        return lax.fori_loop(rows_done + 1, nblk, lambda q, prev: pair(q, key(n), prev), prev, unroll=True)

    if rows_done < nblk:
        prev = lax.fori_loop(0, half_blk, column, prev)
    last_q, last_k = piece(prev[0]), piece(prev[1])
    dv_acc[:, last_k] += dot_nn(dot_ref[:, last_q], p_ref[...])
    dk_acc[:, last_k] += dot_nn(qt_ref[:, last_q], dst_ref[...])
    dq_acc[:, last_q] += dot_nn(kt_ref[:, last_k], ds_ref[...])
    if rows_done < nblk:
        finish_kv(half_blk - 1)
        lax.fori_loop(rows_done, nblk, lambda q, _: (finish_q(q), 0)[1], 0)
    else:
        lax.fori_loop(0, half_blk, lambda k, _: (finish_kv(k), 0)[1], 0)
        finish_q(rows_done - 1)

    settle(0)
    settle(1)
    for r in range(1, tp_size):
        over_tp(0, r).wait()
        over_tp(1, r).wait()


def layer_kernel(cp_size, tp_size, x_ref, dy_ref, wq_ref, wk_ref, wv_ref, wo_ref, rows_ref, o_rows_ref, oy_ref, wy_ref,
                 qkv, do_v, xg, dyg, w_sem, in_sem, p_send, p_recv, p_local, h_send, h_recv, h_local,
                 x_send, x_recv, g_send, g_recv, send, recv, local, y_send, y_recv):
    seq = qkv.shape[1]
    bq = seq // (2 * cp_size)
    meet(*others('cp', cp_size), *others('tp', tp_size))
    gather = Gather(tp_size, dy_ref, dyg, g_send, g_recv)
    pl.run_scoped(
        functools.partial(
            project_phase, cp_size, tp_size, x_ref, (wq_ref, wk_ref, wv_ref), qkv, xg, gather,
            p_send, p_recv, p_local, w_sem, in_sem.at[0], x_send, x_recv),
        pltpu.VMEM((3, *wq_ref.shape), BF16), pltpu.VMEM((cp_size, 3, xg.shape[0], HEAD_DIM), BF16))
    turned, total, square = pltpu.VMEM((HEAD_DIM, seq), BF16), pltpu.VMEM((HEAD_DIM, seq), F32), pltpu.VMEM((bq, bq), BF16)
    logs = pltpu.VMEM((2 * cp_size, 8, bq), F32)

    def attend(o_v, ot_v, l_v):
        pl.run_scoped(
            functools.partial(forward_phase, cp_size, tp_size, gather, wo_ref, qkv, do_v, h_send, h_recv, h_local, in_sem, o_v, ot_v, l_v),
            turned, pltpu.VMEM((HEAD_DIM, bq), BF16), pltpu.VMEM((bq, bq), F32), pltpu.VMEM((HEAD_DIM, bq), F32),
            pltpu.VMEM(wo_ref.shape, BF16), pltpu.VMEM((cp_size, 1, dyg.shape[0], HEAD_DIM), BF16))
        pl.run_scoped(
            functools.partial(
                backward_phase, cp_size, tp_size, wo_ref, rows_ref, o_rows_ref, oy_ref, wy_ref, qkv, do_v, o_v, ot_v, l_v,
                send, recv, local, y_send, y_recv),
            logs, turned, turned, turned, square, square, square, total, total, total, pltpu.VMEM(qkv.shape, BF16))

    pl.run_scoped(attend, pltpu.VMEM((seq, HEAD_DIM), BF16), turned, logs)


def layer(x_blk, dy_blk, weights, w_out, cp_size, tp_size):
    block, width = x_blk.shape
    cols = w_out.shape[0]
    rows = block * tp_size
    seq = rows * cp_size
    pairs = seq * seq // 2
    each = DMA((Gather.STEPS, 2))
    gathered = pltpu.VMEM((rows, width), BF16)
    return pl.pallas_call(
        functools.partial(layer_kernel, cp_size, tp_size),
        out_shape=(
            jax.ShapeDtypeStruct((3, rows, cols), BF16),
            jax.ShapeDtypeStruct((rows, cols), BF16),
            jax.ShapeDtypeStruct((tp_size - 1, block, cols), BF16),
            jax.ShapeDtypeStruct((tp_size - 1, cols // cp_size, width), BF16),
        ),
        in_specs=[ANYWHERE] * 6,
        out_specs=(ANYWHERE,) * 4,
        scratch_shapes=[
            pltpu.VMEM((3, seq, HEAD_DIM), BF16),
            pltpu.VMEM((1, seq, HEAD_DIM), BF16),
            gathered, gathered, DMA((3,)), DMA((2,)), *head_sems(cp_size), *head_sems(cp_size), each, each, each, each,
            DMA((3, 2 * cp_size)), DMA((3, cp_size, 2)), DMA((3, 2)), DMA((2, tp_size)), DMA((2, tp_size)),
        ],
        compiler_params=params(0),
        cost_estimate=pl.CostEstimate(flops=14 * pairs * HEAD_DIM + 8 * rows * width * cols, bytes_accessed=8 * width * cols, transcendentals=2 * pairs),
        name="project_attend",
    )(x_blk, dy_blk, *weights, w_out)


def reduce_kernel(cp_size, tp_size, chunks, rows_ref, wq_ref, wk_ref, wv_ref, o_rows_ref, oy_ref, wo_ref, wy_ref,
                  out_ref, y_ref, wx_ref, sib_ref,
                  g_v, w_v, part, mid, last, out_v, stage, y_acc, o_v, in_sem, w_sem, out_sem, sends, recvs,
                  x_send, x_recv, d_send, d_recv, o_sem, s_sem):
    me, right, left = ring('tp', tp_size)
    far = lax.rem(me + 2, tp_size)
    block = part.shape[1]
    half = block // 2
    low, high = pl.ds(0, half), pl.ds(half, half)
    wide = part.shape[2] // chunks
    weights = (wq_ref, wk_ref, wv_ref)

    def w_load(n, a):
        return pltpu.make_async_copy(weights[a].at[rows_at(n * wide, wide), :], w_v.at[lax.rem(n, 2), a], w_sem.at[lax.rem(n, 2), a])

    owners = (far, right, left, me)
    blocks = [rows_at(owner * block, block) for owner in owners]
    loads = [pltpu.make_async_copy(rows_ref.at[:, rows, :], g_v.at[:, rows, :], in_sem.at[k]) for k, rows in enumerate(blocks)]
    loads[FAR].start()
    for a in range(3):
        w_load(0, a).start()
    for load in loads[RIGHT:]:
        load.start()
    me_c, mate = lax.axis_index('cp'), partner()
    chips = cp_size // 2
    ahead, behind = lax.rem(me_c + 2, cp_size), lax.rem(me_c + cp_size - 2, cp_size)
    nearest = (1, chips - 1) if chips > 2 else (1,)
    meet(*beside(tp_size), {'cp': mate}, *({'cp': peer} for peer in (ahead, behind)[:len(nearest)]))
    share = wy_ref.shape[1]

    def share_ref(s, k):
        return wy_ref.at[s] if k == 0 else wx_ref.at[s, k - 1]

    def x_copy(s, n, src, dst, peer):
        return pltpu.make_async_remote_copy(
            src_ref=src, dst_ref=dst, send_sem=x_send.at[s, n], recv_sem=x_recv.at[s, n], device_id={'cp': peer}, device_id_type=MESH)

    def along(s, n):
        return x_copy(s, n, wy_ref.at[s], wx_ref.at[s, nearest[n] - 1], (ahead, behind)[n])

    def relay(s, n):
        rows = pl.ds(n * (share // 2), share // 2)
        return x_copy(s, 2 + n, wx_ref.at[s, nearest[n] - 1, rows, :], wx_ref.at[s, 1, rows, :], (ahead, behind)[n])

    def across(s, k):
        return pltpu.make_async_remote_copy(
            src_ref=share_ref(s, k), dst_ref=sib_ref.at[s, k], send_sem=d_send.at[s, k], recv_sem=d_recv.at[s, k],
            device_id={'cp': mate}, device_id_type=MESH)

    slots = range(tp_size - 1)
    for s in slots:
        for n in range(len(nearest)):
            along(s, n).start()
        across(s, 0).start()
    o_loads = [pltpu.make_async_copy(o_rows_ref.at[rows_at(me * (o_rows_ref.shape[0] // tp_size), o_rows_ref.shape[0] // tp_size), :], o_v.at[0], o_sem.at[0])]
    for s in range(tp_size - 1):
        o_loads.append(pltpu.make_async_copy(oy_ref.at[s], o_v.at[s + 1], o_sem.at[s + 1]))
    for copy in o_loads:
        copy.start()

    kinds = ('far_r', 'far_l', 'plain_r', 'plain_l', 'sum_r', 'sum_l')

    def hop(kind, n):
        cols = rows_at(n * wide, wide)
        src, dst, peer = {
            'far_r': (part.at[FAR, low, cols], mid.at[0, :, cols], right),
            'far_l': (part.at[FAR, high, cols], mid.at[1, :, cols], left),
            'plain_r': (part.at[RIGHT, high, cols], last.at[0, high, cols], right),
            'plain_l': (part.at[LEFT, low, cols], last.at[1, low, cols], left),
            'sum_r': (part.at[RIGHT, low, cols], last.at[0, low, cols], right),
            'sum_l': (part.at[LEFT, high, cols], last.at[1, high, cols], left),
        }[kind]
        k = kinds.index(kind)
        return pltpu.make_async_remote_copy(
            src_ref=src, dst_ref=dst, send_sem=sends.at[k, n], recv_sem=recvs.at[k, n], device_id={'tp': peer}, device_id_type=MESH)

    def compute(n, _):
        slot = lax.rem(n, 2)

        @pl.when(n + 1 < chunks)
        def _():
            for a in range(3):
                w_load(n + 1, a).start()

        for a in range(3):
            w_load(n, a).wait()
        cols = rows_at(n * wide, wide)
        ready = {FAR: ('far_r', 'far_l'), RIGHT: ('plain_r',), LEFT: ('plain_l',), OWN: ()}
        for k, rows in enumerate(blocks):
            @pl.when(n == 0)
            def _():
                loads[k].wait()

            total = dot_nt(g_v[0, rows, :], w_v[slot, 0])
            total = total + dot_nt(g_v[1, rows, :], w_v[slot, 1])
            part[k, :, cols] = total + dot_nt(g_v[2, rows, :], w_v[slot, 2])
            for kind in ready[k]:
                hop(kind, n).start()
        return 0

    lax.fori_loop(0, chunks, compute, 0)
    for s in slots:
        for n, k in enumerate(nearest):
            along(s, n).wait_recv()
            if chips > 2:
                relay(s, n).start()
            across(s, k).start()

    def forward_sums(n, _):
        cols = rows_at(n * wide, wide)
        hop('far_r', n).wait_recv()
        part[RIGHT, :half, cols] += mid[0, :, cols]
        hop('sum_r', n).start()
        hop('far_l', n).wait_recv()
        part[LEFT, half:, cols] += mid[1, :, cols]
        hop('sum_l', n).start()
        return 0

    lax.fori_loop(0, chunks, forward_sums, 0)

    if chips > 2:
        for s in slots:
            for n in range(2):
                relay(s, n).wait_recv()
            across(s, 2).start()
    for copy in o_loads:
        copy.wait()
    span = stage.shape[2]
    halves = y_acc.shape[1] // span

    def stage_copies(n):
        s, h = divmod(n, halves)
        cols = pl.ds(h * span, span)
        slot = n % 2
        if s == 0:
            return [pltpu.make_async_copy(wo_ref.at[:, cols], stage.at[slot], s_sem.at[slot, 0])]
        copies = []
        for k in range(cp_size // 2):
            mine, its = lax.rem(me_c + cp_size - 2 * k, cp_size), lax.rem(mate + cp_size - 2 * k, cp_size)
            copies.append(pltpu.make_async_copy(
                share_ref(s - 1, k).at[:, cols], stage.at[slot, rows_at(mine * share, share), :], s_sem.at[slot, 2 * k]))
            copies.append(pltpu.make_async_copy(
                sib_ref.at[s - 1, k, :, cols], stage.at[slot, rows_at(its * share, share), :], s_sem.at[slot, 2 * k + 1]))
        return copies

    def stage_start(n):
        s, h = divmod(n, halves)
        if s > 0 and h == 0:
            for k in range(cp_size // 2):
                across(s - 1, k).wait_recv()
        for copy in stage_copies(n):
            copy.start()

    total_steps = tp_size * halves
    stage_start(0)
    for n in range(total_steps):
        if n + 1 < total_steps:
            stage_start(n + 1)
        for copy in stage_copies(n):
            copy.wait()
        s, h = divmod(n, halves)
        tile = min(512, span)

        def y_step(j, _):
            cols = rows_at(j * tile, tile)
            out = rows_at(h * span + j * tile, tile)
            product = dot_nn(o_v[s], stage[n % 2, :, cols])
            if s == 0:
                y_acc[:, out] = product
            elif s < tp_size - 1:
                y_acc[:, out] += product
            else:
                out_v[:, out] = (y_acc[:, out] + product).astype(BF16)
            return 0

        lax.fori_loop(0, span // tile, y_step, 0)
    y_out = pltpu.make_async_copy(out_v, y_ref, in_sem.at[OWN])
    y_out.start()
    y_out.wait()

    def put(n):
        cols = rows_at(n * wide, wide)
        return pltpu.make_async_copy(out_v.at[:, cols], out_ref.at[:, cols], out_sem.at[n])

    def finish(n, _):
        cols = rows_at(n * wide, wide)
        for kind in ('plain_r', 'plain_l', 'sum_r', 'sum_l'):
            hop(kind, n).wait_recv()
        out_v[:, cols] = (part[OWN, :, cols] + last[0, :, cols] + last[1, :, cols]).astype(BF16)
        put(n).start()
        return 0

    lax.fori_loop(0, chunks, finish, 0)

    def close(n, _):
        put(n).wait()
        for kind in kinds:
            hop(kind, n).wait_send()
        return 0

    lax.fori_loop(0, chunks, close, 0)
    for s in slots:
        for k in range(chips):
            across(s, k).wait_send()
        for n in range(len(nearest)):
            along(s, n).wait_send()
            if chips > 2:
                relay(s, n).wait_send()


def reduce_out(grad_rows, weights, o_rows, oy, w_out, wy, cp_size, tp_size):
    width, cols = weights[0].shape
    share = wy.shape[1]
    pairs = cp_size // 2
    rows = grad_rows.shape[1]
    block = rows // tp_size
    chunks = 8
    wide = width // chunks
    return pl.pallas_call(
        functools.partial(reduce_kernel, cp_size, tp_size, chunks),
        out_shape=(
            jax.ShapeDtypeStruct((block, width), BF16),
            jax.ShapeDtypeStruct((block, width), BF16),
            jax.ShapeDtypeStruct((tp_size - 1, pairs - 1, share, width), BF16),
            jax.ShapeDtypeStruct((tp_size - 1, pairs, share, width), BF16),
        ),
        in_specs=[ANYWHERE] * 8,
        out_specs=(ANYWHERE,) * 4,
        scratch_shapes=[
            pltpu.VMEM((3, rows, cols), BF16),
            pltpu.VMEM((2, 3, wide, cols), BF16),
            pltpu.VMEM((4, block, width), F32),
            pltpu.VMEM((2, block // 2, width), F32),
            pltpu.VMEM((2, block, width), F32),
            pltpu.VMEM((block, width), BF16),
            pltpu.VMEM((2, cols, width // 4), BF16),
            pltpu.VMEM((block, width), F32),
            pltpu.VMEM((tp_size, block, cols), BF16),
            DMA((4,)), DMA((2, 3)), DMA((chunks,)), DMA((6, chunks)), DMA((6, chunks)),
            DMA((tp_size - 1, 4)), DMA((tp_size - 1, 4)), DMA((tp_size - 1, pairs)), DMA((tp_size - 1, pairs)),
            DMA((tp_size,)), DMA((2, cp_size)),
        ],
        compiler_params=params(1),
        cost_estimate=pl.CostEstimate(flops=6 * rows * width * cols, bytes_accessed=6 * width * cols, transcendentals=0),
        name="project_reduce",
    )(grad_rows, *weights, o_rows, oy, w_out, wy)


def solution(mesh):
    cp_size, tp_size = mesh.shape['cp'], mesh.shape['tp']
    row_spec = P(('dp', 'cp', 'tp'), None)

    def local_step(x_blk, dy_blk, w_query, w_key, w_value, w_out):
        weights = (w_query, w_key, w_value)
        grad_rows, o_rows, oy, wy = layer(x_blk, dy_blk, weights, w_out, cp_size, tp_size)
        dx_blk, y_blk, _, _ = reduce_out(grad_rows, weights, o_rows, oy, w_out, wy, cp_size, tp_size)
        return y_blk, dx_blk

    weight = P(None, 'tp')
    return jax.shard_map(local_step, mesh=mesh, in_specs=(row_spec, row_spec, weight, weight, weight, P('tp', None)), out_specs=(row_spec, row_spec), check_vma=False)
```
